16 devices in a mesh: vp: 2 (over z), dp: 8 (over y, x, core).
Axes of the slice: x: 2, y: 2, z: 2, core: 2. Of those that a mesh axis runs over, the one named last changes fastest.
Arguments:
- student_x: bfloat16 [1280, 1536], P('dp')
- teacher_x: bfloat16 [256, 1536], P('dp')
- w_in: bfloat16 [1536, 2048], replicated
- b_in: bfloat16 [2048], replicated
- w_mid: bfloat16 [2048, 2048], replicated
- b_mid: bfloat16 [2048], replicated
- w_out: bfloat16 [2048, 384], replicated
- b_out: bfloat16 [384], replicated
- protos: bfloat16 [384, 131072], P(None, 'vp')
- ema_w_in: bfloat16 [1536, 2048], replicated
- ema_b_in: bfloat16 [2048], replicated
- ema_w_mid: bfloat16 [2048, 2048], replicated
- ema_b_mid: bfloat16 [2048], replicated
- ema_w_out: bfloat16 [2048, 384], replicated
- ema_b_out: bfloat16 [384], replicated
- ema_protos: bfloat16 [384, 131072], P(None, 'vp')
Outputs:
- output 1: float32 [], replicated
- output 2: float32 [1536, 2048], replicated
- output 3: float32 [2048], replicated
- output 4: float32 [2048, 2048], replicated
- output 5: float32 [2048], replicated
- output 6: float32 [2048, 384], replicated
- output 7: float32 [384], replicated
- output 8: float32 [384, 131072], P(None, 'vp')
All inputs are finite; a program needn't handle non-finite values.
Results may differ from the reference program's by a relative error of at most 0.00516174.
Values sent between devices are 32-bit elements.
A program may use at most 1 GiB of HBM per device.

```python
import jax
import jax.numpy as jnp
from jax import lax
from functools import partial

EMBED_DIM = 1536
HIDDEN_DIM = 2048
BOTTLENECK = 384
PROTOTYPES = 131072
TOTAL_IMAGES = 128
ALL_CROPS = 10
GLOBAL_CROPS = 2
SINK_ITERS = 3
IMAGE_BLOCK = 8
TEMP_STUDENT = 0.1
TEMP_TEACHER = 0.04


def setup_inputs(seed: int = 0) -> dict:
    keys = jax.random.split(jax.random.key(seed), 20)
    n_clusters = 4
    centers = jax.random.normal(keys[0], (n_clusters, EMBED_DIM), jnp.float32)
    cluster_of = (jnp.arange(TOTAL_IMAGES) * n_clusters) // TOTAL_IMAGES
    img_mean = centers[cluster_of] + 0.7 * jax.random.normal(keys[1], (TOTAL_IMAGES, EMBED_DIM), jnp.float32)
    teacher_x = img_mean[:, None, :] + 0.5 * jax.random.normal(keys[2], (TOTAL_IMAGES, GLOBAL_CROPS, EMBED_DIM), jnp.float32)
    student_x = img_mean[:, None, :] + 0.7 * jax.random.normal(keys[3], (TOTAL_IMAGES, ALL_CROPS, EMBED_DIM), jnp.float32)

    def make_dense(key, fan_in, fan_out):
        return jax.random.normal(key, (fan_in, fan_out), jnp.float32) * fan_in ** -0.5

    def make_bias(key, width):
        return 0.5 * jax.random.normal(key, (width,), jnp.float32)

    w_in = make_dense(keys[4], EMBED_DIM, HIDDEN_DIM)
    b_in = make_bias(keys[5], HIDDEN_DIM)
    w_mid = make_dense(keys[6], HIDDEN_DIM, HIDDEN_DIM)
    b_mid = make_bias(keys[7], HIDDEN_DIM)
    w_out = make_dense(keys[8], HIDDEN_DIM, BOTTLENECK)
    b_out = make_bias(keys[9], BOTTLENECK)
    col_scale = jnp.exp(0.5 * jax.random.normal(keys[10], (1, PROTOTYPES), jnp.float32))
    protos = jax.random.normal(keys[11], (BOTTLENECK, PROTOTYPES), jnp.float32) * col_scale
    ema_w_in = 0.8 * w_in + 0.6 * make_dense(keys[12], EMBED_DIM, HIDDEN_DIM)
    ema_b_in = 0.8 * b_in + 0.6 * make_bias(keys[13], HIDDEN_DIM)
    ema_w_mid = 0.8 * w_mid + 0.6 * make_dense(keys[14], HIDDEN_DIM, HIDDEN_DIM)
    ema_b_mid = 0.8 * b_mid + 0.6 * make_bias(keys[15], HIDDEN_DIM)
    ema_w_out = 0.8 * w_out + 0.6 * make_dense(keys[16], HIDDEN_DIM, BOTTLENECK)
    ema_b_out = 0.8 * b_out + 0.6 * make_bias(keys[17], BOTTLENECK)
    ema_protos = 0.8 * protos + 0.6 * jax.random.normal(keys[18], (BOTTLENECK, PROTOTYPES), jnp.float32) * col_scale
    return {
        'student_x': student_x.reshape(TOTAL_IMAGES * ALL_CROPS, EMBED_DIM).astype(jnp.bfloat16),
        'teacher_x': teacher_x.reshape(TOTAL_IMAGES * GLOBAL_CROPS, EMBED_DIM).astype(jnp.bfloat16),
        'w_in': w_in.astype(jnp.bfloat16),
        'b_in': b_in.astype(jnp.bfloat16),
        'w_mid': w_mid.astype(jnp.bfloat16),
        'b_mid': b_mid.astype(jnp.bfloat16),
        'w_out': w_out.astype(jnp.bfloat16),
        'b_out': b_out.astype(jnp.bfloat16),
        'protos': protos.astype(jnp.bfloat16),
        'ema_w_in': ema_w_in.astype(jnp.bfloat16),
        'ema_b_in': ema_b_in.astype(jnp.bfloat16),
        'ema_w_mid': ema_w_mid.astype(jnp.bfloat16),
        'ema_b_mid': ema_b_mid.astype(jnp.bfloat16),
        'ema_w_out': ema_w_out.astype(jnp.bfloat16),
        'ema_b_out': ema_b_out.astype(jnp.bfloat16),
        'ema_protos': ema_protos.astype(jnp.bfloat16),
    }


def snap_bf16(vals):
    return vals.astype(jnp.bfloat16).astype(jnp.float32)


def head_mlp(feats, w_in, b_in, w_mid, b_mid, w_out, b_out):
    hid_one = snap_bf16(jax.nn.gelu(jnp.dot(feats, w_in, preferred_element_type=jnp.float32) + b_in, approximate=False))
    hid_two = snap_bf16(jax.nn.gelu(jnp.dot(hid_one, w_mid, preferred_element_type=jnp.float32) + b_mid, approximate=False))
    proj = jnp.dot(hid_two, w_out, preferred_element_type=jnp.float32) + b_out
    return snap_bf16(proj / jnp.sqrt(jnp.sum(proj * proj, axis=-1, keepdims=True)))


def col_normalize(protos):
    return snap_bf16(protos / jnp.sqrt(jnp.sum(protos * protos, axis=0, keepdims=True)))


def block_loss(q_blk, emb_blk, proto_mat):
    logits = jnp.dot(emb_blk, proto_mat, preferred_element_type=jnp.float32) / TEMP_STUDENT
    log_p = jax.nn.log_softmax(logits.reshape(IMAGE_BLOCK, ALL_CROPS, PROTOTYPES), axis=-1)
    cross = jnp.einsum('iak,ivk->iav', q_blk, log_p)
    pair_mask = (jnp.arange(GLOBAL_CROPS)[:, None] != jnp.arange(ALL_CROPS)[None, :]).astype(jnp.float32)
    return -jnp.sum(cross * pair_mask) / (TOTAL_IMAGES * GLOBAL_CROPS * (ALL_CROPS - 1))


def reference(student_x, teacher_x, w_in, b_in, w_mid, b_mid, w_out, b_out, protos,
              ema_w_in, ema_b_in, ema_w_mid, ema_b_mid, ema_w_out, ema_b_out, ema_protos):
    t_emb = head_mlp(teacher_x.astype(jnp.float32), ema_w_in.astype(jnp.float32), ema_b_in.astype(jnp.float32),
                     ema_w_mid.astype(jnp.float32), ema_b_mid.astype(jnp.float32),
                     ema_w_out.astype(jnp.float32), ema_b_out.astype(jnp.float32))
    t_logits = jnp.dot(t_emb, col_normalize(ema_protos.astype(jnp.float32)), preferred_element_type=jnp.float32)
    n_rows = GLOBAL_CROPS * TOTAL_IMAGES
    q_mat = jnp.exp(t_logits / TEMP_TEACHER)
    q_mat = q_mat / jnp.sum(q_mat)
    for _ in range(SINK_ITERS):
        q_mat = q_mat / jnp.sum(q_mat, axis=0, keepdims=True) / PROTOTYPES
        q_mat = q_mat / jnp.sum(q_mat, axis=1, keepdims=True) / n_rows
    q_mat = q_mat * n_rows
    n_blocks = TOTAL_IMAGES // IMAGE_BLOCK
    q_blocks = q_mat.reshape(n_blocks, IMAGE_BLOCK, GLOBAL_CROPS, PROTOTYPES)

    feats = student_x.astype(jnp.float32)
    student_params = (w_in.astype(jnp.float32), b_in.astype(jnp.float32), w_mid.astype(jnp.float32),
                      b_mid.astype(jnp.float32), w_out.astype(jnp.float32), b_out.astype(jnp.float32))

    def student_embed(params):
        return head_mlp(feats, params[0], params[1], params[2], params[3], params[4], params[5])

    s_emb, emb_vjp = jax.vjp(student_embed, student_params)
    proto_unit, proto_vjp = jax.vjp(col_normalize, protos.astype(jnp.float32))
    emb_blocks = s_emb.reshape(n_blocks, IMAGE_BLOCK * ALL_CROPS, BOTTLENECK)

    def scan_step(carry, blk):
        q_blk, emb_blk = blk
        part_loss, blk_vjp = jax.vjp(partial(block_loss, q_blk), emb_blk, proto_unit)
        g_emb_blk, g_unit_blk = blk_vjp(jnp.ones((), jnp.float32))
        return (carry[0] + part_loss, carry[1] + g_unit_blk), g_emb_blk

    init = (jnp.zeros((), jnp.float32), jnp.zeros((BOTTLENECK, PROTOTYPES), jnp.float32))
    (loss, g_unit), g_emb = lax.scan(scan_step, init, (q_blocks, emb_blocks))
    g_params = emb_vjp(g_emb.reshape(TOTAL_IMAGES * ALL_CROPS, BOTTLENECK))[0]
    g_protos = proto_vjp(g_unit)[0]
    return (loss, g_params[0], g_params[1], g_params[2], g_params[3], g_params[4], g_params[5], g_protos)
```

```python
import functools

import jax
import jax.numpy as jnp
from jax import lax
from jax.experimental import pallas as pl
from jax.experimental.pallas import tpu as pltpu
from jax.sharding import PartitionSpec as P

ALL_CROPS = 10
GLOBAL_CROPS = 2
TEMP_STUDENT = 0.1
TEMP_TEACHER = 0.04
LOG2E = 1.4426950408889634
LANES = 128
NB_A = 512
NB_B = 512
OUT_SLOTS = 4
F32 = jnp.float32
BF16 = jnp.bfloat16
MESH = pl.DeviceIdType.MESH
HBM = pl.BlockSpec(memory_space=pl.ANY)
VMEM = pl.BlockSpec(memory_space=pltpu.VMEM)


def gelu_slope(pre):
    cdf = 0.5 * (1.0 + lax.erf(pre * 0.7071067811865476))
    return cdf + pre * jnp.exp(-0.5 * pre * pre) * 0.3989422804014327


def mlp_forward(feats, w_in, b_in, w_mid, b_mid, w_out, b_out):
    pre_one = jnp.dot(feats, w_in, preferred_element_type=F32) + b_in.astype(F32)
    hid_one = jax.nn.gelu(pre_one, approximate=False).astype(BF16)
    pre_two = jnp.dot(hid_one, w_mid, preferred_element_type=F32) + b_mid.astype(F32)
    hid_two = jax.nn.gelu(pre_two, approximate=False).astype(BF16)
    proj = jnp.dot(hid_two, w_out, preferred_element_type=F32) + b_out.astype(F32)
    inv_norm = lax.rsqrt(jnp.sum(proj * proj, axis=-1, keepdims=True))
    unit = proj * inv_norm
    return unit, (pre_one, hid_one, pre_two, hid_two, unit, inv_norm)


def mlp_backward(g_emb, feats, saved, w_mid, w_out):
    pre_one, hid_one, pre_two, hid_two, unit, inv_norm = saved
    g_proj = (g_emb - unit * jnp.sum(unit * g_emb, axis=-1, keepdims=True)) * inv_norm
    g_proj_lo = g_proj.astype(BF16)
    g_w_out = jnp.einsum('nh,nb->hb', hid_two, g_proj_lo, preferred_element_type=F32)
    g_hid_two = jnp.einsum('nb,hb->nh', g_proj_lo, w_out, preferred_element_type=F32)
    g_pre_two = g_hid_two.astype(BF16).astype(F32) * gelu_slope(pre_two)
    g_pre_two_lo = g_pre_two.astype(BF16)
    g_w_mid = jnp.einsum('ng,nh->gh', hid_one, g_pre_two_lo, preferred_element_type=F32)
    g_hid_one = jnp.einsum('nh,gh->ng', g_pre_two_lo, w_mid, preferred_element_type=F32)
    g_pre_one = g_hid_one.astype(BF16).astype(F32) * gelu_slope(pre_one)
    g_w_in = jnp.einsum('nf,nh->fh', feats, g_pre_one.astype(BF16), preferred_element_type=F32)
    return (g_w_in, jnp.sum(g_pre_one, axis=0), g_w_mid, jnp.sum(g_pre_two, axis=0), g_w_out, jnp.sum(g_proj, axis=0))


def unit_columns(block):
    block_f = block.astype(F32)
    inv_col = lax.rsqrt(jnp.sum(block_f * block_f, axis=0, keepdims=True))
    return block_f * inv_col, inv_col


def dot(left, right):
    return jnp.dot(left, right, preferred_element_type=F32)


def dot_t(left, right):
    return lax.dot_general(left, right, (((1,), (1,)), ((), ())), preferred_element_type=F32)


def to_column(row):
    return jnp.transpose(jnp.broadcast_to(row, (LANES, row.shape[1])))


def to_row(acc):
    return jnp.sum(jnp.transpose(acc), axis=0, keepdims=True)


def fold_lanes(wide):
    total = wide[:, :LANES]
    for start in range(LANES, wide.shape[1], LANES):
        total = total + wide[:, start:start + LANES]
    return total


def my_place():
    return lax.axis_index('vp'), lax.axis_index('dp')


def gather_kernel(n_dp, block_ref, all_ref, out_sem, in_sem, fwd_out, fwd_in):
    vp, me = my_place()
    n_chip = n_dp // 2
    chip, core = me // 2, me % 2
    partner = chip * 2 + 1 - core
    barrier = pltpu.get_barrier_semaphore()
    pl.semaphore_signal(barrier, inc=1, device_id=(vp, partner), device_id_type=MESH)
    for k in range(1, n_chip):
        peer = ((chip + k) % n_chip) * 2 + core
        pl.semaphore_signal(barrier, inc=1, device_id=(vp, peer), device_id_type=MESH)
    pl.semaphore_wait(barrier, n_chip)
    sends = []
    for k in range(1, n_chip):
        peer = ((chip + k) % n_chip) * 2 + core
        sends.append(pltpu.make_async_remote_copy(
            src_ref=block_ref, dst_ref=all_ref.at[me], send_sem=out_sem.at[k], recv_sem=in_sem.at[chip],
            device_id=(vp, peer), device_id_type=MESH))
    own = pltpu.make_async_remote_copy(
        src_ref=block_ref, dst_ref=all_ref.at[me], send_sem=fwd_out.at[chip], recv_sem=fwd_in.at[chip],
        device_id=(vp, partner), device_id_type=MESH)
    for copy in sends:
        copy.start()
    own.start()
    all_ref[me] = block_ref[...]
    for k in range(1, n_chip):
        src = (chip + n_chip - k) % n_chip
        slot = src * 2 + core
        peer_copy = pltpu.make_async_remote_copy(
            src_ref=block_ref, dst_ref=all_ref.at[slot], send_sem=out_sem.at[k], recv_sem=in_sem.at[src],
            device_id=(vp, partner), device_id_type=MESH)
        peer_copy.wait_recv()
        forward = pltpu.make_async_remote_copy(
            src_ref=all_ref.at[slot], dst_ref=all_ref.at[slot], send_sem=fwd_out.at[src], recv_sem=fwd_in.at[src],
            device_id=(vp, partner), device_id_type=MESH)
        forward.start()
    for copy in sends:
        copy.wait_send()
    for src in range(n_chip):
        slot = src * 2 + core
        other = src * 2 + 1 - core
        pltpu.make_async_remote_copy(
            src_ref=all_ref.at[slot], dst_ref=all_ref.at[other], send_sem=fwd_out.at[src], recv_sem=fwd_in.at[src],
            device_id=(vp, partner), device_id_type=MESH).wait()


def gather_dp(block, n_dp, collective_id):
    return pl.pallas_call(
        functools.partial(gather_kernel, n_dp),
        out_shape=jax.ShapeDtypeStruct((n_dp,) + block.shape, block.dtype),
        in_specs=[VMEM],
        out_specs=VMEM,
        scratch_shapes=[pltpu.SemaphoreType.DMA((n_dp // 2,))] * 4,
        compiler_params=pltpu.CompilerParams(
            collective_id=collective_id, has_side_effects=True, vmem_limit_bytes=48 << 20),
        name="gather_dp",
    )(block)


def stats_kernel(n_vp, n_dp, zs_ref, zt_ref, v_hbm, vt_hbm, c_ref, rs_ref, r_ref, ge_ref, loss_ref,
                 vbuf, tbuf, in_sem, ubuf, kbuf, acc_s, acc_r, wbuf, snd, rcv, send_sem, recv_sem, c_out, c_in):
    vp, dp = my_place()
    n_dev = n_vp * n_dp
    me = vp * n_dp + dp
    rows, rows_t = zs_ref.shape[0], zt_ref.shape[0]
    n_img = rows // ALL_CROPS
    n_col = kbuf.shape[1]
    n_blk = n_col // NB_A
    base = dp * n_col

    barrier = pltpu.get_barrier_semaphore()
    for k in range(1, n_dev):
        peer = (me + k) % n_dev
        pl.semaphore_signal(barrier, inc=1, device_id=(peer // n_dp, peer % n_dp), device_id_type=MESH)

    def load(j, slot):
        cols = pl.ds(pl.multiple_of(base + j * NB_A, NB_A), NB_A)
        return (pltpu.make_async_copy(v_hbm.at[:, cols], vbuf.at[slot], in_sem.at[0, slot]),
                pltpu.make_async_copy(vt_hbm.at[:, cols], tbuf.at[slot], in_sem.at[1, slot]))

    for copy in load(0, 0):
        copy.start()
    acc_s[...] = jnp.zeros_like(acc_s)
    acc_r[...] = jnp.zeros_like(acc_r)
    ge_ref[...] = jnp.zeros_like(ge_ref)

    @pl.loop(0, n_blk)
    def _(j):
        slot = j % 2

        @pl.when(j + 1 < n_blk)
        def _():
            for copy in load(j + 1, 1 - slot):
                copy.start()

        for copy in load(j, slot):
            copy.wait()
        here = pl.ds(pl.multiple_of(j * NB_A, NB_A), NB_A)
        unit_t = unit_columns(tbuf[slot])[0].astype(BF16)
        kern = jnp.exp2(dot(zt_ref[...], unit_t) * (LOG2E / TEMP_TEACHER))
        kbuf[:, here] = kern
        acc_r[...] += fold_lanes(kern * (1.0 / jnp.sum(kern, axis=0, keepdims=True)))
        unit = unit_columns(vbuf[slot])[0].astype(BF16)
        ubuf[:, here] = unit
        exp_s = jnp.exp2(dot(zs_ref[...], unit) * (LOG2E / TEMP_STUDENT))
        acc_s[...] += fold_lanes(exp_s)
        ge_ref[...] += dot_t(exp_s.astype(BF16), unit)

    pl.semaphore_wait(barrier, n_dev - 1)

    def exchange(step, width):
        def copy(k, dst, peer):
            return pltpu.make_async_remote_copy(
                src_ref=snd.at[step, :, :width], dst_ref=rcv.at[step, dst, :, :width],
                send_sem=send_sem.at[step, k], recv_sem=recv_sem.at[step, dst],
                device_id=(peer // n_dp, peer % n_dp), device_id_type=MESH)
        for k in range(1, n_dev):
            copy(k, me, (me + k) % n_dev).start()
        rcv[step, me, :, :width] = snd[step, :, :width]
        for k in range(1, n_dev):
            src = (me + n_dev - k) % n_dev
            copy(k, src, src).wait()
        total = rcv[step, 0, :, :width]
        for k in range(1, n_dev):
            total = total + rcv[step, k, :, :width]
        return total

    snd[0, :, :rows_t] = to_row(acc_r[...])
    snd[0, :, rows_t:rows_t + rows] = to_row(acc_s[...])
    total = exchange(0, rows_t + rows)
    row_sum = total[:, rows_t:]
    rs_ref[...] = row_sum
    r_row = 1.0 / total[:, :rows_t]

    for step in (1, 2):
        r_col = to_column(r_row)
        acc_r[...] = jnp.zeros_like(acc_r)

        @pl.loop(0, n_col // LANES)
        def _(j):
            here = pl.ds(pl.multiple_of(j * LANES, LANES), LANES)
            kern = kbuf[:, here]
            c_row = 1.0 / jnp.sum(kern * r_col, axis=0, keepdims=True)
            acc_r[...] += kern * c_row
            if step == 2:
                c_ref[dp, :, here] = c_row

        if step == 2:
            for k in range(1, n_dp):
                pltpu.make_async_remote_copy(
                    src_ref=c_ref.at[dp], dst_ref=c_ref.at[dp], send_sem=c_out.at[k], recv_sem=c_in.at[dp],
                    device_id=(vp, (dp + k) % n_dp), device_id_type=MESH).start()
        snd[step, :, :rows_t] = to_row(acc_r[...])
        r_row = 1.0 / exchange(step, rows_t)
    r_ref[...] = r_row

    r_col = to_column(r_row)
    r_wide = jnp.concatenate([r_col] * (NB_A // LANES), axis=1)
    wbuf[...] = jnp.zeros_like(wbuf)

    @pl.loop(0, n_blk)
    def _(j):
        here = pl.ds(pl.multiple_of(j * NB_A, NB_A), NB_A)
        q_mat = kbuf[:, here] * c_ref[dp, :, here] * r_wide
        q_hi = q_mat.astype(BF16)
        q_lo = (q_mat - q_hi.astype(F32)).astype(BF16)
        unit = ubuf[:, here]
        wbuf[...] += dot_t(q_hi, unit) + dot_t(q_lo, unit)

    w_zero = wbuf[:n_img]
    w_one = wbuf[n_img:]
    w_both = w_zero + w_one
    scale = 1.0 / (n_img * GLOBAL_CROPS * (ALL_CROPS - 1))
    log_rs = jnp.log(row_sum)
    inv_rs = to_column(1.0 / row_sum)
    loss = jnp.zeros((1, LANES), F32)
    for v in range(ALL_CROPS):
        block = pl.ds(v * n_img, n_img)
        count = float(GLOBAL_CROPS - (v < GLOBAL_CROPS))
        w_v = (w_one, w_zero)[v] if v < GLOBAL_CROPS else w_both
        inv = inv_rs[v * n_img:(v + 1) * n_img]
        inv = jnp.concatenate([inv] * (ge_ref.shape[1] // LANES), axis=1)
        dots = fold_lanes(jnp.sum(zs_ref[block].astype(F32) * w_v, axis=0, keepdims=True))
        logs = log_rs[:, v * n_img:(v + 1) * n_img]
        loss += (count / n_dev) * logs - (1.0 / TEMP_STUDENT) * dots
        ge_ref[block] = (count * (ge_ref[block] * inv) - w_v) * (scale / TEMP_STUDENT)
    loss_ref[...] = loss * scale

    for k in range(1, n_dp):
        src = (dp + n_dp - k) % n_dp
        pltpu.make_async_remote_copy(
            src_ref=c_ref.at[dp], dst_ref=c_ref.at[src], send_sem=c_out.at[k], recv_sem=c_in.at[src],
            device_id=(vp, src), device_id_type=MESH).wait()


def sinkhorn_stats(z_s, z_t, protos, ema_protos, n_vp, n_dp):
    rows, width = z_s.shape
    rows_t = z_t.shape[0]
    n_col = protos.shape[1] // n_dp
    n_dev = n_vp * n_dp
    flops = 2 * rows * n_col * width * 2
    return pl.pallas_call(
        functools.partial(stats_kernel, n_vp, n_dp),
        out_shape=(jax.ShapeDtypeStruct((n_dp, 1, n_col), F32),
                   jax.ShapeDtypeStruct((1, rows), F32),
                   jax.ShapeDtypeStruct((1, rows_t), F32),
                   jax.ShapeDtypeStruct((rows, width), F32),
                   jax.ShapeDtypeStruct((1, LANES), F32)),
        in_specs=[VMEM, VMEM, HBM, HBM],
        out_specs=(VMEM,) * 5,
        scratch_shapes=[
            pltpu.VMEM((2, width, NB_A), BF16),
            pltpu.VMEM((2, width, NB_A), BF16),
            pltpu.SemaphoreType.DMA((2, 2)),
            pltpu.VMEM((width, n_col), BF16),
            pltpu.VMEM((rows_t, n_col), F32),
            pltpu.VMEM((rows, LANES), F32),
            pltpu.VMEM((rows_t, LANES), F32),
            pltpu.VMEM((rows_t, width), F32),
            pltpu.VMEM((3, 1, rows + rows_t), F32),
            pltpu.VMEM((3, n_dev, 1, rows + rows_t), F32),
            pltpu.SemaphoreType.DMA((3, n_dev)),
            pltpu.SemaphoreType.DMA((3, n_dev)),
            pltpu.SemaphoreType.DMA((n_dp,)),
            pltpu.SemaphoreType.DMA((n_dp,)),
        ],
        compiler_params=pltpu.CompilerParams(
            collective_id=1, has_side_effects=True, vmem_limit_bytes=60 << 20),
        cost_estimate=pl.CostEstimate(flops=flops, bytes_accessed=4 * width * n_col, transcendentals=rows * n_col),
        name="sinkhorn_stats",
    )(z_s, z_t, protos, ema_protos)


def grads_kernel(zs_ref, zst_ref, zt_ref, rs_ref, r_ref, c_ref, v_hbm, vt_hbm, g_hbm,
                 vbuf, tbuf, obuf, in_sem, loc_sem, out_sem, recv_sem):
    vp, dp = my_place()
    chip, core = dp // 2, dp % 2
    partner = chip * 2 + 1 - core
    rows, rows_t = zs_ref.shape[0], zt_ref.shape[0]
    n_img = rows // ALL_CROPS
    half = v_hbm.shape[1] // 2
    n_slice = c_ref.shape[2]
    n_blk = half // NB_B
    base = core * half
    barrier = pltpu.get_barrier_semaphore()
    pl.semaphore_signal(barrier, inc=1, device_id=(vp, partner), device_id_type=MESH)

    def load(j, slot):
        cols = pl.ds(pl.multiple_of(base + j * NB_B, NB_B), NB_B)
        return (pltpu.make_async_copy(v_hbm.at[:, cols], vbuf.at[slot], in_sem.at[0, slot]),
                pltpu.make_async_copy(vt_hbm.at[:, cols], tbuf.at[slot], in_sem.at[1, slot]))

    def store(j):
        slot = j % OUT_SLOTS
        cols = pl.ds(pl.multiple_of(base + j * NB_B, NB_B), NB_B)
        return (pltpu.make_async_copy(obuf.at[slot], g_hbm.at[:, cols], loc_sem.at[slot]),
                pltpu.make_async_remote_copy(
                    src_ref=obuf.at[slot], dst_ref=g_hbm.at[:, cols], send_sem=out_sem.at[slot],
                    recv_sem=recv_sem.at[j], device_id=(vp, partner), device_id_type=MESH))

    def finish(j):
        local, remote = store(j)
        local.wait()
        remote.wait_send()

    for copy in load(0, 0):
        copy.start()
    scale = 1.0 / (n_img * GLOBAL_CROPS * (ALL_CROPS - 1)) / TEMP_STUDENT
    lanes = lax.broadcasted_iota(jnp.int32, (1, rows), 1)
    weight = jnp.where(lanes < GLOBAL_CROPS * n_img, scale, GLOBAL_CROPS * scale)
    bias = to_column(jnp.log(weight / rs_ref[...]) * LOG2E)
    bias = jnp.concatenate([bias] * (NB_B // LANES), axis=1)
    r_col = to_column(r_ref[...] * scale)
    r_wide = jnp.concatenate([r_col] * (NB_B // LANES), axis=1)
    pl.semaphore_wait(barrier, 1)

    @pl.loop(0, n_blk)
    def _(j):
        slot = j % 2

        @pl.when(j + 1 < n_blk)
        def _():
            for copy in load(j + 1, 1 - slot):
                copy.start()

        @pl.when(j >= 1)
        def _():
            for copy in store(j - 1):
                copy.start()

        @pl.when(j >= OUT_SLOTS)
        def _():
            finish(j - OUT_SLOTS)

        for copy in load(j, slot):
            copy.wait()
        unit_t = unit_columns(tbuf[slot])[0].astype(BF16)
        col = base + j * NB_B
        c_row = c_ref[col // n_slice, :, pl.ds(pl.multiple_of(col % n_slice, NB_B), NB_B)]
        q_mat = jnp.exp2(dot(zt_ref[...], unit_t) * (LOG2E / TEMP_TEACHER)) * c_row * r_wide
        q_zero, q_one = q_mat[:n_img], q_mat[n_img:]
        q_both = q_zero + q_one
        unit, inv_col = unit_columns(vbuf[slot])
        logits = dot(zs_ref[...], unit.astype(BF16))
        soft = jnp.exp2(logits * (LOG2E / TEMP_STUDENT) + bias)
        target = jnp.concatenate([q_one, q_zero] + [q_both] * (ALL_CROPS - GLOBAL_CROPS), axis=0)
        g_unit = dot(zst_ref[...], (soft - target).astype(BF16))
        obuf[j % OUT_SLOTS] = (g_unit - unit * jnp.sum(unit * g_unit, axis=0, keepdims=True)) * inv_col

    for copy in store(n_blk - 1):
        copy.start()
    for j in range(n_blk - OUT_SLOTS, n_blk):
        finish(j)

    @pl.loop(0, n_blk)
    def _(j):
        store(j)[1].wait_recv()


def proto_grads(z_s, z_t, row_sum, r_row, c_all, protos, ema_protos):
    rows, width = z_s.shape
    rows_t = z_t.shape[0]
    n_col = protos.shape[1]
    n_blk = n_col // 2 // NB_B
    return pl.pallas_call(
        grads_kernel,
        out_shape=jax.ShapeDtypeStruct((width, n_col), F32),
        in_specs=[VMEM] * 6 + [HBM] * 2,
        out_specs=HBM,
        scratch_shapes=[
            pltpu.VMEM((2, width, NB_B), BF16),
            pltpu.VMEM((2, width, NB_B), BF16),
            pltpu.VMEM((OUT_SLOTS, width, NB_B), F32),
            pltpu.SemaphoreType.DMA((2, 2)),
            pltpu.SemaphoreType.DMA((OUT_SLOTS,)),
            pltpu.SemaphoreType.DMA((OUT_SLOTS,)),
            pltpu.SemaphoreType.DMA((n_blk,)),
        ],
        compiler_params=pltpu.CompilerParams(
            collective_id=2, has_side_effects=True, vmem_limit_bytes=60 << 20),
        cost_estimate=pl.CostEstimate(
            flops=2 * rows * n_col * width, bytes_accessed=4 * width * n_col, transcendentals=rows * n_col // 2),
        name="proto_grads",
    )(z_s, z_s.T, z_t, row_sum, r_row, c_all, protos, ema_protos)


def solution(mesh):
    n_vp = mesh.shape['vp']
    n_dp = mesh.shape['dp']

    def local_step(student_x, teacher_x, w_in, b_in, w_mid, b_mid, w_out, b_out, protos,
                   ema_w_in, ema_b_in, ema_w_mid, ema_b_mid, ema_w_out, ema_b_out, ema_protos):
        rows, feat = student_x.shape
        n_img = rows // ALL_CROPS
        width = protos.shape[0]
        total_img = n_img * n_dp
        t_emb = mlp_forward(teacher_x, ema_w_in, ema_b_in, ema_w_mid, ema_b_mid, ema_w_out, ema_b_out)[0]
        s_emb = mlp_forward(student_x, w_in, b_in, w_mid, b_mid, w_out, b_out)[0]
        z_all = gather_dp(jnp.concatenate([s_emb, t_emb], axis=0), n_dp, 0)
        z_s = z_all[:, :rows].reshape(total_img, ALL_CROPS, width).transpose(1, 0, 2).reshape(-1, width).astype(BF16)
        z_t = z_all[:, rows:].reshape(total_img, GLOBAL_CROPS, width).transpose(1, 0, 2).reshape(-1, width).astype(BF16)
        c_all, row_sum, r_row, g_emb, loss = sinkhorn_stats(z_s, z_t, protos, ema_protos, n_vp, n_dp)
        g_protos = proto_grads(z_s, z_t, row_sum, r_row, c_all, protos, ema_protos)
        g_emb, loss = lax.psum((g_emb, loss), ('vp', 'dp'))
        x_all = gather_dp(student_x.astype(F32), n_dp, 3).reshape(n_dp * rows, feat).astype(BF16)
        g_emb = g_emb.reshape(ALL_CROPS, total_img, width).transpose(1, 0, 2).reshape(-1, width)
        saved = mlp_forward(x_all, w_in, b_in, w_mid, b_mid, w_out, b_out)[1]
        head_grads = mlp_backward(g_emb, x_all, saved, w_mid, w_out)
        return (jnp.sum(loss),) + tuple(head_grads) + (g_protos,)

    by_rows = P('dp', None)
    by_cols = P(None, 'vp')
    replicated = P()
    head_specs = (replicated,) * 6
    in_specs = (by_rows, by_rows) + head_specs + (by_cols,) + head_specs + (by_cols,)
    out_specs = (replicated,) * 7 + (by_cols,)
    return jax.shard_map(local_step, mesh=mesh, in_specs=in_specs, out_specs=out_specs, check_vma=False)
```

```python
import functools

import jax
import jax.numpy as jnp
from jax import lax
from jax.experimental import pallas as pl
from jax.experimental.pallas import tpu as pltpu
from jax.sharding import PartitionSpec as P

ALL_CROPS = 10
GLOBAL_CROPS = 2
TEMP_STUDENT = 0.1
TEMP_TEACHER = 0.04
LOG2E = 1.4426950408889634
LANES = 128
NB_A = 512
NB_B = 512
OUT_SLOTS = 4
F32 = jnp.float32
BF16 = jnp.bfloat16
MESH = pl.DeviceIdType.MESH
HBM = pl.BlockSpec(memory_space=pl.ANY)
VMEM = pl.BlockSpec(memory_space=pltpu.VMEM)


def mlp_forward(feats, w_in, b_in, w_mid, b_mid, w_out, b_out):
    pre_one = jnp.dot(feats, w_in, preferred_element_type=F32) + b_in.astype(F32)
    hid_one = jax.nn.gelu(pre_one, approximate=False).astype(BF16)
    pre_two = jnp.dot(hid_one, w_mid, preferred_element_type=F32) + b_mid.astype(F32)
    hid_two = jax.nn.gelu(pre_two, approximate=False).astype(BF16)
    proj = jnp.dot(hid_two, w_out, preferred_element_type=F32) + b_out.astype(F32)
    inv_norm = lax.rsqrt(jnp.sum(proj * proj, axis=-1, keepdims=True))
    unit = proj * inv_norm
    return unit, (pre_one, hid_one, pre_two, hid_two, unit, inv_norm)


def mlp_backward(g_emb, feats, saved, w_mid, w_out):
    slope_one, hid_one, slope_two, hid_two, unit, inv_norm = saved
    g_proj = (g_emb - unit * jnp.sum(unit * g_emb, axis=-1, keepdims=True)) * inv_norm
    g_proj_lo = g_proj.astype(BF16)
    g_w_out = jnp.einsum('nh,nb->hb', hid_two, g_proj_lo, preferred_element_type=F32)
    g_hid_two = jnp.einsum('nb,hb->nh', g_proj_lo, w_out, preferred_element_type=F32)
    g_pre_two = g_hid_two.astype(BF16).astype(F32) * slope_two
    g_pre_two_lo = g_pre_two.astype(BF16)
    g_w_mid = jnp.einsum('ng,nh->gh', hid_one, g_pre_two_lo, preferred_element_type=F32)
    g_hid_one = jnp.einsum('nh,gh->ng', g_pre_two_lo, w_mid, preferred_element_type=F32)
    g_pre_one = g_hid_one.astype(BF16).astype(F32) * slope_one
    g_w_in = jnp.einsum('nf,nh->fh', feats, g_pre_one.astype(BF16), preferred_element_type=F32)
    return (g_w_in, jnp.sum(g_pre_one, axis=0), g_w_mid, jnp.sum(g_pre_two, axis=0), g_w_out, jnp.sum(g_proj, axis=0))


def unit_columns(block):
    block_f = block.astype(F32)
    inv_col = lax.rsqrt(jnp.sum(block_f * block_f, axis=0, keepdims=True))
    return block_f * inv_col, inv_col


def dot(left, right):
    return jnp.dot(left, right, preferred_element_type=F32)


def dot_t(left, right):
    return lax.dot_general(left, right, (((1,), (1,)), ((), ())), preferred_element_type=F32)


def to_column(row):
    return jnp.transpose(jnp.broadcast_to(row, (LANES, row.shape[1])))


def to_row(acc):
    return jnp.sum(jnp.transpose(acc), axis=0, keepdims=True)


def fold_lanes(wide):
    total = wide[:, :LANES]
    for start in range(LANES, wide.shape[1], LANES):
        total = total + wide[:, start:start + LANES]
    return total


def my_place():
    return lax.axis_index('vp'), lax.axis_index('dp')


def gather_kernel(n_dp, block_ref, all_ref, out_sem, in_sem, fwd_out, fwd_in):
    vp, me = my_place()
    n_chip = n_dp // 2
    chip, core = me // 2, me % 2
    partner = chip * 2 + 1 - core
    n_row = block_ref.shape[1]

    def part(slot):
        return all_ref.at[:, pl.ds(pl.multiple_of(slot * n_row, n_row), n_row)]

    barrier = pltpu.get_barrier_semaphore()
    pl.semaphore_signal(barrier, inc=1, device_id=(vp, partner), device_id_type=MESH)
    for k in range(1, n_chip):
        peer = ((chip + k) % n_chip) * 2 + core
        pl.semaphore_signal(barrier, inc=1, device_id=(vp, peer), device_id_type=MESH)
    pl.semaphore_wait(barrier, n_chip)
    sends = []
    for k in range(1, n_chip):
        peer = ((chip + k) % n_chip) * 2 + core
        sends.append(pltpu.make_async_remote_copy(
            src_ref=block_ref, dst_ref=part(me), send_sem=out_sem.at[k], recv_sem=in_sem.at[chip],
            device_id=(vp, peer), device_id_type=MESH))
    own = pltpu.make_async_remote_copy(
        src_ref=block_ref, dst_ref=part(me), send_sem=fwd_out.at[chip], recv_sem=fwd_in.at[chip],
        device_id=(vp, partner), device_id_type=MESH)
    for copy in sends:
        copy.start()
    own.start()
    all_ref[:, pl.ds(pl.multiple_of(me * n_row, n_row), n_row)] = block_ref[...]
    for k in range(1, n_chip):
        src = (chip + n_chip - k) % n_chip
        slot = src * 2 + core
        peer_copy = pltpu.make_async_remote_copy(
            src_ref=block_ref, dst_ref=part(slot), send_sem=out_sem.at[k], recv_sem=in_sem.at[src],
            device_id=(vp, partner), device_id_type=MESH)
        peer_copy.wait_recv()
        forward = pltpu.make_async_remote_copy(
            src_ref=part(slot), dst_ref=part(slot), send_sem=fwd_out.at[src], recv_sem=fwd_in.at[src],
            device_id=(vp, partner), device_id_type=MESH)
        forward.start()
    for copy in sends:
        copy.wait_send()
    for src in range(n_chip):
        slot = src * 2 + core
        other = src * 2 + 1 - core
        pltpu.make_async_remote_copy(
            src_ref=part(slot), dst_ref=part(other), send_sem=fwd_out.at[src], recv_sem=fwd_in.at[src],
            device_id=(vp, partner), device_id_type=MESH).wait()


def gather_dp(block, n_dp, collective_id):
    groups, n_row, width = block.shape
    return pl.pallas_call(
        functools.partial(gather_kernel, n_dp),
        out_shape=jax.ShapeDtypeStruct((groups, n_row * n_dp, width), block.dtype),
        in_specs=[VMEM],
        out_specs=VMEM,
        scratch_shapes=[pltpu.SemaphoreType.DMA((n_dp // 2,))] * 4,
        compiler_params=pltpu.CompilerParams(
            collective_id=collective_id, has_side_effects=True, vmem_limit_bytes=48 << 20),
        name="gather_dp",
    )(block)


def stats_kernel(n_vp, n_dp, zs_ref, zt_ref, v_hbm, vt_hbm, c_ref, rs_ref, r_ref, ge_ref, loss_ref,
                 vbuf, tbuf, in_sem, ubuf, kbuf, acc_s, acc_r, wbuf, snd, rcv, send_sem, recv_sem, c_out, c_in):
    vp, dp = my_place()
    n_dev = n_vp * n_dp
    me = vp * n_dp + dp
    rows, rows_t = zs_ref.shape[0], zt_ref.shape[0]
    n_img = rows // ALL_CROPS
    n_col = kbuf.shape[1]
    n_blk = n_col // NB_A
    base = dp * n_col

    barrier = pltpu.get_barrier_semaphore()
    for k in range(1, n_dev):
        peer = (me + k) % n_dev
        pl.semaphore_signal(barrier, inc=1, device_id=(peer // n_dp, peer % n_dp), device_id_type=MESH)

    def load(j, slot):
        cols = pl.ds(pl.multiple_of(base + j * NB_A, NB_A), NB_A)
        return (pltpu.make_async_copy(v_hbm.at[:, cols], vbuf.at[slot], in_sem.at[0, slot]),
                pltpu.make_async_copy(vt_hbm.at[:, cols], tbuf.at[slot], in_sem.at[1, slot]))

    for copy in load(0, 0):
        copy.start()
    acc_s[...] = jnp.zeros_like(acc_s)
    acc_r[...] = jnp.zeros_like(acc_r)
    ge_ref[...] = jnp.zeros_like(ge_ref)

    @pl.loop(0, n_blk)
    def _(j):
        slot = j % 2

        @pl.when(j + 1 < n_blk)
        def _():
            for copy in load(j + 1, 1 - slot):
                copy.start()

        for copy in load(j, slot):
            copy.wait()
        here = pl.ds(pl.multiple_of(j * NB_A, NB_A), NB_A)
        unit_t = unit_columns(tbuf[slot])[0].astype(BF16)
        kern = jnp.exp2(dot(zt_ref[...], unit_t) * (LOG2E / TEMP_TEACHER))
        kbuf[:, here] = kern
        acc_r[...] += fold_lanes(kern * (1.0 / jnp.sum(kern, axis=0, keepdims=True)))
        unit = unit_columns(vbuf[slot])[0].astype(BF16)
        ubuf[:, here] = unit
        exp_s = jnp.exp2(dot(zs_ref[...], unit) * (LOG2E / TEMP_STUDENT))
        acc_s[...] += fold_lanes(exp_s)
        ge_ref[...] += dot_t(exp_s.astype(BF16), unit)

    pl.semaphore_wait(barrier, n_dev - 1)

    def exchange(step, width):
        def copy(k, dst, peer):
            return pltpu.make_async_remote_copy(
                src_ref=snd.at[step, :, :width], dst_ref=rcv.at[step, dst, :, :width],
                send_sem=send_sem.at[step, k], recv_sem=recv_sem.at[step, dst],
                device_id=(peer // n_dp, peer % n_dp), device_id_type=MESH)
        for k in range(1, n_dev):
            copy(k, me, (me + k) % n_dev).start()
        rcv[step, me, :, :width] = snd[step, :, :width]
        for k in range(1, n_dev):
            src = (me + n_dev - k) % n_dev
            copy(k, src, src).wait()
        total = rcv[step, 0, :, :width]
        for k in range(1, n_dev):
            total = total + rcv[step, k, :, :width]
        return total

    snd[0, :, :rows_t] = to_row(acc_r[...])
    snd[0, :, rows_t:rows_t + rows] = to_row(acc_s[...])
    total = exchange(0, rows_t + rows)
    row_sum = total[:, rows_t:]
    rs_ref[...] = row_sum
    r_row = 1.0 / total[:, :rows_t]

    for step in (1, 2):
        r_col = to_column(r_row)
        acc_r[...] = jnp.zeros_like(acc_r)

        @pl.loop(0, n_col // LANES)
        def _(j):
            here = pl.ds(pl.multiple_of(j * LANES, LANES), LANES)
            kern = kbuf[:, here]
            c_row = 1.0 / jnp.sum(kern * r_col, axis=0, keepdims=True)
            acc_r[...] += kern * c_row
            if step == 2:
                c_ref[dp, :, here] = c_row

        if step == 2:
            for k in range(1, n_dp):
                pltpu.make_async_remote_copy(
                    src_ref=c_ref.at[dp], dst_ref=c_ref.at[dp], send_sem=c_out.at[k], recv_sem=c_in.at[dp],
                    device_id=(vp, (dp + k) % n_dp), device_id_type=MESH).start()
        snd[step, :, :rows_t] = to_row(acc_r[...])
        r_row = 1.0 / exchange(step, rows_t)
    r_ref[...] = r_row

    r_col = to_column(r_row)
    r_wide = jnp.concatenate([r_col] * (NB_A // LANES), axis=1)
    wbuf[...] = jnp.zeros_like(wbuf)

    @pl.loop(0, n_blk)
    def _(j):
        here = pl.ds(pl.multiple_of(j * NB_A, NB_A), NB_A)
        q_mat = kbuf[:, here] * c_ref[dp, :, here] * r_wide
        q_hi = q_mat.astype(BF16)
        q_lo = (q_mat - q_hi.astype(F32)).astype(BF16)
        unit = ubuf[:, here]
        wbuf[...] += dot_t(q_hi, unit) + dot_t(q_lo, unit)

    w_zero = wbuf[:n_img]
    w_one = wbuf[n_img:]
    w_both = w_zero + w_one
    scale = 1.0 / (n_img * GLOBAL_CROPS * (ALL_CROPS - 1))
    log_rs = jnp.log(row_sum)
    inv_rs = to_column(1.0 / row_sum)
    loss = jnp.zeros((1, LANES), F32)
    for v in range(ALL_CROPS):
        block = pl.ds(v * n_img, n_img)
        count = float(GLOBAL_CROPS - (v < GLOBAL_CROPS))
        w_v = (w_one, w_zero)[v] if v < GLOBAL_CROPS else w_both
        inv = inv_rs[v * n_img:(v + 1) * n_img]
        inv = jnp.concatenate([inv] * (ge_ref.shape[1] // LANES), axis=1)
        dots = fold_lanes(jnp.sum(zs_ref[block].astype(F32) * w_v, axis=0, keepdims=True))
        logs = log_rs[:, v * n_img:(v + 1) * n_img]
        loss += (count / n_dev) * logs - (1.0 / TEMP_STUDENT) * dots
        ge_ref[block] = (count * (ge_ref[block] * inv) - w_v) * (scale / TEMP_STUDENT)
    loss_ref[...] = loss * scale

    for k in range(1, n_dp):
        src = (dp + n_dp - k) % n_dp
        pltpu.make_async_remote_copy(
            src_ref=c_ref.at[dp], dst_ref=c_ref.at[src], send_sem=c_out.at[k], recv_sem=c_in.at[src],
            device_id=(vp, src), device_id_type=MESH).wait()


def sinkhorn_stats(z_s, z_t, protos, ema_protos, n_vp, n_dp):
    rows, width = z_s.shape
    rows_t = z_t.shape[0]
    n_col = protos.shape[1] // n_dp
    n_dev = n_vp * n_dp
    flops = 2 * rows * n_col * width * 2
    return pl.pallas_call(
        functools.partial(stats_kernel, n_vp, n_dp),
        out_shape=(jax.ShapeDtypeStruct((n_dp, 1, n_col), F32),
                   jax.ShapeDtypeStruct((1, rows), F32),
                   jax.ShapeDtypeStruct((1, rows_t), F32),
                   jax.ShapeDtypeStruct((rows, width), F32),
                   jax.ShapeDtypeStruct((1, LANES), F32)),
        in_specs=[VMEM, VMEM, HBM, HBM],
        out_specs=(VMEM,) * 5,
        scratch_shapes=[
            pltpu.VMEM((2, width, NB_A), BF16),
            pltpu.VMEM((2, width, NB_A), BF16),
            pltpu.SemaphoreType.DMA((2, 2)),
            pltpu.VMEM((width, n_col), BF16),
            pltpu.VMEM((rows_t, n_col), F32),
            pltpu.VMEM((rows, LANES), F32),
            pltpu.VMEM((rows_t, LANES), F32),
            pltpu.VMEM((rows_t, width), F32),
            pltpu.VMEM((3, 1, rows + rows_t), F32),
            pltpu.VMEM((3, n_dev, 1, rows + rows_t), F32),
            pltpu.SemaphoreType.DMA((3, n_dev)),
            pltpu.SemaphoreType.DMA((3, n_dev)),
            pltpu.SemaphoreType.DMA((n_dp,)),
            pltpu.SemaphoreType.DMA((n_dp,)),
        ],
        compiler_params=pltpu.CompilerParams(
            collective_id=1, has_side_effects=True, vmem_limit_bytes=60 << 20),
        cost_estimate=pl.CostEstimate(flops=flops, bytes_accessed=4 * width * n_col, transcendentals=rows * n_col),
        name="sinkhorn_stats",
    )(z_s, z_t, protos, ema_protos)


def grads_kernel(n_vp, n_dp, zs_ref, zst_ref, zt_ref, rs_ref, r_ref, c_ref, ge_ref, loss_ref, x_ref, v_hbm, vt_hbm,
                 g_hbm, ge_all, loss_all, x_all, vbuf, tbuf, obuf, part_ge, sum_ge, part_loss, in_sem, loc_sem, out_sem,
                 recv_sem, rs_out, rs_in, ag_out, ag_in, ls_out, ls_in, x_out, x_in, xf_out, xf_in, x_own):
    vp, dp = my_place()
    n_dev = n_vp * n_dp
    me = vp * n_dp + dp
    n_chip = n_dp // 2
    chip, core = dp // 2, dp % 2
    partner = chip * 2 + 1 - core
    rows, rows_t = zs_ref.shape[0], zt_ref.shape[0]
    n_img = rows // ALL_CROPS
    n_own = rows // n_dev
    n_loc = x_ref.shape[1]
    half = v_hbm.shape[1] // 2
    n_slice = c_ref.shape[2]
    n_blk = half // NB_B
    base = core * half
    barrier = pltpu.get_barrier_semaphore()
    for k in range(1, n_dev):
        peer = (me + k) % n_dev
        pl.semaphore_signal(barrier, inc=1, device_id=(peer // n_dp, peer % n_dp), device_id_type=MESH)

    def load(j, slot):
        cols = pl.ds(pl.multiple_of(base + j * NB_B, NB_B), NB_B)
        return (pltpu.make_async_copy(v_hbm.at[:, cols], vbuf.at[slot], in_sem.at[0, slot]),
                pltpu.make_async_copy(vt_hbm.at[:, cols], tbuf.at[slot], in_sem.at[1, slot]))

    def local_store(j):
        slot = j % OUT_SLOTS
        cols = pl.ds(pl.multiple_of(base + j * NB_B, NB_B), NB_B)
        return pltpu.make_async_copy(obuf.at[slot], g_hbm.at[:, cols], loc_sem.at[slot])

    def remote_store(j):
        slot = j % OUT_SLOTS
        cols = pl.ds(pl.multiple_of(base + j * NB_B, NB_B), NB_B)
        return pltpu.make_async_remote_copy(
            src_ref=obuf.at[slot], dst_ref=g_hbm.at[:, cols], send_sem=out_sem.at[slot],
            recv_sem=recv_sem.at[j], device_id=(vp, partner), device_id_type=MESH)

    def peer_of(k):
        peer = (me + k) % n_dev
        return peer, (peer // n_dp, peer % n_dp)

    def scatter(k, peer, dst, device):
        return pltpu.make_async_remote_copy(
            src_ref=ge_ref.at[pl.ds(pl.multiple_of(peer * n_own, n_own), n_own)], dst_ref=part_ge.at[dst],
            send_sem=rs_out.at[k], recv_sem=rs_in.at[dst], device_id=device, device_id_type=MESH)

    def spread(k, owner, device):
        return pltpu.make_async_remote_copy(
            src_ref=sum_ge, dst_ref=ge_all.at[pl.ds(pl.multiple_of(owner * n_own, n_own), n_own)],
            send_sem=ag_out.at[k], recv_sem=ag_in.at[owner], device_id=device, device_id_type=MESH)

    def loss_send(k, dst, device):
        return pltpu.make_async_remote_copy(
            src_ref=loss_ref, dst_ref=part_loss.at[dst], send_sem=ls_out.at[k], recv_sem=ls_in.at[dst],
            device_id=device, device_id_type=MESH)

    def x_part(slot):
        return x_all.at[:, pl.ds(pl.multiple_of(slot * n_loc, n_loc), n_loc)]

    def x_send(k, src_chip, slot, device):
        return pltpu.make_async_remote_copy(
            src_ref=x_ref, dst_ref=x_part(slot), send_sem=x_out.at[k], recv_sem=x_in.at[src_chip],
            device_id=device, device_id_type=MESH)

    def x_forward(src_chip, slot):
        return pltpu.make_async_remote_copy(
            src_ref=x_part(slot), dst_ref=x_part(slot), send_sem=xf_out.at[src_chip], recv_sem=xf_in.at[src_chip],
            device_id=(vp, partner), device_id_type=MESH)

    for copy in load(0, 0):
        copy.start()
    x_local = pltpu.make_async_copy(x_ref, x_part(dp), x_own.at[0])
    x_local.start()
    scale = 1.0 / (n_img * GLOBAL_CROPS * (ALL_CROPS - 1)) / TEMP_STUDENT
    lanes = lax.broadcasted_iota(jnp.int32, (1, rows), 1)
    weight = jnp.where(lanes < GLOBAL_CROPS * n_img, scale, GLOBAL_CROPS * scale)
    bias = to_column(jnp.log(weight / rs_ref[...]) * LOG2E)
    bias = jnp.concatenate([bias] * (NB_B // LANES), axis=1)
    r_col = to_column(r_ref[...] * scale)
    r_wide = jnp.concatenate([r_col] * (NB_B // LANES), axis=1)
    pl.semaphore_wait(barrier, n_dev - 1)
    for k in range(1, n_dev):
        peer, device = peer_of(k)
        loss_send(k, me, device).start()
        scatter(k, peer, me, device).start()
    for k in range(1, n_chip):
        x_send(k, chip, dp, (vp, ((chip + k) % n_chip) * 2 + core)).start()
    part_ge[me] = ge_ref[pl.ds(pl.multiple_of(me * n_own, n_own), n_own)]
    part_loss[me] = loss_ref[...]

    @pl.loop(0, n_blk)
    def _(j):
        slot = j % 2

        @pl.when(j + 1 < n_blk)
        def _():
            for copy in load(j + 1, 1 - slot):
                copy.start()

        @pl.when(j >= 1)
        def _():
            local_store(j - 1).start()
            remote_store(j - 1).start()

        @pl.when(j >= OUT_SLOTS)
        def _():
            local_store(j - OUT_SLOTS).wait()
            remote_store(j - OUT_SLOTS).wait_send()

        @pl.when(j == n_blk // 2)
        def _():
            for k in range(1, n_dev):
                src = (me + n_dev - k) % n_dev
                scatter(k, src, src, (vp, partner)).wait()
                loss_send(k, src, (vp, partner)).wait()
            total = part_ge[0]
            loss = part_loss[0]
            for k in range(1, n_dev):
                total = total + part_ge[k]
                loss = loss + part_loss[k]
            loss_all[...] = loss
            sum_ge[...] = total
            ge_all[pl.ds(pl.multiple_of(me * n_own, n_own), n_own)] = total

        @pl.when(j == n_blk // 2 + 1)
        def _():
            for k in range(1, n_dev):
                spread(k, me, peer_of(k)[1]).start()

        @pl.when(j == n_blk - 4)
        def _():
            x_local.wait()
            x_forward(chip, dp).start()
            for k in range(1, n_chip):
                src = (chip + n_chip - k) % n_chip
                x_send(k, src, src * 2 + core, (vp, partner)).wait()
                x_forward(src, src * 2 + core).start()

        for copy in load(j, slot):
            copy.wait()
        unit_t = unit_columns(tbuf[slot])[0].astype(BF16)
        col = base + j * NB_B
        c_row = c_ref[col // n_slice, :, pl.ds(pl.multiple_of(col % n_slice, NB_B), NB_B)]
        q_mat = jnp.exp2(dot(zt_ref[...], unit_t) * (LOG2E / TEMP_TEACHER)) * c_row * r_wide
        q_zero, q_one = q_mat[:n_img], q_mat[n_img:]
        q_both = q_zero + q_one
        unit, inv_col = unit_columns(vbuf[slot])
        logits = dot(zs_ref[...], unit.astype(BF16))
        soft = jnp.exp2(logits * (LOG2E / TEMP_STUDENT) + bias)
        target = jnp.concatenate([q_one, q_zero] + [q_both] * (ALL_CROPS - GLOBAL_CROPS), axis=0)
        g_unit = dot(zst_ref[...], (soft - target).astype(BF16))
        obuf[j % OUT_SLOTS] = (g_unit - unit * jnp.sum(unit * g_unit, axis=0, keepdims=True)) * inv_col

    local_store(n_blk - 1).start()
    remote_store(n_blk - 1).start()
    for j in range(n_blk - OUT_SLOTS, n_blk):
        local_store(j).wait()
        remote_store(j).wait_send()
    for k in range(1, n_dev):
        src = (me + n_dev - k) % n_dev
        spread(k, src, (vp, partner)).wait()
    for src in range(n_chip):
        pltpu.make_async_remote_copy(
            src_ref=x_part(src * 2 + core), dst_ref=x_part(src * 2 + 1 - core), send_sem=xf_out.at[src],
            recv_sem=xf_in.at[src], device_id=(vp, partner), device_id_type=MESH).wait()

    @pl.loop(0, n_blk)
    def _(j):
        remote_store(j).wait_recv()


def proto_grads(z_s, z_t, row_sum, r_row, c_all, g_emb, loss, x_loc, protos, ema_protos, n_vp, n_dp):
    rows, width = z_s.shape
    n_col = protos.shape[1]
    n_blk = n_col // 2 // NB_B
    n_dev = n_vp * n_dp
    dma = pltpu.SemaphoreType.DMA
    return pl.pallas_call(
        functools.partial(grads_kernel, n_vp, n_dp),
        out_shape=(jax.ShapeDtypeStruct((width, n_col), F32),
                   jax.ShapeDtypeStruct((rows, width), F32),
                   jax.ShapeDtypeStruct((1, LANES), F32),
                   jax.ShapeDtypeStruct((x_loc.shape[0], x_loc.shape[1] * n_dp, x_loc.shape[2]), F32)),
        in_specs=[VMEM] * 9 + [HBM] * 2,
        out_specs=(HBM, VMEM, VMEM, HBM),
        scratch_shapes=[
            pltpu.VMEM((2, width, NB_B), BF16),
            pltpu.VMEM((2, width, NB_B), BF16),
            pltpu.VMEM((OUT_SLOTS, width, NB_B), F32),
            pltpu.VMEM((n_dev, rows // n_dev, width), F32),
            pltpu.VMEM((rows // n_dev, width), F32),
            pltpu.VMEM((n_dev, 1, LANES), F32),
            dma((2, 2)),
            dma((OUT_SLOTS,)),
            dma((OUT_SLOTS,)),
            dma((n_blk,)),
        ] + [dma((n_dev,))] * 6 + [dma((n_dp // 2,))] * 4 + [dma((1,))],
        compiler_params=pltpu.CompilerParams(
            collective_id=2, has_side_effects=True, vmem_limit_bytes=60 << 20),
        cost_estimate=pl.CostEstimate(
            flops=2 * rows * n_col * width, bytes_accessed=4 * width * n_col, transcendentals=rows * n_col // 2),
        name="proto_grads",
    )(z_s, z_s.T, z_t, row_sum, r_row, c_all, g_emb, loss, x_loc, protos, ema_protos)


def dense_kernel(first, n_step, *refs):
    if first:
        x_ref, w_ref, b_ref, src, hid_ref, slope_ref, dst, cbuf, rd_sem, wr_sem = refs
    else:
        x_ref, w_ref, b_ref, src, _, hid_ref, slope_ref, dst, cbuf, rd_sem, wr_sem = refs
    i = pl.program_id(0)
    chunk = cbuf.shape[2]
    base = 0 if first else n_step * chunk

    def cols(step):
        return pl.ds(pl.multiple_of(base + step * chunk, chunk), chunk)

    def read(step):
        return pltpu.make_async_copy(src.at[:, cols(step)], cbuf.at[step % 2], rd_sem.at[step % 2])

    def write(step):
        return pltpu.make_async_copy(cbuf.at[step % 2], dst.at[:, cols(step)], wr_sem.at[step % 2])

    @pl.when(i >= 2)
    def _():
        write(i - 2).wait()

    read(i).start()
    pre = dot(x_ref[...], w_ref[...]) + b_ref[...].astype(F32)
    cdf = 0.5 * (1.0 + lax.erf(pre * 0.7071067811865476))
    hid_ref[...] = (pre * cdf).astype(BF16)
    slope_ref[...] = cdf + pre * jnp.exp(-0.5 * pre * pre) * 0.3989422804014327
    read(i).wait()
    write(i).start()

    @pl.when(i == n_step - 1)
    def _():
        write(i - 1).wait()
        write(i).wait()


def dense_gelu(feats, weight, bias, src, dst, block=256):
    rows, depth = feats.shape
    n_out = weight.shape[1]
    n_step = n_out // block
    first = dst is None
    chunk = src.shape[1] // 2 // n_step
    args = (feats, weight, bias.reshape(1, n_out), src) + (() if first else (dst,))
    return pl.pallas_call(
        functools.partial(dense_kernel, first, n_step),
        grid=(n_step,),
        out_shape=(jax.ShapeDtypeStruct((rows, n_out), BF16),
                   jax.ShapeDtypeStruct((rows, n_out), F32),
                   jax.ShapeDtypeStruct(src.shape, F32)),
        in_specs=[pl.BlockSpec((rows, depth), lambda i: (0, 0), pipeline_mode=pl.Buffered(1)),
                  pl.BlockSpec((depth, block), lambda i: (0, i)),
                  pl.BlockSpec((1, block), lambda i: (0, i)), HBM] + ([] if first else [HBM]),
        out_specs=(pl.BlockSpec((rows, block), lambda i: (0, i)),
                   pl.BlockSpec((rows, block), lambda i: (0, i)), HBM),
        scratch_shapes=[pltpu.VMEM((2, src.shape[0], chunk), F32),
                        pltpu.SemaphoreType.DMA((2,)), pltpu.SemaphoreType.DMA((2,))],
        input_output_aliases={} if first else {4: 2},
        compiler_params=pltpu.CompilerParams(
            dimension_semantics=("arbitrary",), vmem_limit_bytes=56 << 20),
        cost_estimate=pl.CostEstimate(
            flops=2 * rows * depth * n_out, bytes_accessed=4 * src.shape[0] * src.shape[1], transcendentals=rows * n_out),
        name="dense_gelu",
    )(*args)


def solution(mesh):
    n_vp = mesh.shape['vp']
    n_dp = mesh.shape['dp']

    def local_step(student_x, teacher_x, w_in, b_in, w_mid, b_mid, w_out, b_out, protos,
                   ema_w_in, ema_b_in, ema_w_mid, ema_b_mid, ema_w_out, ema_b_out, ema_protos):
        rows, feat = student_x.shape
        n_img = rows // ALL_CROPS
        width = protos.shape[0]
        x_loc = student_x.reshape(n_img, ALL_CROPS, feat).transpose(1, 0, 2)
        t_loc = teacher_x.reshape(n_img, GLOBAL_CROPS, feat).transpose(1, 0, 2).reshape(-1, feat)
        t_emb = mlp_forward(t_loc, ema_w_in, ema_b_in, ema_w_mid, ema_b_mid, ema_w_out, ema_b_out)[0]
        s_emb = mlp_forward(x_loc.reshape(rows, feat), w_in, b_in, w_mid, b_mid, w_out, b_out)[0]
        z_loc = jnp.concatenate([s_emb, t_emb], axis=0).reshape(ALL_CROPS + GLOBAL_CROPS, n_img, width)
        z_all = gather_dp(z_loc, n_dp, 0).reshape(-1, width).astype(BF16)
        z_s, z_t = z_all[:rows * n_dp], z_all[rows * n_dp:]
        c_all, row_sum, r_row, g_emb, loss = sinkhorn_stats(z_s, z_t, protos, ema_protos, n_vp, n_dp)
        g_temp, g_emb, loss, x_all = proto_grads(
            z_s, z_t, row_sum, r_row, c_all, g_emb, loss, x_loc.astype(F32), protos, ema_protos, n_vp, n_dp)
        x_all = x_all.reshape(rows * n_dp, feat).astype(BF16)
        hid_one, slope_one, g_protos = dense_gelu(x_all, w_in, b_in, g_temp, None)
        hid_two, slope_two, g_protos = dense_gelu(hid_one, w_mid, b_mid, g_temp, g_protos)
        proj = jnp.dot(hid_two, w_out, preferred_element_type=F32) + b_out.astype(F32)
        inv_norm = lax.rsqrt(jnp.sum(proj * proj, axis=-1, keepdims=True))
        saved = (slope_one, hid_one, slope_two, hid_two, proj * inv_norm, inv_norm)
        head_grads = mlp_backward(g_emb, x_all, saved, w_mid, w_out)
        return (jnp.sum(loss),) + tuple(head_grads) + (g_protos,)

    by_rows = P('dp', None)
    by_cols = P(None, 'vp')
    replicated = P()
    head_specs = (replicated,) * 6
    in_specs = (by_rows, by_rows) + head_specs + (by_cols,) + head_specs + (by_cols,)
    out_specs = (replicated,) * 7 + (by_cols,)
    return jax.shard_map(local_step, mesh=mesh, in_specs=in_specs, out_specs=out_specs, check_vma=False)
```

```python
import functools

import jax
import jax.numpy as jnp
from jax import lax
from jax.experimental import pallas as pl
from jax.experimental.pallas import tpu as pltpu
from jax.sharding import PartitionSpec as P

ALL_CROPS = 10
GLOBAL_CROPS = 2
TEMP_STUDENT = 0.1
TEMP_TEACHER = 0.04
LOG2E = 1.4426950408889634
LANES = 128
NB_A = 512
NB_B = 1024
OUT_SLOTS = 3
HB = 256
F32 = jnp.float32
BF16 = jnp.bfloat16
MESH = pl.DeviceIdType.MESH
HBM = pl.BlockSpec(memory_space=pl.ANY)
VMEM = pl.BlockSpec(memory_space=pltpu.VMEM)


def mlp_forward(feats, w_in, b_in, w_mid, b_mid, w_out, b_out):
    pre_one = jnp.dot(feats, w_in, preferred_element_type=F32) + b_in.astype(F32)
    hid_one = jax.nn.gelu(pre_one, approximate=False).astype(BF16)
    pre_two = jnp.dot(hid_one, w_mid, preferred_element_type=F32) + b_mid.astype(F32)
    hid_two = jax.nn.gelu(pre_two, approximate=False).astype(BF16)
    proj = jnp.dot(hid_two, w_out, preferred_element_type=F32) + b_out.astype(F32)
    inv_norm = lax.rsqrt(jnp.sum(proj * proj, axis=-1, keepdims=True))
    return proj * inv_norm


def unit_columns(block):
    block_f = block.astype(F32)
    inv_col = lax.rsqrt(jnp.sum(block_f * block_f, axis=0, keepdims=True))
    return block_f * inv_col, inv_col


def dot(left, right):
    return jnp.dot(left, right, preferred_element_type=F32)


def dot_t(left, right):
    return lax.dot_general(left, right, (((1,), (1,)), ((), ())), preferred_element_type=F32)


def to_column(row):
    return jnp.transpose(jnp.broadcast_to(row, (LANES, row.shape[1])))


def to_row(acc):
    return jnp.sum(jnp.transpose(acc), axis=0, keepdims=True)


def fold_lanes(wide):
    total = wide[:, :LANES]
    for start in range(LANES, wide.shape[1], LANES):
        total = total + wide[:, start:start + LANES]
    return total


def my_place():
    return lax.axis_index('vp'), lax.axis_index('dp')


def gather_kernel(n_dp, block_ref, all_ref, out_sem, in_sem, fwd_out, fwd_in):
    vp, me = my_place()
    n_chip = n_dp // 2
    chip, core = me // 2, me % 2
    partner = chip * 2 + 1 - core
    n_row = block_ref.shape[1]

    def part(slot):
        return all_ref.at[:, pl.ds(pl.multiple_of(slot * n_row, n_row), n_row)]

    barrier = pltpu.get_barrier_semaphore()
    pl.semaphore_signal(barrier, inc=1, device_id=(vp, partner), device_id_type=MESH)
    for k in range(1, n_chip):
        peer = ((chip + k) % n_chip) * 2 + core
        pl.semaphore_signal(barrier, inc=1, device_id=(vp, peer), device_id_type=MESH)
    pl.semaphore_wait(barrier, n_chip)
    sends = []
    for k in range(1, n_chip):
        peer = ((chip + k) % n_chip) * 2 + core
        sends.append(pltpu.make_async_remote_copy(
            src_ref=block_ref, dst_ref=part(me), send_sem=out_sem.at[k], recv_sem=in_sem.at[chip],
            device_id=(vp, peer), device_id_type=MESH))
    own = pltpu.make_async_remote_copy(
        src_ref=block_ref, dst_ref=part(me), send_sem=fwd_out.at[chip], recv_sem=fwd_in.at[chip],
        device_id=(vp, partner), device_id_type=MESH)
    for copy in sends:
        copy.start()
    own.start()
    all_ref[:, pl.ds(pl.multiple_of(me * n_row, n_row), n_row)] = block_ref[...]
    for k in range(1, n_chip):
        src = (chip + n_chip - k) % n_chip
        slot = src * 2 + core
        peer_copy = pltpu.make_async_remote_copy(
            src_ref=block_ref, dst_ref=part(slot), send_sem=out_sem.at[k], recv_sem=in_sem.at[src],
            device_id=(vp, partner), device_id_type=MESH)
        peer_copy.wait_recv()
        forward = pltpu.make_async_remote_copy(
            src_ref=part(slot), dst_ref=part(slot), send_sem=fwd_out.at[src], recv_sem=fwd_in.at[src],
            device_id=(vp, partner), device_id_type=MESH)
        forward.start()
    for copy in sends:
        copy.wait_send()
    for src in range(n_chip):
        slot = src * 2 + core
        other = src * 2 + 1 - core
        pltpu.make_async_remote_copy(
            src_ref=part(slot), dst_ref=part(other), send_sem=fwd_out.at[src], recv_sem=fwd_in.at[src],
            device_id=(vp, partner), device_id_type=MESH).wait()


def gather_dp(block, n_dp, collective_id):
    groups, n_row, width = block.shape
    return pl.pallas_call(
        functools.partial(gather_kernel, n_dp),
        out_shape=jax.ShapeDtypeStruct((groups, n_row * n_dp, width), block.dtype),
        in_specs=[VMEM],
        out_specs=VMEM,
        scratch_shapes=[pltpu.SemaphoreType.DMA((n_dp // 2,))] * 4,
        compiler_params=pltpu.CompilerParams(
            collective_id=collective_id, has_side_effects=True, vmem_limit_bytes=48 << 20),
        name="gather_dp",
    )(block)


def stats_kernel(n_vp, n_dp, zs_ref, zt_ref, v_hbm, vt_hbm, c_ref, rs_ref, r_ref, ge_ref, loss_ref,
                 vbuf, tbuf, in_sem, ubuf, kbuf, acc_s, acc_r, wbuf, snd, rcv, send_sem, recv_sem, c_out, c_in):
    vp, dp = my_place()
    n_dev = n_vp * n_dp
    me = vp * n_dp + dp
    rows, rows_t = zs_ref.shape[0], zt_ref.shape[0]
    n_img = rows // ALL_CROPS
    n_col = kbuf.shape[1]
    n_blk = n_col // NB_A
    base = dp * n_col

    barrier = pltpu.get_barrier_semaphore()
    for k in range(1, n_dev):
        peer = (me + k) % n_dev
        pl.semaphore_signal(barrier, inc=1, device_id=(peer // n_dp, peer % n_dp), device_id_type=MESH)

    def load(j, slot):
        cols = pl.ds(pl.multiple_of(base + j * NB_A, NB_A), NB_A)
        return (pltpu.make_async_copy(v_hbm.at[:, cols], vbuf.at[slot], in_sem.at[0, slot]),
                pltpu.make_async_copy(vt_hbm.at[:, cols], tbuf.at[slot], in_sem.at[1, slot]))

    for copy in load(0, 0):
        copy.start()
    acc_s[...] = jnp.zeros_like(acc_s)
    acc_r[...] = jnp.zeros_like(acc_r)
    ge_ref[...] = jnp.zeros_like(ge_ref)

    @pl.loop(0, n_blk)
    def _(j):
        slot = j % 2

        @pl.when(j + 1 < n_blk)
        def _():
            for copy in load(j + 1, 1 - slot):
                copy.start()

        for copy in load(j, slot):
            copy.wait()
        here = pl.ds(pl.multiple_of(j * NB_A, NB_A), NB_A)
        unit_t = unit_columns(tbuf[slot])[0].astype(BF16)
        kern = jnp.exp2(dot(zt_ref[...], unit_t) * (LOG2E / TEMP_TEACHER))
        kbuf[:, here] = kern
        acc_r[...] += fold_lanes(kern * (1.0 / jnp.sum(kern, axis=0, keepdims=True)))
        unit = unit_columns(vbuf[slot])[0].astype(BF16)
        ubuf[:, here] = unit
        exp_s = jnp.exp2(dot(zs_ref[...], unit) * (LOG2E / TEMP_STUDENT))
        acc_s[...] += fold_lanes(exp_s)
        ge_ref[...] += dot_t(exp_s.astype(BF16), unit)

    pl.semaphore_wait(barrier, n_dev - 1)

    def exchange(step, width):
        def copy(k, dst, peer):
            return pltpu.make_async_remote_copy(
                src_ref=snd.at[step, :, :width], dst_ref=rcv.at[step, dst, :, :width],
                send_sem=send_sem.at[step, k], recv_sem=recv_sem.at[step, dst],
                device_id=(peer // n_dp, peer % n_dp), device_id_type=MESH)
        for k in range(1, n_dev):
            copy(k, me, (me + k) % n_dev).start()
        rcv[step, me, :, :width] = snd[step, :, :width]
        for k in range(1, n_dev):
            src = (me + n_dev - k) % n_dev
            copy(k, src, src).wait()
        total = rcv[step, 0, :, :width]
        for k in range(1, n_dev):
            total = total + rcv[step, k, :, :width]
        return total

    snd[0, :, :rows_t] = to_row(acc_r[...])
    snd[0, :, rows_t:rows_t + rows] = to_row(acc_s[...])
    total = exchange(0, rows_t + rows)
    row_sum = total[:, rows_t:]
    rs_ref[...] = row_sum
    r_row = 1.0 / total[:, :rows_t]

    for step in (1, 2):
        r_col = to_column(r_row)
        acc_r[...] = jnp.zeros_like(acc_r)

        @pl.loop(0, n_col // LANES)
        def _(j):
            here = pl.ds(pl.multiple_of(j * LANES, LANES), LANES)
            kern = kbuf[:, here]
            c_row = 1.0 / jnp.sum(kern * r_col, axis=0, keepdims=True)
            acc_r[...] += kern * c_row
            if step == 2:
                c_ref[dp, :, here] = c_row

        if step == 2:
            for k in range(1, n_dp):
                pltpu.make_async_remote_copy(
                    src_ref=c_ref.at[dp], dst_ref=c_ref.at[dp], send_sem=c_out.at[k], recv_sem=c_in.at[dp],
                    device_id=(vp, (dp + k) % n_dp), device_id_type=MESH).start()
        snd[step, :, :rows_t] = to_row(acc_r[...])
        r_row = 1.0 / exchange(step, rows_t)
    r_ref[...] = r_row

    r_col = to_column(r_row)
    r_wide = jnp.concatenate([r_col] * (NB_A // LANES), axis=1)
    wbuf[...] = jnp.zeros_like(wbuf)

    @pl.loop(0, n_blk)
    def _(j):
        here = pl.ds(pl.multiple_of(j * NB_A, NB_A), NB_A)
        q_mat = kbuf[:, here] * c_ref[dp, :, here] * r_wide
        q_hi = q_mat.astype(BF16)
        q_lo = (q_mat - q_hi.astype(F32)).astype(BF16)
        unit = ubuf[:, here]
        wbuf[...] += dot_t(q_hi, unit) + dot_t(q_lo, unit)

    w_zero = wbuf[:n_img]
    w_one = wbuf[n_img:]
    w_both = w_zero + w_one
    scale = 1.0 / (n_img * GLOBAL_CROPS * (ALL_CROPS - 1))
    log_rs = jnp.log(row_sum)
    inv_rs = to_column(1.0 / row_sum)
    loss = jnp.zeros((1, LANES), F32)
    for v in range(ALL_CROPS):
        block = pl.ds(v * n_img, n_img)
        count = float(GLOBAL_CROPS - (v < GLOBAL_CROPS))
        w_v = (w_one, w_zero)[v] if v < GLOBAL_CROPS else w_both
        inv = inv_rs[v * n_img:(v + 1) * n_img]
        inv = jnp.concatenate([inv] * (ge_ref.shape[1] // LANES), axis=1)
        dots = fold_lanes(jnp.sum(zs_ref[block].astype(F32) * w_v, axis=0, keepdims=True))
        logs = log_rs[:, v * n_img:(v + 1) * n_img]
        loss += (count / n_dev) * logs - (1.0 / TEMP_STUDENT) * dots
        ge_ref[block] = (count * (ge_ref[block] * inv) - w_v) * (scale / TEMP_STUDENT)
    loss_ref[...] = loss * scale

    for k in range(1, n_dp):
        src = (dp + n_dp - k) % n_dp
        pltpu.make_async_remote_copy(
            src_ref=c_ref.at[dp], dst_ref=c_ref.at[src], send_sem=c_out.at[k], recv_sem=c_in.at[src],
            device_id=(vp, src), device_id_type=MESH).wait()


def sinkhorn_stats(z_s, z_t, protos, ema_protos, n_vp, n_dp):
    rows, width = z_s.shape
    rows_t = z_t.shape[0]
    n_col = protos.shape[1] // n_dp
    n_dev = n_vp * n_dp
    flops = 2 * rows * n_col * width * 2
    return pl.pallas_call(
        functools.partial(stats_kernel, n_vp, n_dp),
        out_shape=(jax.ShapeDtypeStruct((n_dp, 1, n_col), F32),
                   jax.ShapeDtypeStruct((1, rows), F32),
                   jax.ShapeDtypeStruct((1, rows_t), F32),
                   jax.ShapeDtypeStruct((rows, width), F32),
                   jax.ShapeDtypeStruct((1, LANES), F32)),
        in_specs=[VMEM, VMEM, HBM, HBM],
        out_specs=(VMEM,) * 5,
        scratch_shapes=[
            pltpu.VMEM((2, width, NB_A), BF16),
            pltpu.VMEM((2, width, NB_A), BF16),
            pltpu.SemaphoreType.DMA((2, 2)),
            pltpu.VMEM((width, n_col), BF16),
            pltpu.VMEM((rows_t, n_col), F32),
            pltpu.VMEM((rows, LANES), F32),
            pltpu.VMEM((rows_t, LANES), F32),
            pltpu.VMEM((rows_t, width), F32),
            pltpu.VMEM((3, 1, rows + rows_t), F32),
            pltpu.VMEM((3, n_dev, 1, rows + rows_t), F32),
            pltpu.SemaphoreType.DMA((3, n_dev)),
            pltpu.SemaphoreType.DMA((3, n_dev)),
            pltpu.SemaphoreType.DMA((n_dp,)),
            pltpu.SemaphoreType.DMA((n_dp,)),
        ],
        compiler_params=pltpu.CompilerParams(
            collective_id=1, has_side_effects=True, vmem_limit_bytes=60 << 20),
        cost_estimate=pl.CostEstimate(flops=flops, bytes_accessed=4 * width * n_col, transcendentals=rows * n_col),
        name="sinkhorn_stats",
    )(z_s, z_t, protos, ema_protos)


def grads_kernel(n_vp, n_dp, zs_ref, zst_ref, zt_ref, rs_ref, r_ref, c_ref, ge_ref, loss_ref, x_ref, v_hbm, vt_hbm,
                 g_hbm, ge_all, loss_all, x_all, vbuf, tbuf, obuf, part_ge, sum_ge, part_loss, in_sem, loc_sem, out_sem,
                 recv_sem, rs_out, rs_in, ag_out, ag_in, ls_out, ls_in, x_out, x_in, xf_out, xf_in, x_own):
    vp, dp = my_place()
    n_dev = n_vp * n_dp
    me = vp * n_dp + dp
    n_chip = n_dp // 2
    chip, core = dp // 2, dp % 2
    partner = chip * 2 + 1 - core
    rows, rows_t = zs_ref.shape[0], zt_ref.shape[0]
    n_img = rows // ALL_CROPS
    n_own = rows // n_dev
    n_loc = x_ref.shape[1]
    half = v_hbm.shape[1] // 2
    n_slice = c_ref.shape[2]
    n_blk = half // NB_B
    base = core * half
    barrier = pltpu.get_barrier_semaphore()
    for k in range(1, n_dev):
        peer = (me + k) % n_dev
        pl.semaphore_signal(barrier, inc=1, device_id=(peer // n_dp, peer % n_dp), device_id_type=MESH)

    def load(j, slot):
        cols = pl.ds(pl.multiple_of(base + j * NB_B, NB_B), NB_B)
        return (pltpu.make_async_copy(v_hbm.at[:, cols], vbuf.at[slot], in_sem.at[0, slot]),
                pltpu.make_async_copy(vt_hbm.at[:, cols], tbuf.at[slot], in_sem.at[1, slot]))

    def local_store(j):
        slot = j % OUT_SLOTS
        cols = pl.ds(pl.multiple_of(base + j * NB_B, NB_B), NB_B)
        return pltpu.make_async_copy(obuf.at[slot], g_hbm.at[:, cols], loc_sem.at[slot])

    def remote_store(j):
        slot = j % OUT_SLOTS
        cols = pl.ds(pl.multiple_of(base + j * NB_B, NB_B), NB_B)
        return pltpu.make_async_remote_copy(
            src_ref=obuf.at[slot], dst_ref=g_hbm.at[:, cols], send_sem=out_sem.at[slot],
            recv_sem=recv_sem.at[j], device_id=(vp, partner), device_id_type=MESH)

    def peer_of(k):
        peer = (me + k) % n_dev
        return peer, (peer // n_dp, peer % n_dp)

    def scatter(k, peer, dst, device):
        return pltpu.make_async_remote_copy(
            src_ref=ge_ref.at[pl.ds(pl.multiple_of(peer * n_own, n_own), n_own)], dst_ref=part_ge.at[dst],
            send_sem=rs_out.at[k], recv_sem=rs_in.at[dst], device_id=device, device_id_type=MESH)

    def spread(k, owner, device):
        return pltpu.make_async_remote_copy(
            src_ref=sum_ge, dst_ref=ge_all.at[pl.ds(pl.multiple_of(owner * n_own, n_own), n_own)],
            send_sem=ag_out.at[k], recv_sem=ag_in.at[owner], device_id=device, device_id_type=MESH)

    def loss_send(k, dst, device):
        return pltpu.make_async_remote_copy(
            src_ref=loss_ref, dst_ref=part_loss.at[dst], send_sem=ls_out.at[k], recv_sem=ls_in.at[dst],
            device_id=device, device_id_type=MESH)

    def x_part(slot):
        return x_all.at[:, pl.ds(pl.multiple_of(slot * n_loc, n_loc), n_loc)]

    def x_send(k, src_chip, slot, device):
        return pltpu.make_async_remote_copy(
            src_ref=x_ref, dst_ref=x_part(slot), send_sem=x_out.at[k], recv_sem=x_in.at[src_chip],
            device_id=device, device_id_type=MESH)

    def x_forward(src_chip, slot):
        return pltpu.make_async_remote_copy(
            src_ref=x_part(slot), dst_ref=x_part(slot), send_sem=xf_out.at[src_chip], recv_sem=xf_in.at[src_chip],
            device_id=(vp, partner), device_id_type=MESH)

    for copy in load(0, 0):
        copy.start()
    x_local = pltpu.make_async_copy(x_ref, x_part(dp), x_own.at[0])
    x_local.start()
    scale = 1.0 / (n_img * GLOBAL_CROPS * (ALL_CROPS - 1)) / TEMP_STUDENT
    lanes = lax.broadcasted_iota(jnp.int32, (1, rows), 1)
    weight = jnp.where(lanes < GLOBAL_CROPS * n_img, scale, GLOBAL_CROPS * scale)
    bias = to_column(jnp.log(weight / rs_ref[...]) * LOG2E)
    bias = jnp.concatenate([bias] * (NB_B // LANES), axis=1)
    r_col = to_column(r_ref[...] * scale)
    r_wide = jnp.concatenate([r_col] * (NB_B // LANES), axis=1)
    pl.semaphore_wait(barrier, n_dev - 1)
    for k in range(1, n_dev):
        peer, device = peer_of(k)
        loss_send(k, me, device).start()
        scatter(k, peer, me, device).start()
    for k in range(1, n_chip):
        x_send(k, chip, dp, (vp, ((chip + k) % n_chip) * 2 + core)).start()
    part_ge[me] = ge_ref[pl.ds(pl.multiple_of(me * n_own, n_own), n_own)]
    part_loss[me] = loss_ref[...]

    @pl.loop(0, n_blk)
    def _(j):
        slot = j % 2

        @pl.when(j + 1 < n_blk)
        def _():
            for copy in load(j + 1, 1 - slot):
                copy.start()

        @pl.when(j >= 1)
        def _():
            local_store(j - 1).start()
            remote_store(j - 1).start()

        @pl.when(j >= OUT_SLOTS)
        def _():
            local_store(j - OUT_SLOTS).wait()
            remote_store(j - OUT_SLOTS).wait_send()

        @pl.when(j == n_blk // 2)
        def _():
            for k in range(1, n_dev):
                src = (me + n_dev - k) % n_dev
                scatter(k, src, src, (vp, partner)).wait()
                loss_send(k, src, (vp, partner)).wait()
            total = part_ge[0]
            loss = part_loss[0]
            for k in range(1, n_dev):
                total = total + part_ge[k]
                loss = loss + part_loss[k]
            loss_all[...] = loss
            sum_ge[...] = total
            ge_all[pl.ds(pl.multiple_of(me * n_own, n_own), n_own)] = total

        @pl.when(j == n_blk // 2 + 1)
        def _():
            for k in range(1, n_dev):
                spread(k, me, peer_of(k)[1]).start()

        @pl.when(j == n_blk - 4)
        def _():
            x_local.wait()
            x_forward(chip, dp).start()
            for k in range(1, n_chip):
                src = (chip + n_chip - k) % n_chip
                x_send(k, src, src * 2 + core, (vp, partner)).wait()
                x_forward(src, src * 2 + core).start()

        for copy in load(j, slot):
            copy.wait()
        unit_t = unit_columns(tbuf[slot])[0].astype(BF16)
        col = base + j * NB_B
        c_row = c_ref[col // n_slice, :, pl.ds(pl.multiple_of(col % n_slice, NB_B), NB_B)]
        q_mat = jnp.exp2(dot(zt_ref[...], unit_t) * (LOG2E / TEMP_TEACHER)) * c_row * r_wide
        q_zero, q_one = q_mat[:n_img], q_mat[n_img:]
        q_both = q_zero + q_one
        unit, inv_col = unit_columns(vbuf[slot])
        logits = dot(zs_ref[...], unit.astype(BF16))
        soft = jnp.exp2(logits * (LOG2E / TEMP_STUDENT) + bias)
        target = jnp.concatenate([q_one, q_zero] + [q_both] * (ALL_CROPS - GLOBAL_CROPS), axis=0)
        g_unit = dot(zst_ref[...], (soft - target).astype(BF16))
        obuf[j % OUT_SLOTS] = (g_unit - unit * jnp.sum(unit * g_unit, axis=0, keepdims=True)) * inv_col

    local_store(n_blk - 1).start()
    remote_store(n_blk - 1).start()
    for j in range(n_blk - OUT_SLOTS, n_blk):
        local_store(j).wait()
        remote_store(j).wait_send()
    for k in range(1, n_dev):
        src = (me + n_dev - k) % n_dev
        spread(k, src, (vp, partner)).wait()
    for src in range(n_chip):
        pltpu.make_async_remote_copy(
            src_ref=x_part(src * 2 + core), dst_ref=x_part(src * 2 + 1 - core), send_sem=xf_out.at[src],
            recv_sem=xf_in.at[src], device_id=(vp, partner), device_id_type=MESH).wait()

    @pl.loop(0, n_blk)
    def _(j):
        remote_store(j).wait_recv()


def proto_grads(z_s, z_t, row_sum, r_row, c_all, g_emb, loss, x_loc, protos, ema_protos, n_vp, n_dp):
    rows, width = z_s.shape
    n_col = protos.shape[1]
    n_blk = n_col // 2 // NB_B
    n_dev = n_vp * n_dp
    dma = pltpu.SemaphoreType.DMA
    return pl.pallas_call(
        functools.partial(grads_kernel, n_vp, n_dp),
        out_shape=(jax.ShapeDtypeStruct((width, n_col), F32),
                   jax.ShapeDtypeStruct((rows, width), F32),
                   jax.ShapeDtypeStruct((1, LANES), F32),
                   jax.ShapeDtypeStruct((x_loc.shape[0], x_loc.shape[1] * n_dp, x_loc.shape[2]), F32)),
        in_specs=[VMEM] * 9 + [HBM] * 2,
        out_specs=(HBM, VMEM, VMEM, HBM),
        scratch_shapes=[
            pltpu.VMEM((2, width, NB_B), BF16),
            pltpu.VMEM((2, width, NB_B), BF16),
            pltpu.VMEM((OUT_SLOTS, width, NB_B), F32),
            pltpu.VMEM((n_dev, rows // n_dev, width), F32),
            pltpu.VMEM((rows // n_dev, width), F32),
            pltpu.VMEM((n_dev, 1, LANES), F32),
            dma((2, 2)),
            dma((OUT_SLOTS,)),
            dma((OUT_SLOTS,)),
            dma((n_blk,)),
        ] + [dma((n_dev,))] * 6 + [dma((n_dp // 2,))] * 4 + [dma((1,))],
        compiler_params=pltpu.CompilerParams(
            collective_id=2, has_side_effects=True, vmem_limit_bytes=60 << 20),
        cost_estimate=pl.CostEstimate(
            flops=2 * rows * n_col * width, bytes_accessed=4 * width * n_col, transcendentals=rows * n_col // 2),
        name="proto_grads",
    )(z_s, z_s.T, z_t, row_sum, r_row, c_all, g_emb, loss, x_loc, protos, ema_protos)


def head_kernel(x_hbm, wi_hbm, wm_hbm, wo_hbm, bi_ref, bm_ref, bo_ref, ge_ref,
                h1_hbm, h2_hbm, g2_hbm, g1_hbm, gp_ref, bias_ref,
                x_buf, wi, wm, wo, hid_one, hid_two, slope_one, slope_two, stage, grad_two, gp_stage, snd, rcv,
                ld_sem, loc_sem, out_sem, in_sem, gp_sem, bs_sem):
    vp, dp = my_place()
    chip, core = dp // 2, dp % 2
    partner = chip * 2 + 1 - core
    half, n_hid = hid_one.shape
    n_out = wo.shape[1]
    n_blk = n_hid // HB
    mine = pl.ds(pl.multiple_of(core * half, half), half)
    device = (vp, partner)
    barrier = pltpu.get_barrier_semaphore()
    pl.semaphore_signal(barrier, inc=1, device_id=device, device_id_type=MESH)
    loads = [pltpu.make_async_copy(x_hbm.at[mine], x_buf, ld_sem.at[0]),
             pltpu.make_async_copy(wi_hbm, wi, ld_sem.at[1]),
             pltpu.make_async_copy(wm_hbm, wm, ld_sem.at[2]),
             pltpu.make_async_copy(wo_hbm, wo, ld_sem.at[3])]
    for copy in loads:
        copy.start()
    pl.semaphore_wait(barrier, 1)

    def block(j):
        return pl.ds(pl.multiple_of(j * HB, HB), HB)

    def keep(array, dst, j):
        return pltpu.make_async_copy(
            stage.at[array % 2, :, block(j)], dst.at[mine, block(j)], loc_sem.at[array, j])

    def send(array, dst, j):
        return pltpu.make_async_remote_copy(
            src_ref=stage.at[array % 2, :, block(j)], dst_ref=dst.at[mine, block(j)], send_sem=out_sem.at[array, j],
            recv_sem=in_sem.at[array, j], device_id=device, device_id_type=MESH)

    def flush(array, dst, j):
        keep(array, dst, j).start()
        send(array, dst, j).start()

    def drain(array, dst):
        @pl.loop(0, n_blk)
        def _(j):
            keep(array, dst, j).wait()
            send(array, dst, j).wait_send()

    def layer(array, feats, weight, b_ref, hid, slope, dst):
        @pl.loop(0, n_blk)
        def _(j):
            @pl.when(j >= 1)
            def _():
                flush(array, dst, j - 1)

            pre = dot(feats, weight[:, block(j)]) + b_ref[:, block(j)].astype(F32)
            cdf = 0.5 * (1.0 + lax.erf(pre * 0.7071067811865476))
            low = (pre * cdf).astype(BF16)
            hid[:, block(j)] = low
            stage[array % 2, :, block(j)] = low.astype(F32)
            slope[:, block(j)] = cdf + pre * jnp.exp(-0.5 * pre * pre) * 0.3989422804014327
        flush(array, dst, n_blk - 1)

    loads[0].wait()
    loads[1].wait()
    layer(0, x_buf[...].astype(BF16), wi, bi_ref, hid_one, slope_one, h1_hbm)
    loads[2].wait()
    layer(1, hid_one[...], wm, bm_ref, hid_two, slope_two, h2_hbm)
    loads[3].wait()
    proj = dot(hid_two[...], wo[...]) + bo_ref[...].astype(F32)
    inv_norm = lax.rsqrt(jnp.sum(proj * proj, axis=-1, keepdims=True))
    unit = proj * inv_norm
    g_emb = ge_ref[mine]
    g_proj = (g_emb - unit * jnp.sum(unit * g_emb, axis=-1, keepdims=True)) * inv_norm
    gp_low = g_proj.astype(BF16)
    gp_stage[...] = gp_low.astype(F32)
    gp_ref[mine] = gp_low.astype(F32)
    snd[:, 2 * n_hid:] = jnp.sum(g_proj, axis=0, keepdims=True)
    drain(0, h1_hbm)

    @pl.loop(0, n_blk)
    def _(j):
        @pl.when(j >= 1)
        def _():
            flush(2, g2_hbm, j - 1)

        g_hid = dot_t(gp_low, wo[block(j), :])
        g_pre = g_hid.astype(BF16).astype(F32) * slope_two[:, block(j)]
        snd[:, block(j)] = jnp.sum(g_pre, axis=0, keepdims=True)
        low = g_pre.astype(BF16)
        grad_two[:, block(j)] = low
        stage[0, :, block(j)] = low.astype(F32)
    flush(2, g2_hbm, n_blk - 1)
    gp_send = pltpu.make_async_remote_copy(
        src_ref=gp_stage, dst_ref=gp_ref.at[mine], send_sem=gp_sem.at[0], recv_sem=gp_sem.at[1],
        device_id=device, device_id_type=MESH)
    gp_send.start()
    drain(1, h2_hbm)

    @pl.loop(0, n_blk)
    def _(j):
        @pl.when(j >= 1)
        def _():
            flush(3, g1_hbm, j - 1)

        g_hid = dot_t(grad_two[...], wm[block(j), :])
        g_pre = g_hid.astype(BF16).astype(F32) * slope_one[:, block(j)]
        snd[:, pl.ds(pl.multiple_of(n_hid + j * HB, HB), HB)] = jnp.sum(g_pre, axis=0, keepdims=True)
        stage[1, :, block(j)] = g_pre.astype(BF16).astype(F32)
    flush(3, g1_hbm, n_blk - 1)
    bias_send = pltpu.make_async_remote_copy(
        src_ref=snd, dst_ref=rcv, send_sem=bs_sem.at[0], recv_sem=bs_sem.at[1],
        device_id=device, device_id_type=MESH)
    bias_send.start()
    drain(2, g2_hbm)
    drain(3, g1_hbm)
    gp_send.wait()
    bias_send.wait()
    bias_ref[...] = snd[...] + rcv[...]
    for array, dst in enumerate((h1_hbm, h2_hbm, g2_hbm, g1_hbm)):
        @pl.loop(0, n_blk)
        def _(j):
            send(array, dst, j).wait_recv()


def head_pass(x_all, w_in, b_in, w_mid, b_mid, w_out, b_out, g_emb):
    rows, feat = x_all.shape
    n_hid, n_out = w_out.shape
    half = rows // 2
    n_blk = n_hid // HB
    n_bias = 2 * n_hid + n_out
    dma = pltpu.SemaphoreType.DMA
    wide = jax.ShapeDtypeStruct((rows, n_hid), F32)
    return pl.pallas_call(
        head_kernel,
        out_shape=(wide, wide, wide, wide, jax.ShapeDtypeStruct((rows, n_out), F32),
                   jax.ShapeDtypeStruct((1, n_bias), F32)),
        in_specs=[HBM] * 4 + [VMEM] * 4,
        out_specs=(HBM,) * 4 + (VMEM,) * 2,
        scratch_shapes=[
            pltpu.VMEM((half, feat), F32),
            pltpu.VMEM((feat, n_hid), BF16),
            pltpu.VMEM((n_hid, n_hid), BF16),
            pltpu.VMEM((n_hid, n_out), BF16),
            pltpu.VMEM((half, n_hid), BF16),
            pltpu.VMEM((half, n_hid), BF16),
            pltpu.VMEM((half, n_hid), F32),
            pltpu.VMEM((half, n_hid), F32),
            pltpu.VMEM((2, half, n_hid), F32),
            pltpu.VMEM((half, n_hid), BF16),
            pltpu.VMEM((half, n_out), F32),
            pltpu.VMEM((1, n_bias), F32),
            pltpu.VMEM((1, n_bias), F32),
            dma((4,)), dma((4, n_blk)), dma((4, n_blk)), dma((4, n_blk)), dma((2,)), dma((2,)),
        ],
        compiler_params=pltpu.CompilerParams(
            collective_id=3, has_side_effects=True, vmem_limit_bytes=63 << 20),
        cost_estimate=pl.CostEstimate(
            flops=2 * rows * (feat + 2 * n_hid) * n_hid, bytes_accessed=16 * rows * n_hid, transcendentals=2 * rows * n_hid),
        name="head_pass",
    )(x_all, w_in, w_mid, w_out, b_in.reshape(1, -1), b_mid.reshape(1, -1), b_out.reshape(1, -1), g_emb)


def wgrad_kernel(first, n_step, base, *refs):
    if first:
        a_ref, b_ref, src, out_ref, dst, low, cbuf, rd_sem, wr_sem = refs
    else:
        a_ref, b_ref, src, _, out_ref, dst, low, cbuf, rd_sem, wr_sem = refs
    i = pl.program_id(0)
    chunk = cbuf.shape[2]

    def cols(step):
        return pl.ds(pl.multiple_of(base + step * chunk, chunk), chunk)

    def read(step):
        return pltpu.make_async_copy(src.at[:, cols(step)], cbuf.at[step % 3], rd_sem.at[step % 3])

    def write(step):
        return pltpu.make_async_copy(cbuf.at[step % 3], dst.at[:, cols(step)], wr_sem.at[step % 3])

    @pl.when(i == 0)
    def _():
        read(0).start()
        low[...] = b_ref[...].astype(BF16)

    @pl.when(i >= 2)
    def _():
        write(i - 2).wait()

    @pl.when(i + 1 < n_step)
    def _():
        read(i + 1).start()

    read(i).wait()
    write(i).start()
    out_ref[...] = lax.dot_general(
        a_ref[...].astype(BF16), low[...], (((0,), (0,)), ((), ())), preferred_element_type=F32)

    @pl.when(i == n_step - 1)
    def _():
        write(i - 1).wait()
        write(i).wait()


def wgrad(left, right, src, dst, start, width, block=256):
    rows, n_left = left.shape
    n_right = right.shape[1]
    n_step = n_left // block
    first = dst is None
    chunk = width // n_step
    args = (left, right, src) + (() if first else (dst,))
    return pl.pallas_call(
        functools.partial(wgrad_kernel, first, n_step, start),
        grid=(n_step,),
        out_shape=(jax.ShapeDtypeStruct((n_left, n_right), F32), jax.ShapeDtypeStruct(src.shape, F32)),
        in_specs=[pl.BlockSpec((rows, block), lambda i: (0, i)),
                  pl.BlockSpec((rows, n_right), lambda i: (0, 0), pipeline_mode=pl.Buffered(1)),
                  HBM] + ([] if first else [HBM]),
        out_specs=(pl.BlockSpec((block, n_right), lambda i: (i, 0)), HBM),
        scratch_shapes=[pltpu.VMEM((rows, n_right), BF16),
                        pltpu.VMEM((3, src.shape[0], chunk), F32),
                        pltpu.SemaphoreType.DMA((3,)), pltpu.SemaphoreType.DMA((3,))],
        input_output_aliases={} if first else {3: 1},
        compiler_params=pltpu.CompilerParams(
            dimension_semantics=("arbitrary",), vmem_limit_bytes=60 << 20),
        cost_estimate=pl.CostEstimate(
            flops=2 * rows * n_left * n_right, bytes_accessed=8 * src.shape[0] * width, transcendentals=0),
        name="wgrad",
    )(*args)


def solution(mesh):
    n_vp = mesh.shape['vp']
    n_dp = mesh.shape['dp']

    def local_step(student_x, teacher_x, w_in, b_in, w_mid, b_mid, w_out, b_out, protos,
                   ema_w_in, ema_b_in, ema_w_mid, ema_b_mid, ema_w_out, ema_b_out, ema_protos):
        rows, feat = student_x.shape
        n_img = rows // ALL_CROPS
        width = protos.shape[0]
        x_loc = student_x.reshape(n_img, ALL_CROPS, feat).transpose(1, 0, 2)
        t_loc = teacher_x.reshape(n_img, GLOBAL_CROPS, feat).transpose(1, 0, 2).reshape(-1, feat)
        t_emb = mlp_forward(t_loc, ema_w_in, ema_b_in, ema_w_mid, ema_b_mid, ema_w_out, ema_b_out)
        s_emb = mlp_forward(x_loc.reshape(rows, feat), w_in, b_in, w_mid, b_mid, w_out, b_out)
        z_loc = jnp.concatenate([s_emb, t_emb], axis=0).reshape(ALL_CROPS + GLOBAL_CROPS, n_img, width)
        z_all = gather_dp(z_loc, n_dp, 0).reshape(-1, width).astype(BF16)
        z_s, z_t = z_all[:rows * n_dp], z_all[rows * n_dp:]
        c_all, row_sum, r_row, g_emb, loss = sinkhorn_stats(z_s, z_t, protos, ema_protos, n_vp, n_dp)
        g_temp, g_emb, loss, x_all = proto_grads(
            z_s, z_t, row_sum, r_row, c_all, g_emb, loss, x_loc.astype(F32), protos, ema_protos, n_vp, n_dp)
        x_all = x_all.reshape(rows * n_dp, feat)
        hid_one, hid_two, g_two, g_one, g_proj, biases = head_pass(
            x_all, w_in, b_in, w_mid, b_mid, w_out, b_out, g_emb)
        n_hid = w_mid.shape[0]
        part = protos.shape[1] // 8
        g_w_mid, g_protos = wgrad(hid_one, g_two, g_temp, None, 0, 4 * part)
        g_w_in, g_protos = wgrad(x_all, g_one, g_temp, g_protos, 4 * part, 3 * part)
        g_w_out, g_protos = wgrad(hid_two, g_proj, g_temp, g_protos, 7 * part, part)
        biases = biases.reshape(-1)
        g_b_mid, g_b_in, g_b_out = biases[:n_hid], biases[n_hid:2 * n_hid], biases[2 * n_hid:]
        return (jnp.sum(loss), g_w_in, g_b_in, g_w_mid, g_b_mid, g_w_out, g_b_out, g_protos)

    by_rows = P('dp', None)
    by_cols = P(None, 'vp')
    replicated = P()
    head_specs = (replicated,) * 6
    in_specs = (by_rows, by_rows) + head_specs + (by_cols,) + head_specs + (by_cols,)
    out_specs = (replicated,) * 7 + (by_cols,)
    return jax.shard_map(local_step, mesh=mesh, in_specs=in_specs, out_specs=out_specs, check_vma=False)
```

```python
import functools

import jax
import jax.numpy as jnp
from jax import lax
from jax.experimental import pallas as pl
from jax.experimental.pallas import tpu as pltpu
from jax.sharding import PartitionSpec as P

ALL_CROPS = 10
GLOBAL_CROPS = 2
TEMP_STUDENT = 0.1
TEMP_TEACHER = 0.04
LOG2E = 1.4426950408889634
LANES = 128
NB_A = 1024
NB_B = 1024
OUT_SLOTS = 3
HB = 256
FIRST = 22
EARLY = 30
F32 = jnp.float32
BF16 = jnp.bfloat16
MESH = pl.DeviceIdType.MESH
HBM = pl.BlockSpec(memory_space=pl.ANY)
VMEM = pl.BlockSpec(memory_space=pltpu.VMEM)


def mlp_forward(feats, w_in, b_in, w_mid, b_mid, w_out, b_out):
    pre_one = jnp.dot(feats, w_in, preferred_element_type=F32) + b_in.astype(F32)
    hid_one = jax.nn.gelu(pre_one, approximate=False).astype(BF16)
    pre_two = jnp.dot(hid_one, w_mid, preferred_element_type=F32) + b_mid.astype(F32)
    hid_two = jax.nn.gelu(pre_two, approximate=False).astype(BF16)
    proj = jnp.dot(hid_two, w_out, preferred_element_type=F32) + b_out.astype(F32)
    inv_norm = lax.rsqrt(jnp.sum(proj * proj, axis=-1, keepdims=True))
    return proj * inv_norm


def unit_columns(block):
    block_f = block.astype(F32)
    inv_col = lax.rsqrt(jnp.sum(block_f * block_f, axis=0, keepdims=True))
    return block_f * inv_col, inv_col


def dot(left, right):
    return jnp.dot(left, right, preferred_element_type=F32)


def dot_t(left, right):
    return lax.dot_general(left, right, (((1,), (1,)), ((), ())), preferred_element_type=F32)


def to_column(row):
    return jnp.transpose(jnp.broadcast_to(row, (LANES, row.shape[1])))


def to_row(acc):
    return jnp.sum(jnp.transpose(acc), axis=0, keepdims=True)


def fold_lanes(wide):
    total = wide[:, :LANES]
    for start in range(LANES, wide.shape[1], LANES):
        total = total + wide[:, start:start + LANES]
    return total


def my_place():
    return lax.axis_index('vp'), lax.axis_index('dp')


def gather_kernel(n_dp, block_ref, all_ref, out_sem, in_sem, fwd_out, fwd_in):
    vp, me = my_place()
    n_chip = n_dp // 2
    chip, core = me // 2, me % 2
    partner = chip * 2 + 1 - core
    n_row = block_ref.shape[1]

    def part(slot):
        return all_ref.at[:, pl.ds(pl.multiple_of(slot * n_row, n_row), n_row)]

    barrier = pltpu.get_barrier_semaphore()
    pl.semaphore_signal(barrier, inc=1, device_id=(vp, partner), device_id_type=MESH)
    for k in range(1, n_chip):
        peer = ((chip + k) % n_chip) * 2 + core
        pl.semaphore_signal(barrier, inc=1, device_id=(vp, peer), device_id_type=MESH)
    pl.semaphore_wait(barrier, n_chip)
    sends = []
    for k in range(1, n_chip):
        peer = ((chip + k) % n_chip) * 2 + core
        sends.append(pltpu.make_async_remote_copy(
            src_ref=block_ref, dst_ref=part(me), send_sem=out_sem.at[k], recv_sem=in_sem.at[chip],
            device_id=(vp, peer), device_id_type=MESH))
    own = pltpu.make_async_remote_copy(
        src_ref=block_ref, dst_ref=part(me), send_sem=fwd_out.at[chip], recv_sem=fwd_in.at[chip],
        device_id=(vp, partner), device_id_type=MESH)
    for copy in sends:
        copy.start()
    own.start()
    all_ref[:, pl.ds(pl.multiple_of(me * n_row, n_row), n_row)] = block_ref[...]
    for k in range(1, n_chip):
        src = (chip + n_chip - k) % n_chip
        slot = src * 2 + core
        peer_copy = pltpu.make_async_remote_copy(
            src_ref=block_ref, dst_ref=part(slot), send_sem=out_sem.at[k], recv_sem=in_sem.at[src],
            device_id=(vp, partner), device_id_type=MESH)
        peer_copy.wait_recv()
        forward = pltpu.make_async_remote_copy(
            src_ref=part(slot), dst_ref=part(slot), send_sem=fwd_out.at[src], recv_sem=fwd_in.at[src],
            device_id=(vp, partner), device_id_type=MESH)
        forward.start()
    for copy in sends:
        copy.wait_send()
    for src in range(n_chip):
        slot = src * 2 + core
        other = src * 2 + 1 - core
        pltpu.make_async_remote_copy(
            src_ref=part(slot), dst_ref=part(other), send_sem=fwd_out.at[src], recv_sem=fwd_in.at[src],
            device_id=(vp, partner), device_id_type=MESH).wait()


def gather_dp(block, n_dp, collective_id):
    groups, n_row, width = block.shape
    return pl.pallas_call(
        functools.partial(gather_kernel, n_dp),
        out_shape=jax.ShapeDtypeStruct((groups, n_row * n_dp, width), block.dtype),
        in_specs=[VMEM],
        out_specs=VMEM,
        scratch_shapes=[pltpu.SemaphoreType.DMA((n_dp // 2,))] * 4,
        compiler_params=pltpu.CompilerParams(
            collective_id=collective_id, has_side_effects=True, vmem_limit_bytes=48 << 20),
        name="gather_dp",
    )(block)


def stats_kernel(n_vp, n_dp, zs_ref, zt_ref, v_hbm, vt_hbm, c_ref, rs_ref, r_ref, ge_ref, loss_ref,
                 vbuf, tbuf, in_sem, ubuf, kbuf, acc_s, acc_r, wbuf, snd, rcv, send_sem, recv_sem, c_out, c_in):
    vp, dp = my_place()
    n_dev = n_vp * n_dp
    me = vp * n_dp + dp
    rows, rows_t = zs_ref.shape[0], zt_ref.shape[0]
    n_img = rows // ALL_CROPS
    n_col = kbuf.shape[1]
    n_blk = n_col // NB_A
    base = dp * n_col

    barrier = pltpu.get_barrier_semaphore()
    for k in range(1, n_dev):
        peer = (me + k) % n_dev
        pl.semaphore_signal(barrier, inc=1, device_id=(peer // n_dp, peer % n_dp), device_id_type=MESH)

    def load(which, j):
        src, buf = ((v_hbm, vbuf), (vt_hbm, tbuf))[which]
        cols = pl.ds(pl.multiple_of(base + j * NB_A, NB_A), NB_A)
        return pltpu.make_async_copy(src.at[:, cols], buf.at[j % 2], in_sem.at[which, j % 2])

    load(1, 0).start()
    load(0, 0).start()
    acc_s[...] = jnp.zeros_like(acc_s)
    acc_r[...] = jnp.zeros_like(acc_r)
    ge_ref[...] = jnp.zeros_like(ge_ref)

    @pl.loop(0, n_blk)
    def _(j):
        @pl.when(j + 1 < n_blk)
        def _():
            load(1, j + 1).start()

        load(1, j).wait()
        unit_t = unit_columns(tbuf[j % 2])[0].astype(BF16)
        kern = jnp.exp2(dot(zt_ref[...], unit_t) * (LOG2E / TEMP_TEACHER))
        kbuf[:, pl.ds(pl.multiple_of(j * NB_A, NB_A), NB_A)] = kern
        acc_r[...] += fold_lanes(kern * (1.0 / jnp.sum(kern, axis=0, keepdims=True)))

    pl.semaphore_wait(barrier, n_dev - 1)

    def message(step, k, dst, peer, width):
        return pltpu.make_async_remote_copy(
            src_ref=snd.at[step, :, :width], dst_ref=rcv.at[step, dst, :, :width],
            send_sem=send_sem.at[step, k], recv_sem=recv_sem.at[step, dst],
            device_id=(peer // n_dp, peer % n_dp), device_id_type=MESH)

    def publish(step, value):
        width = value.shape[1]
        snd[step, :, :width] = value
        for k in range(1, n_dev):
            message(step, k, me, (me + k) % n_dev, width).start()
        rcv[step, me, :, :width] = value

    def collect(step, width):
        for k in range(1, n_dev):
            src = (me + n_dev - k) % n_dev
            message(step, k, src, src, width).wait()
        total = rcv[step, 0, :, :width]
        for k in range(1, n_dev):
            total = total + rcv[step, k, :, :width]
        return total

    def student(first, last):
        @pl.loop(first, last)
        def _(j):
            @pl.when(j + 1 < n_blk)
            def _():
                load(0, j + 1).start()

            load(0, j).wait()
            unit = unit_columns(vbuf[j % 2])[0].astype(BF16)
            ubuf[:, pl.ds(pl.multiple_of(j * NB_A, NB_A), NB_A)] = unit
            exp_s = jnp.exp2(dot(zs_ref[...], unit) * (LOG2E / TEMP_STUDENT))
            acc_s[...] += fold_lanes(exp_s)
            ge_ref[...] += dot_t(exp_s.astype(BF16), unit)

    def rescale(r_row, keep):
        r_col = to_column(r_row)
        acc_r[...] = jnp.zeros_like(acc_r)
        span = 4 * LANES

        @pl.loop(0, n_col // span)
        def _(j):
            total = acc_r[...]
            for k in range(4):
                here = pl.ds(pl.multiple_of(j * span + k * LANES, LANES), LANES)
                kern = kbuf[:, here]
                c_row = 1.0 / jnp.sum(kern * r_col, axis=0, keepdims=True)
                total = total + kern * c_row
                if keep:
                    c_ref[dp, :, here] = c_row
            acc_r[...] = total

    third = (n_blk * 3) // 8
    publish(0, to_row(acc_r[...]))
    student(0, third)
    rescale(1.0 / collect(0, rows_t), False)
    publish(1, to_row(acc_r[...]))
    student(third, 2 * third)
    rescale(1.0 / collect(1, rows_t), True)
    publish(2, to_row(acc_r[...]))
    for k in range(1, n_dp):
        pltpu.make_async_remote_copy(
            src_ref=c_ref.at[dp], dst_ref=c_ref.at[dp], send_sem=c_out.at[k], recv_sem=c_in.at[dp],
            device_id=(vp, (dp + k) % n_dp), device_id_type=MESH).start()
    student(2 * third, n_blk)
    publish(3, to_row(acc_s[...]))
    r_row = 1.0 / collect(2, rows_t)
    r_ref[...] = r_row

    r_col = to_column(r_row)
    r_wide = jnp.concatenate([r_col] * (NB_A // LANES), axis=1)
    wbuf[...] = jnp.zeros_like(wbuf)

    @pl.loop(0, n_blk)
    def _(j):
        here = pl.ds(pl.multiple_of(j * NB_A, NB_A), NB_A)
        q_mat = kbuf[:, here] * c_ref[dp, :, here] * r_wide
        q_hi = q_mat.astype(BF16)
        q_lo = (q_mat - q_hi.astype(F32)).astype(BF16)
        both = dot_t(jnp.concatenate([q_hi, q_lo], axis=0), ubuf[:, here])
        wbuf[...] += both[:rows_t] + both[rows_t:]

    row_sum = collect(3, rows)
    rs_ref[...] = row_sum
    w_zero = wbuf[:n_img]
    w_one = wbuf[n_img:]
    w_both = w_zero + w_one
    scale = 1.0 / (n_img * GLOBAL_CROPS * (ALL_CROPS - 1))
    log_rs = jnp.log(row_sum)
    inv_rs = to_column(1.0 / row_sum)
    loss = jnp.zeros((1, LANES), F32)
    for v in range(ALL_CROPS):
        block = pl.ds(v * n_img, n_img)
        count = float(GLOBAL_CROPS - (v < GLOBAL_CROPS))
        w_v = (w_one, w_zero)[v] if v < GLOBAL_CROPS else w_both
        inv = inv_rs[v * n_img:(v + 1) * n_img]
        inv = jnp.concatenate([inv] * (ge_ref.shape[1] // LANES), axis=1)
        dots = fold_lanes(jnp.sum(zs_ref[block].astype(F32) * w_v, axis=0, keepdims=True))
        logs = log_rs[:, v * n_img:(v + 1) * n_img]
        loss += (count / n_dev) * logs - (1.0 / TEMP_STUDENT) * dots
        ge_ref[block] = (count * (ge_ref[block] * inv) - w_v) * (scale / TEMP_STUDENT)
    loss_ref[...] = loss * scale

    for k in range(1, n_dp):
        src = (dp + n_dp - k) % n_dp
        pltpu.make_async_remote_copy(
            src_ref=c_ref.at[dp], dst_ref=c_ref.at[src], send_sem=c_out.at[k], recv_sem=c_in.at[src],
            device_id=(vp, src), device_id_type=MESH).wait()


def sinkhorn_stats(z_s, z_t, protos, ema_protos, n_vp, n_dp):
    rows, width = z_s.shape
    rows_t = z_t.shape[0]
    n_col = protos.shape[1] // n_dp
    n_dev = n_vp * n_dp
    flops = 2 * rows * n_col * width * 2
    return pl.pallas_call(
        functools.partial(stats_kernel, n_vp, n_dp),
        out_shape=(jax.ShapeDtypeStruct((n_dp, 1, n_col), F32),
                   jax.ShapeDtypeStruct((1, rows), F32),
                   jax.ShapeDtypeStruct((1, rows_t), F32),
                   jax.ShapeDtypeStruct((rows, width), F32),
                   jax.ShapeDtypeStruct((1, LANES), F32)),
        in_specs=[VMEM, VMEM, HBM, HBM],
        out_specs=(VMEM,) * 5,
        scratch_shapes=[
            pltpu.VMEM((2, width, NB_A), BF16),
            pltpu.VMEM((2, width, NB_A), BF16),
            pltpu.SemaphoreType.DMA((2, 2)),
            pltpu.VMEM((width, n_col), BF16),
            pltpu.VMEM((rows_t, n_col), F32),
            pltpu.VMEM((rows, LANES), F32),
            pltpu.VMEM((rows_t, LANES), F32),
            pltpu.VMEM((rows_t, width), F32),
            pltpu.VMEM((4, 1, rows), F32),
            pltpu.VMEM((4, n_dev, 1, rows), F32),
            pltpu.SemaphoreType.DMA((4, n_dev)),
            pltpu.SemaphoreType.DMA((4, n_dev)),
            pltpu.SemaphoreType.DMA((n_dp,)),
            pltpu.SemaphoreType.DMA((n_dp,)),
        ],
        compiler_params=pltpu.CompilerParams(
            collective_id=1, has_side_effects=True, vmem_limit_bytes=60 << 20),
        cost_estimate=pl.CostEstimate(flops=flops, bytes_accessed=4 * width * n_col, transcendentals=rows * n_col),
        name="sinkhorn_stats",
    )(z_s, z_t, protos, ema_protos)


def row_weights(rs_ref, r_ref, rows, n_img):
    scale = 1.0 / (n_img * GLOBAL_CROPS * (ALL_CROPS - 1)) / TEMP_STUDENT
    lanes = lax.broadcasted_iota(jnp.int32, (1, rows), 1)
    weight = jnp.where(lanes < GLOBAL_CROPS * n_img, scale, GLOBAL_CROPS * scale)
    bias = to_column(jnp.log(weight / rs_ref[...]) * LOG2E)
    r_col = to_column(r_ref[...] * scale)
    return jnp.concatenate([bias] * (NB_B // LANES), axis=1), jnp.concatenate([r_col] * (NB_B // LANES), axis=1)


def grad_block(zs_ref, zst_ref, zt_ref, c_ref, bias, r_wide, v_block, t_block, col, n_img):
    n_slice = c_ref.shape[2]
    unit_t = unit_columns(t_block)[0].astype(BF16)
    c_row = c_ref[col // n_slice, :, pl.ds(pl.multiple_of(col % n_slice, NB_B), NB_B)]
    q_mat = jnp.exp2(dot(zt_ref[...], unit_t) * (LOG2E / TEMP_TEACHER)) * c_row * r_wide
    q_zero, q_one = q_mat[:n_img], q_mat[n_img:]
    q_both = q_zero + q_one
    unit, inv_col = unit_columns(v_block)
    logits = dot(zs_ref[...], unit.astype(BF16))
    soft = jnp.exp2(logits * (LOG2E / TEMP_STUDENT) + bias)
    target = jnp.concatenate([q_one, q_zero] + [q_both] * (ALL_CROPS - GLOBAL_CROPS), axis=0)
    g_unit = dot(zst_ref[...], (soft - target).astype(BF16))
    return (g_unit - unit * jnp.sum(unit * g_unit, axis=0, keepdims=True)) * inv_col


def grads_kernel(n_vp, n_dp, zs_ref, zst_ref, zt_ref, rs_ref, r_ref, c_ref, ge_ref, loss_ref, x_ref, v_hbm, vt_hbm,
                 g_hbm, ge_all, loss_all, x_all, vbuf, tbuf, obuf, part_ge, sum_ge, part_loss, in_sem, loc_sem, out_sem,
                 recv_sem, rs_out, rs_in, ag_out, ag_in, ls_out, ls_in, x_out, x_in, xf_out, xf_in, x_own):
    vp, dp = my_place()
    n_dev = n_vp * n_dp
    me = vp * n_dp + dp
    n_chip = n_dp // 2
    chip, core = dp // 2, dp % 2
    partner = chip * 2 + 1 - core
    rows, rows_t = zs_ref.shape[0], zt_ref.shape[0]
    n_img = rows // ALL_CROPS
    n_own = rows // n_dev
    n_loc = x_ref.shape[1]
    half = v_hbm.shape[1] // 2
    n_blk = FIRST
    base = core * half
    barrier = pltpu.get_barrier_semaphore()
    for k in range(1, n_dev):
        peer = (me + k) % n_dev
        pl.semaphore_signal(barrier, inc=1, device_id=(peer // n_dp, peer % n_dp), device_id_type=MESH)

    def load(j, slot):
        cols = pl.ds(pl.multiple_of(base + j * NB_B, NB_B), NB_B)
        return (pltpu.make_async_copy(v_hbm.at[:, cols], vbuf.at[slot], in_sem.at[0, slot]),
                pltpu.make_async_copy(vt_hbm.at[:, cols], tbuf.at[slot], in_sem.at[1, slot]))

    def local_store(j):
        slot = j % OUT_SLOTS
        cols = pl.ds(pl.multiple_of(base + j * NB_B, NB_B), NB_B)
        return pltpu.make_async_copy(obuf.at[slot], g_hbm.at[:, cols], loc_sem.at[slot])

    def remote_store(j):
        slot = j % OUT_SLOTS
        cols = pl.ds(pl.multiple_of(base + j * NB_B, NB_B), NB_B)
        return pltpu.make_async_remote_copy(
            src_ref=obuf.at[slot], dst_ref=g_hbm.at[:, cols], send_sem=out_sem.at[slot],
            recv_sem=recv_sem.at[j], device_id=(vp, partner), device_id_type=MESH)

    def peer_of(k):
        peer = (me + k) % n_dev
        return peer, (peer // n_dp, peer % n_dp)

    def scatter(k, peer, dst, device):
        return pltpu.make_async_remote_copy(
            src_ref=ge_ref.at[pl.ds(pl.multiple_of(peer * n_own, n_own), n_own)], dst_ref=part_ge.at[dst],
            send_sem=rs_out.at[k], recv_sem=rs_in.at[dst], device_id=device, device_id_type=MESH)

    def spread(k, owner, device):
        return pltpu.make_async_remote_copy(
            src_ref=sum_ge, dst_ref=ge_all.at[pl.ds(pl.multiple_of(owner * n_own, n_own), n_own)],
            send_sem=ag_out.at[k], recv_sem=ag_in.at[owner], device_id=device, device_id_type=MESH)

    def loss_send(k, dst, device):
        return pltpu.make_async_remote_copy(
            src_ref=loss_ref, dst_ref=part_loss.at[dst], send_sem=ls_out.at[k], recv_sem=ls_in.at[dst],
            device_id=device, device_id_type=MESH)

    def x_part(slot):
        return x_all.at[:, pl.ds(pl.multiple_of(slot * n_loc, n_loc), n_loc)]

    def x_send(k, src_chip, slot, device):
        return pltpu.make_async_remote_copy(
            src_ref=x_ref, dst_ref=x_part(slot), send_sem=x_out.at[k], recv_sem=x_in.at[src_chip],
            device_id=device, device_id_type=MESH)

    def x_forward(src_chip, slot):
        return pltpu.make_async_remote_copy(
            src_ref=x_part(slot), dst_ref=x_part(slot), send_sem=xf_out.at[src_chip], recv_sem=xf_in.at[src_chip],
            device_id=(vp, partner), device_id_type=MESH)

    for copy in load(0, 0):
        copy.start()
    x_local = pltpu.make_async_copy(x_ref, x_part(dp), x_own.at[0])
    x_local.start()
    bias, r_wide = row_weights(rs_ref, r_ref, rows, n_img)
    pl.semaphore_wait(barrier, n_dev - 1)
    for k in range(1, n_dev):
        peer, device = peer_of(k)
        loss_send(k, me, device).start()
        scatter(k, peer, me, device).start()
    for k in range(1, n_chip):
        x_send(k, chip, dp, (vp, ((chip + k) % n_chip) * 2 + core)).start()
    part_ge[me] = ge_ref[pl.ds(pl.multiple_of(me * n_own, n_own), n_own)]
    part_loss[me] = loss_ref[...]

    @pl.loop(0, n_blk)
    def _(j):
        slot = j % 2

        @pl.when(j + 1 < n_blk)
        def _():
            for copy in load(j + 1, 1 - slot):
                copy.start()

        @pl.when(j >= 1)
        def _():
            local_store(j - 1).start()
            remote_store(j - 1).start()

        @pl.when(j >= OUT_SLOTS)
        def _():
            local_store(j - OUT_SLOTS).wait()
            remote_store(j - OUT_SLOTS).wait_send()

        @pl.when(j == n_blk // 2)
        def _():
            for k in range(1, n_dev):
                src = (me + n_dev - k) % n_dev
                scatter(k, src, src, (vp, partner)).wait()
                loss_send(k, src, (vp, partner)).wait()
            total = part_ge[0]
            loss = part_loss[0]
            for k in range(1, n_dev):
                total = total + part_ge[k]
                loss = loss + part_loss[k]
            loss_all[...] = loss
            sum_ge[...] = total
            ge_all[pl.ds(pl.multiple_of(me * n_own, n_own), n_own)] = total

        @pl.when(j == n_blk // 2 + 1)
        def _():
            for k in range(1, n_dev):
                spread(k, me, peer_of(k)[1]).start()

        @pl.when(j == n_blk - 4)
        def _():
            x_local.wait()
            x_forward(chip, dp).start()
            for k in range(1, n_chip):
                src = (chip + n_chip - k) % n_chip
                x_send(k, src, src * 2 + core, (vp, partner)).wait()
                x_forward(src, src * 2 + core).start()

        for copy in load(j, slot):
            copy.wait()
        obuf[j % OUT_SLOTS] = grad_block(
            zs_ref, zst_ref, zt_ref, c_ref, bias, r_wide, vbuf[slot], tbuf[slot], base + j * NB_B, n_img)

    local_store(n_blk - 1).start()
    remote_store(n_blk - 1).start()
    for j in range(n_blk - OUT_SLOTS, n_blk):
        local_store(j).wait()
        remote_store(j).wait_send()
    for k in range(1, n_dev):
        src = (me + n_dev - k) % n_dev
        spread(k, src, (vp, partner)).wait()
    for src in range(n_chip):
        pltpu.make_async_remote_copy(
            src_ref=x_part(src * 2 + core), dst_ref=x_part(src * 2 + 1 - core), send_sem=xf_out.at[src],
            recv_sem=xf_in.at[src], device_id=(vp, partner), device_id_type=MESH).wait()

    @pl.loop(0, n_blk)
    def _(j):
        remote_store(j).wait_recv()


def proto_grads(z_s, z_st, z_t, row_sum, r_row, c_all, g_emb, loss, x_loc, protos, ema_protos, n_vp, n_dp):
    rows, width = z_s.shape
    n_col = protos.shape[1]
    n_blk = FIRST
    n_dev = n_vp * n_dp
    dma = pltpu.SemaphoreType.DMA
    return pl.pallas_call(
        functools.partial(grads_kernel, n_vp, n_dp),
        out_shape=(jax.ShapeDtypeStruct((width, n_col), F32),
                   jax.ShapeDtypeStruct((rows, width), F32),
                   jax.ShapeDtypeStruct((1, LANES), F32),
                   jax.ShapeDtypeStruct((x_loc.shape[0], x_loc.shape[1] * n_dp, x_loc.shape[2]), F32)),
        in_specs=[VMEM] * 9 + [HBM] * 2,
        out_specs=(HBM, VMEM, VMEM, HBM),
        scratch_shapes=[
            pltpu.VMEM((2, width, NB_B), BF16),
            pltpu.VMEM((2, width, NB_B), BF16),
            pltpu.VMEM((OUT_SLOTS, width, NB_B), F32),
            pltpu.VMEM((n_dev, rows // n_dev, width), F32),
            pltpu.VMEM((rows // n_dev, width), F32),
            pltpu.VMEM((n_dev, 1, LANES), F32),
            dma((2, 2)),
            dma((OUT_SLOTS,)),
            dma((OUT_SLOTS,)),
            dma((n_blk,)),
        ] + [dma((n_dev,))] * 6 + [dma((n_dp // 2,))] * 4 + [dma((1,))],
        compiler_params=pltpu.CompilerParams(
            collective_id=2, has_side_effects=True, vmem_limit_bytes=60 << 20),
        cost_estimate=pl.CostEstimate(
            flops=2 * rows * n_col * width, bytes_accessed=4 * width * n_col, transcendentals=rows * n_col // 2),
        name="proto_grads",
    )(z_s, z_st, z_t, row_sum, r_row, c_all, g_emb, loss, x_loc, protos, ema_protos)


def rest_kernel(core_ref, zs_ref, zst_ref, zt_ref, rs_ref, r_ref, c_ref, v_hbm, vt_hbm, src, dst,
                vbuf, tbuf, obuf, cbuf, in_sem, loc_sem, rd_sem, wr_sem):
    rows = zs_ref.shape[0]
    n_img = rows // ALL_CROPS
    half = v_hbm.shape[1] // 2
    n_blk = half // NB_B - FIRST
    base = core_ref[0] * half + FIRST * NB_B
    each = EARLY // n_blk

    def cols(j):
        return pl.ds(pl.multiple_of(base + j * NB_B, NB_B), NB_B)

    def load(j):
        slot = j % 2
        return (pltpu.make_async_copy(v_hbm.at[:, cols(j)], vbuf.at[slot], in_sem.at[0, slot]),
                pltpu.make_async_copy(vt_hbm.at[:, cols(j)], tbuf.at[slot], in_sem.at[1, slot]))

    def store(j):
        return pltpu.make_async_copy(obuf.at[j % 2], dst.at[:, cols(j)], loc_sem.at[j % 2])

    def piece(j, k):
        p = j * each + k
        start = (p // (EARLY // 2)) * half + (p % (EARLY // 2)) * NB_B
        return pl.ds(pl.multiple_of(start, NB_B), NB_B)

    def read(j, k):
        slot = j % 2
        return pltpu.make_async_copy(src.at[:, piece(j, k)], cbuf.at[slot, k], rd_sem.at[slot, k])

    def write(j, k):
        slot = j % 2
        return pltpu.make_async_copy(cbuf.at[slot, k], dst.at[:, piece(j, k)], wr_sem.at[slot, k])

    for copy in load(0):
        copy.start()
    bias, r_wide = row_weights(rs_ref, r_ref, rows, n_img)

    @pl.loop(0, n_blk)
    def _(j):
        slot = j % 2

        @pl.when(j + 1 < n_blk)
        def _():
            for copy in load(j + 1):
                copy.start()

        @pl.when(j >= 1)
        def _():
            for k in range(each):
                read(j - 1, k).wait()
                write(j - 1, k).start()

        @pl.when(j >= 2)
        def _():
            store(j - 2).wait()
            for k in range(each):
                write(j - 2, k).wait()

        for k in range(each):
            read(j, k).start()
        for copy in load(j):
            copy.wait()
        obuf[slot] = grad_block(
            zs_ref, zst_ref, zt_ref, c_ref, bias, r_wide, vbuf[slot], tbuf[slot], base + j * NB_B, n_img)
        store(j).start()

    last = n_blk - 1
    for k in range(each):
        read(last, k).wait()
        write(last, k).start()
    for j in (last - 1, last):
        store(j).wait()
        for k in range(each):
            write(j, k).wait()


def proto_rest(core, z_s, z_st, z_t, row_sum, r_row, c_all, protos, ema_protos, src):
    rows, width = z_s.shape
    n_col = protos.shape[1]
    n_blk = n_col // 2 // NB_B - FIRST
    each = EARLY // n_blk
    dma = pltpu.SemaphoreType.DMA
    return pl.pallas_call(
        rest_kernel,
        out_shape=jax.ShapeDtypeStruct((width, n_col), F32),
        in_specs=[pl.BlockSpec(memory_space=pltpu.SMEM)] + [VMEM] * 6 + [HBM] * 3,
        out_specs=HBM,
        scratch_shapes=[
            pltpu.VMEM((2, width, NB_B), BF16),
            pltpu.VMEM((2, width, NB_B), BF16),
            pltpu.VMEM((2, width, NB_B), F32),
            pltpu.VMEM((2, each, width, NB_B), F32),
            dma((2, 2)), dma((2,)), dma((2, each)), dma((2, each)),
        ],
        compiler_params=pltpu.CompilerParams(vmem_limit_bytes=60 << 20),
        cost_estimate=pl.CostEstimate(
            flops=rows * n_col * width, bytes_accessed=4 * width * n_col, transcendentals=rows * n_col // 4),
        name="proto_rest",
    )(core, z_s, z_st, z_t, row_sum, r_row, c_all, protos, ema_protos, src)


def head_kernel(x_hbm, wi_hbm, wm_hbm, wo_hbm, g_hbm, bi_ref, bm_ref, bo_ref, ge_ref,
                h1_hbm, h2_hbm, g2_hbm, g1_hbm, far_hbm, gp_ref, bias_ref,
                x_buf, wi, wm, wo, hid_one, hid_two, slope_one, slope_two, stage, grad_two, gp_stage, snd, rcv,
                ld_sem, loc_sem, out_sem, in_sem, gp_sem, bs_sem, far_out, far_in):
    vp, dp = my_place()
    chip, core = dp // 2, dp % 2
    partner = chip * 2 + 1 - core
    half, n_hid = hid_one.shape
    n_out = wo.shape[1]
    n_blk = n_hid // HB
    mine = pl.ds(pl.multiple_of(core * half, half), half)
    device = (vp, partner)
    barrier = pltpu.get_barrier_semaphore()
    pl.semaphore_signal(barrier, inc=1, device_id=device, device_id_type=MESH)
    loads = [pltpu.make_async_copy(x_hbm.at[mine], x_buf, ld_sem.at[0]),
             pltpu.make_async_copy(wi_hbm, wi, ld_sem.at[1]),
             pltpu.make_async_copy(wm_hbm, wm, ld_sem.at[2]),
             pltpu.make_async_copy(wo_hbm, wo, ld_sem.at[3])]
    for copy in loads:
        copy.start()
    n_far = far_hbm.shape[1] // NB_B
    own = core * (g_hbm.shape[1] // 2) + FIRST * NB_B

    def far(j):
        return pltpu.make_async_remote_copy(
            src_ref=g_hbm.at[:, pl.ds(pl.multiple_of(own + j * NB_B, NB_B), NB_B)],
            dst_ref=far_hbm.at[:, pl.ds(pl.multiple_of(j * NB_B, NB_B), NB_B)],
            send_sem=far_out.at[j], recv_sem=far_in.at[j], device_id=device, device_id_type=MESH)

    pl.semaphore_wait(barrier, 1)

    @pl.loop(0, n_far)
    def _(j):
        far(j).start()

    def block(j):
        return pl.ds(pl.multiple_of(j * HB, HB), HB)

    def keep(array, dst, j):
        return pltpu.make_async_copy(
            stage.at[array % 2, :, block(j)], dst.at[mine, block(j)], loc_sem.at[array, j])

    def send(array, dst, j):
        return pltpu.make_async_remote_copy(
            src_ref=stage.at[array % 2, :, block(j)], dst_ref=dst.at[mine, block(j)], send_sem=out_sem.at[array, j],
            recv_sem=in_sem.at[array, j], device_id=device, device_id_type=MESH)

    def flush(array, dst, j):
        keep(array, dst, j).start()
        send(array, dst, j).start()

    def drain(array, dst):
        @pl.loop(0, n_blk)
        def _(j):
            keep(array, dst, j).wait()
            send(array, dst, j).wait_send()

    def layer(array, feats, weight, b_ref, hid, slope, dst):
        @pl.loop(0, n_blk)
        def _(j):
            @pl.when(j >= 1)
            def _():
                flush(array, dst, j - 1)

            pre = dot(feats, weight[:, block(j)]) + b_ref[:, block(j)].astype(F32)
            cdf = 0.5 * (1.0 + lax.erf(pre * 0.7071067811865476))
            low = (pre * cdf).astype(BF16)
            hid[:, block(j)] = low
            stage[array % 2, :, block(j)] = low.astype(F32)
            slope[:, block(j)] = cdf + pre * jnp.exp(-0.5 * pre * pre) * 0.3989422804014327
        flush(array, dst, n_blk - 1)

    loads[0].wait()
    loads[1].wait()
    layer(0, x_buf[...].astype(BF16), wi, bi_ref, hid_one, slope_one, h1_hbm)
    loads[2].wait()
    layer(1, hid_one[...], wm, bm_ref, hid_two, slope_two, h2_hbm)
    loads[3].wait()
    proj = dot(hid_two[...], wo[...]) + bo_ref[...].astype(F32)
    inv_norm = lax.rsqrt(jnp.sum(proj * proj, axis=-1, keepdims=True))
    unit = proj * inv_norm
    g_emb = ge_ref[mine]
    g_proj = (g_emb - unit * jnp.sum(unit * g_emb, axis=-1, keepdims=True)) * inv_norm
    gp_low = g_proj.astype(BF16)
    gp_stage[...] = gp_low.astype(F32)
    gp_ref[mine] = gp_low.astype(F32)
    snd[:, 2 * n_hid:] = jnp.sum(g_proj, axis=0, keepdims=True)
    drain(0, h1_hbm)

    @pl.loop(0, n_blk)
    def _(j):
        @pl.when(j >= 1)
        def _():
            flush(2, g2_hbm, j - 1)

        g_hid = dot_t(gp_low, wo[block(j), :])
        g_pre = g_hid.astype(BF16).astype(F32) * slope_two[:, block(j)]
        snd[:, block(j)] = jnp.sum(g_pre, axis=0, keepdims=True)
        low = g_pre.astype(BF16)
        grad_two[:, block(j)] = low
        stage[0, :, block(j)] = low.astype(F32)
    flush(2, g2_hbm, n_blk - 1)
    gp_send = pltpu.make_async_remote_copy(
        src_ref=gp_stage, dst_ref=gp_ref.at[mine], send_sem=gp_sem.at[0], recv_sem=gp_sem.at[1],
        device_id=device, device_id_type=MESH)
    gp_send.start()
    drain(1, h2_hbm)

    @pl.loop(0, n_blk)
    def _(j):
        @pl.when(j >= 1)
        def _():
            flush(3, g1_hbm, j - 1)

        g_hid = dot_t(grad_two[...], wm[block(j), :])
        g_pre = g_hid.astype(BF16).astype(F32) * slope_one[:, block(j)]
        snd[:, pl.ds(pl.multiple_of(n_hid + j * HB, HB), HB)] = jnp.sum(g_pre, axis=0, keepdims=True)
        stage[1, :, block(j)] = g_pre.astype(BF16).astype(F32)
    flush(3, g1_hbm, n_blk - 1)
    bias_send = pltpu.make_async_remote_copy(
        src_ref=snd, dst_ref=rcv, send_sem=bs_sem.at[0], recv_sem=bs_sem.at[1],
        device_id=device, device_id_type=MESH)
    bias_send.start()
    drain(2, g2_hbm)
    drain(3, g1_hbm)
    gp_send.wait()
    bias_send.wait()
    bias_ref[...] = snd[...] + rcv[...]
    for array, dst in enumerate((h1_hbm, h2_hbm, g2_hbm, g1_hbm)):
        @pl.loop(0, n_blk)
        def _(j):
            send(array, dst, j).wait_recv()

    @pl.loop(0, n_far)
    def _(j):
        far(j).wait()


def head_pass(x_all, w_in, b_in, w_mid, b_mid, w_out, b_out, g_emb, g_protos):
    rows, feat = x_all.shape
    n_hid, n_out = w_out.shape
    half = rows // 2
    n_blk = n_hid // HB
    n_bias = 2 * n_hid + n_out
    dma = pltpu.SemaphoreType.DMA
    wide = jax.ShapeDtypeStruct((rows, n_hid), F32)
    n_far = g_protos.shape[1] // 2 // NB_B - FIRST
    far = jax.ShapeDtypeStruct((g_protos.shape[0], n_far * NB_B), F32)
    return pl.pallas_call(
        head_kernel,
        out_shape=(wide, wide, wide, wide, far, jax.ShapeDtypeStruct((rows, n_out), F32),
                   jax.ShapeDtypeStruct((1, n_bias), F32)),
        in_specs=[HBM] * 5 + [VMEM] * 4,
        out_specs=(HBM,) * 5 + (VMEM,) * 2,
        scratch_shapes=[
            pltpu.VMEM((half, feat), F32),
            pltpu.VMEM((feat, n_hid), BF16),
            pltpu.VMEM((n_hid, n_hid), BF16),
            pltpu.VMEM((n_hid, n_out), BF16),
            pltpu.VMEM((half, n_hid), BF16),
            pltpu.VMEM((half, n_hid), BF16),
            pltpu.VMEM((half, n_hid), F32),
            pltpu.VMEM((half, n_hid), F32),
            pltpu.VMEM((2, half, n_hid), F32),
            pltpu.VMEM((half, n_hid), BF16),
            pltpu.VMEM((half, n_out), F32),
            pltpu.VMEM((1, n_bias), F32),
            pltpu.VMEM((1, n_bias), F32),
            dma((4,)), dma((4, n_blk)), dma((4, n_blk)), dma((4, n_blk)), dma((2,)), dma((2,)), dma((n_far,)), dma((n_far,)),
        ],
        compiler_params=pltpu.CompilerParams(
            collective_id=3, has_side_effects=True, vmem_limit_bytes=63 << 20),
        cost_estimate=pl.CostEstimate(
            flops=2 * rows * (feat + 2 * n_hid) * n_hid, bytes_accessed=16 * rows * n_hid, transcendentals=2 * rows * n_hid),
        name="head_pass",
    )(x_all, w_in, w_mid, w_out, g_protos, b_in.reshape(1, -1), b_mid.reshape(1, -1), b_out.reshape(1, -1), g_emb)


def wgrad_kernel(n_step, src_at, dst_at, skip, core_ref, a_ref, b_ref, src, _, out_ref, dst, low, cbuf, rd_sem, wr_sem):
    i = pl.program_id(0)
    chunk = cbuf.shape[2]
    target = dst_at + (1 - core_ref[0]) * skip

    def read(step):
        cols = pl.ds(pl.multiple_of(src_at + step * chunk, LANES), chunk)
        return pltpu.make_async_copy(src.at[:, cols], cbuf.at[step % 3], rd_sem.at[step % 3])

    def write(step):
        cols = pl.ds(pl.multiple_of(target + step * chunk, LANES), chunk)
        return pltpu.make_async_copy(cbuf.at[step % 3], dst.at[:, cols], wr_sem.at[step % 3])

    @pl.when(i == 0)
    def _():
        read(0).start()
        low[...] = b_ref[...].astype(BF16)

    @pl.when(i >= 2)
    def _():
        write(i - 2).wait()

    @pl.when(i + 1 < n_step)
    def _():
        read(i + 1).start()

    read(i).wait()
    write(i).start()
    out_ref[...] = lax.dot_general(
        a_ref[...].astype(BF16), low[...], (((0,), (0,)), ((), ())), preferred_element_type=F32)

    @pl.when(i == n_step - 1)
    def _():
        write(i - 1).wait()
        write(i).wait()


def wgrad(core, left, right, src, dst, src_at, dst_at, skip, width, block):
    rows, n_left = left.shape
    n_right = right.shape[1]
    n_step = n_left // block
    chunk = width // n_step
    return pl.pallas_call(
        functools.partial(wgrad_kernel, n_step, src_at, dst_at, skip),
        grid=(n_step,),
        out_shape=(jax.ShapeDtypeStruct((n_left, n_right), F32), jax.ShapeDtypeStruct(dst.shape, F32)),
        in_specs=[pl.BlockSpec(memory_space=pltpu.SMEM),
                  pl.BlockSpec((rows, block), lambda i: (0, i)),
                  pl.BlockSpec((rows, n_right), lambda i: (0, 0), pipeline_mode=pl.Buffered(1)),
                  HBM, HBM],
        out_specs=(pl.BlockSpec((block, n_right), lambda i: (i, 0)), HBM),
        scratch_shapes=[pltpu.VMEM((rows, n_right), BF16),
                        pltpu.VMEM((3, src.shape[0], chunk), F32),
                        pltpu.SemaphoreType.DMA((3,)), pltpu.SemaphoreType.DMA((3,))],
        input_output_aliases={4: 1},
        compiler_params=pltpu.CompilerParams(
            dimension_semantics=("arbitrary",), vmem_limit_bytes=60 << 20),
        cost_estimate=pl.CostEstimate(
            flops=2 * rows * n_left * n_right, bytes_accessed=8 * src.shape[0] * width, transcendentals=0),
        name="wgrad",
    )(core, left, right, src, dst)


def solution(mesh):
    n_vp = mesh.shape['vp']
    n_dp = mesh.shape['dp']

    def local_step(student_x, teacher_x, w_in, b_in, w_mid, b_mid, w_out, b_out, protos,
                   ema_w_in, ema_b_in, ema_w_mid, ema_b_mid, ema_w_out, ema_b_out, ema_protos):
        rows, feat = student_x.shape
        n_img = rows // ALL_CROPS
        width = protos.shape[0]
        x_loc = student_x.reshape(n_img, ALL_CROPS, feat).transpose(1, 0, 2)
        t_loc = teacher_x.reshape(n_img, GLOBAL_CROPS, feat).transpose(1, 0, 2).reshape(-1, feat)
        t_emb = mlp_forward(t_loc, ema_w_in, ema_b_in, ema_w_mid, ema_b_mid, ema_w_out, ema_b_out)
        s_emb = mlp_forward(x_loc.reshape(rows, feat), w_in, b_in, w_mid, b_mid, w_out, b_out)
        z_loc = jnp.concatenate([s_emb, t_emb], axis=0).reshape(ALL_CROPS + GLOBAL_CROPS, n_img, width)
        z_all = gather_dp(z_loc, n_dp, 0).reshape(-1, width).astype(BF16)
        z_s, z_t = z_all[:rows * n_dp], z_all[rows * n_dp:]
        c_all, row_sum, r_row, g_emb, loss = sinkhorn_stats(z_s, z_t, protos, ema_protos, n_vp, n_dp)
        z_st = z_s.T
        core = (lax.axis_index('dp') % 2).astype(jnp.int32).reshape(1)
        g_temp, g_emb, loss, x_all = proto_grads(
            z_s, z_st, z_t, row_sum, r_row, c_all, g_emb, loss, x_loc.astype(F32), protos, ema_protos, n_vp, n_dp)
        g_protos = proto_rest(core, z_s, z_st, z_t, row_sum, r_row, c_all, protos, ema_protos, g_temp)
        x_all = x_all.reshape(rows * n_dp, feat)
        hid_one, hid_two, g_two, g_one, g_far, g_proj, biases = head_pass(
            x_all, w_in, b_in, w_mid, b_mid, w_out, b_out, g_emb, g_protos)
        n_hid = w_mid.shape[0]
        half = protos.shape[1] // 2
        done, late = (EARLY // 2) * NB_B, (FIRST - EARLY // 2) * NB_B
        g_w_mid, g_protos = wgrad(
            core, hid_one, g_two, g_far, g_protos, 0, FIRST * NB_B, half, g_far.shape[1], 256)
        g_w_in, g_protos = wgrad(core, x_all, g_one, g_temp, g_protos, done, done, 0, late, 384)
        g_w_out, g_protos = wgrad(core, hid_two, g_proj, g_temp, g_protos, half + done, half + done, 0, late, 256)
        biases = biases.reshape(-1)
        g_b_mid, g_b_in, g_b_out = biases[:n_hid], biases[n_hid:2 * n_hid], biases[2 * n_hid:]
        return (jnp.sum(loss), g_w_in, g_b_in, g_w_mid, g_b_mid, g_w_out, g_b_out, g_protos)

    by_rows = P('dp', None)
    by_cols = P(None, 'vp')
    replicated = P()
    head_specs = (replicated,) * 6
    in_specs = (by_rows, by_rows) + head_specs + (by_cols,) + head_specs + (by_cols,)
    out_specs = (replicated,) * 7 + (by_cols,)
    return jax.shard_map(local_step, mesh=mesh, in_specs=in_specs, out_specs=out_specs, check_vma=False)
```

```python
import functools

import jax
import jax.numpy as jnp
from jax import lax
from jax.experimental import pallas as pl
from jax.experimental.pallas import tpu as pltpu
from jax.sharding import PartitionSpec as P

ALL_CROPS = 10
GLOBAL_CROPS = 2
TEMP_STUDENT = 0.1
TEMP_TEACHER = 0.04
LOG2E = 1.4426950408889634
LANES = 128
NB_A = 1024
NB_B = 1024
OUT_SLOTS = 3
HB = 256
F32 = jnp.float32
BF16 = jnp.bfloat16
MESH = pl.DeviceIdType.MESH
HBM = pl.BlockSpec(memory_space=pl.ANY)
VMEM = pl.BlockSpec(memory_space=pltpu.VMEM)


def mlp_forward(feats, w_in, b_in, w_mid, b_mid, w_out, b_out):
    pre_one = jnp.dot(feats, w_in, preferred_element_type=F32) + b_in.astype(F32)
    hid_one = jax.nn.gelu(pre_one, approximate=False).astype(BF16)
    pre_two = jnp.dot(hid_one, w_mid, preferred_element_type=F32) + b_mid.astype(F32)
    hid_two = jax.nn.gelu(pre_two, approximate=False).astype(BF16)
    proj = jnp.dot(hid_two, w_out, preferred_element_type=F32) + b_out.astype(F32)
    inv_norm = lax.rsqrt(jnp.sum(proj * proj, axis=-1, keepdims=True))
    return proj * inv_norm


def unit_columns(block):
    block_f = block.astype(F32)
    inv_col = lax.rsqrt(jnp.sum(block_f * block_f, axis=0, keepdims=True))
    return block_f * inv_col, inv_col


def dot(left, right):
    return jnp.dot(left, right, preferred_element_type=F32)


def dot_t(left, right):
    return lax.dot_general(left, right, (((1,), (1,)), ((), ())), preferred_element_type=F32)


def to_column(row):
    return jnp.transpose(jnp.broadcast_to(row, (LANES, row.shape[1])))


def to_row(acc):
    return jnp.sum(jnp.transpose(acc), axis=0, keepdims=True)


def fold_lanes(wide):
    total = wide[:, :LANES]
    for start in range(LANES, wide.shape[1], LANES):
        total = total + wide[:, start:start + LANES]
    return total


def my_place():
    return lax.axis_index('vp'), lax.axis_index('dp')


def gather_kernel(n_dp, block_ref, all_ref, out_sem, in_sem, fwd_out, fwd_in):
    vp, me = my_place()
    n_chip = n_dp // 2
    chip, core = me // 2, me % 2
    partner = chip * 2 + 1 - core
    n_row = block_ref.shape[1]

    def part(slot):
        return all_ref.at[:, pl.ds(pl.multiple_of(slot * n_row, n_row), n_row)]

    barrier = pltpu.get_barrier_semaphore()
    pl.semaphore_signal(barrier, inc=1, device_id=(vp, partner), device_id_type=MESH)
    for k in range(1, n_chip):
        peer = ((chip + k) % n_chip) * 2 + core
        pl.semaphore_signal(barrier, inc=1, device_id=(vp, peer), device_id_type=MESH)
    pl.semaphore_wait(barrier, n_chip)
    sends = []
    for k in range(1, n_chip):
        peer = ((chip + k) % n_chip) * 2 + core
        sends.append(pltpu.make_async_remote_copy(
            src_ref=block_ref, dst_ref=part(me), send_sem=out_sem.at[k], recv_sem=in_sem.at[chip],
            device_id=(vp, peer), device_id_type=MESH))
    own = pltpu.make_async_remote_copy(
        src_ref=block_ref, dst_ref=part(me), send_sem=fwd_out.at[chip], recv_sem=fwd_in.at[chip],
        device_id=(vp, partner), device_id_type=MESH)
    for copy in sends:
        copy.start()
    own.start()
    all_ref[:, pl.ds(pl.multiple_of(me * n_row, n_row), n_row)] = block_ref[...]
    for k in range(1, n_chip):
        src = (chip + n_chip - k) % n_chip
        slot = src * 2 + core
        peer_copy = pltpu.make_async_remote_copy(
            src_ref=block_ref, dst_ref=part(slot), send_sem=out_sem.at[k], recv_sem=in_sem.at[src],
            device_id=(vp, partner), device_id_type=MESH)
        peer_copy.wait_recv()
        forward = pltpu.make_async_remote_copy(
            src_ref=part(slot), dst_ref=part(slot), send_sem=fwd_out.at[src], recv_sem=fwd_in.at[src],
            device_id=(vp, partner), device_id_type=MESH)
        forward.start()
    for copy in sends:
        copy.wait_send()
    for src in range(n_chip):
        slot = src * 2 + core
        other = src * 2 + 1 - core
        pltpu.make_async_remote_copy(
            src_ref=part(slot), dst_ref=part(other), send_sem=fwd_out.at[src], recv_sem=fwd_in.at[src],
            device_id=(vp, partner), device_id_type=MESH).wait()


def gather_dp(block, n_dp, collective_id):
    groups, n_row, width = block.shape
    return pl.pallas_call(
        functools.partial(gather_kernel, n_dp),
        out_shape=jax.ShapeDtypeStruct((groups, n_row * n_dp, width), block.dtype),
        in_specs=[VMEM],
        out_specs=VMEM,
        scratch_shapes=[pltpu.SemaphoreType.DMA((n_dp // 2,))] * 4,
        compiler_params=pltpu.CompilerParams(
            collective_id=collective_id, has_side_effects=True, vmem_limit_bytes=48 << 20),
        name="gather_dp",
    )(block)


def stats_kernel(n_vp, n_dp, zs_ref, zt_ref, v_hbm, vt_hbm, c_ref, rs_ref, r_ref, ge_ref, loss_ref,
                 vbuf, tbuf, in_sem, ubuf, kbuf, acc_s, acc_r, wbuf, snd, rcv, send_sem, recv_sem, c_out, c_in):
    vp, dp = my_place()
    n_dev = n_vp * n_dp
    me = vp * n_dp + dp
    rows, rows_t = zs_ref.shape[0], zt_ref.shape[0]
    n_img = rows // ALL_CROPS
    n_col = kbuf.shape[1]
    n_blk = n_col // NB_A
    base = dp * n_col

    barrier = pltpu.get_barrier_semaphore()
    for k in range(1, n_dev):
        peer = (me + k) % n_dev
        pl.semaphore_signal(barrier, inc=1, device_id=(peer // n_dp, peer % n_dp), device_id_type=MESH)

    def load(which, j):
        src, buf = ((v_hbm, vbuf), (vt_hbm, tbuf))[which]
        cols = pl.ds(pl.multiple_of(base + j * NB_A, NB_A), NB_A)
        return pltpu.make_async_copy(src.at[:, cols], buf.at[j % 2], in_sem.at[which, j % 2])

    load(1, 0).start()
    load(0, 0).start()
    acc_s[...] = jnp.zeros_like(acc_s)
    acc_r[...] = jnp.zeros_like(acc_r)
    ge_ref[...] = jnp.zeros_like(ge_ref)

    @pl.loop(0, n_blk)
    def _(j):
        @pl.when(j + 1 < n_blk)
        def _():
            load(1, j + 1).start()

        load(1, j).wait()
        unit_t = unit_columns(tbuf[j % 2])[0].astype(BF16)
        kern = jnp.exp2(dot(zt_ref[...], unit_t) * (LOG2E / TEMP_TEACHER))
        kbuf[:, pl.ds(pl.multiple_of(j * NB_A, NB_A), NB_A)] = kern
        acc_r[...] += fold_lanes(kern * (1.0 / jnp.sum(kern, axis=0, keepdims=True)))

    pl.semaphore_wait(barrier, n_dev - 1)

    def message(step, k, dst, peer, width):
        return pltpu.make_async_remote_copy(
            src_ref=snd.at[step, :, :width], dst_ref=rcv.at[step, dst, :, :width],
            send_sem=send_sem.at[step, k], recv_sem=recv_sem.at[step, dst],
            device_id=(peer // n_dp, peer % n_dp), device_id_type=MESH)

    def publish(step, value):
        width = value.shape[1]
        snd[step, :, :width] = value
        for k in range(1, n_dev):
            message(step, k, me, (me + k) % n_dev, width).start()
        rcv[step, me, :, :width] = value

    def collect(step, width):
        for k in range(1, n_dev):
            src = (me + n_dev - k) % n_dev
            message(step, k, src, src, width).wait()
        total = rcv[step, 0, :, :width]
        for k in range(1, n_dev):
            total = total + rcv[step, k, :, :width]
        return total

    def rescale(r_row, keep):
        r_col = to_column(r_row)
        acc_r[...] = jnp.zeros_like(acc_r)
        span = 4 * LANES

        @pl.loop(0, n_col // span)
        def _(j):
            total = acc_r[...]
            for k in range(4):
                here = pl.ds(pl.multiple_of(j * span + k * LANES, LANES), LANES)
                kern = kbuf[:, here]
                c_row = 1.0 / jnp.sum(kern * r_col, axis=0, keepdims=True)
                total = total + kern * c_row
                if keep:
                    c_ref[dp, :, here] = c_row
            acc_r[...] = total

    third = (n_blk * 3) // 8
    publish(0, to_row(acc_r[...]))

    @pl.loop(0, n_blk)
    def _(j):
        @pl.when(j + 1 < n_blk)
        def _():
            load(0, j + 1).start()

        @pl.when(j == third)
        def _():
            rescale(1.0 / collect(0, rows_t), False)
            publish(1, to_row(acc_r[...]))

        @pl.when(j == 2 * third)
        def _():
            rescale(1.0 / collect(1, rows_t), True)
            publish(2, to_row(acc_r[...]))
            for k in range(1, n_dp):
                pltpu.make_async_remote_copy(
                    src_ref=c_ref.at[dp], dst_ref=c_ref.at[dp], send_sem=c_out.at[k], recv_sem=c_in.at[dp],
                    device_id=(vp, (dp + k) % n_dp), device_id_type=MESH).start()

        load(0, j).wait()
        unit = unit_columns(vbuf[j % 2])[0].astype(BF16)
        ubuf[:, pl.ds(pl.multiple_of(j * NB_A, NB_A), NB_A)] = unit
        exp_s = jnp.exp2(dot(zs_ref[...], unit) * (LOG2E / TEMP_STUDENT))
        acc_s[...] += fold_lanes(exp_s)
        ge_ref[...] += dot_t(exp_s.astype(BF16), unit)

    publish(3, to_row(acc_s[...]))
    r_row = 1.0 / collect(2, rows_t)
    r_ref[...] = r_row

    r_col = to_column(r_row)
    r_wide = jnp.concatenate([r_col] * (NB_A // LANES), axis=1)
    wbuf[...] = jnp.zeros_like(wbuf)

    @pl.loop(0, n_blk)
    def _(j):
        here = pl.ds(pl.multiple_of(j * NB_A, NB_A), NB_A)
        q_mat = kbuf[:, here] * c_ref[dp, :, here] * r_wide
        q_hi = q_mat.astype(BF16)
        q_lo = (q_mat - q_hi.astype(F32)).astype(BF16)
        both = dot_t(jnp.concatenate([q_hi, q_lo], axis=0), ubuf[:, here])
        wbuf[...] += both[:rows_t] + both[rows_t:]

    row_sum = collect(3, rows)
    rs_ref[...] = row_sum
    w_zero = wbuf[:n_img]
    w_one = wbuf[n_img:]
    w_both = w_zero + w_one
    scale = 1.0 / (n_img * GLOBAL_CROPS * (ALL_CROPS - 1))
    log_rs = jnp.log(row_sum)
    inv_rs = to_column(1.0 / row_sum)
    loss = jnp.zeros((1, LANES), F32)
    for v in range(ALL_CROPS):
        block = pl.ds(v * n_img, n_img)
        count = float(GLOBAL_CROPS - (v < GLOBAL_CROPS))
        w_v = (w_one, w_zero)[v] if v < GLOBAL_CROPS else w_both
        inv = inv_rs[v * n_img:(v + 1) * n_img]
        inv = jnp.concatenate([inv] * (ge_ref.shape[1] // LANES), axis=1)
        dots = fold_lanes(jnp.sum(zs_ref[block].astype(F32) * w_v, axis=0, keepdims=True))
        logs = log_rs[:, v * n_img:(v + 1) * n_img]
        loss += (count / n_dev) * logs - (1.0 / TEMP_STUDENT) * dots
        ge_ref[block] = (count * (ge_ref[block] * inv) - w_v) * (scale / TEMP_STUDENT)
    loss_ref[...] = loss * scale

    for k in range(1, n_dp):
        src = (dp + n_dp - k) % n_dp
        pltpu.make_async_remote_copy(
            src_ref=c_ref.at[dp], dst_ref=c_ref.at[src], send_sem=c_out.at[k], recv_sem=c_in.at[src],
            device_id=(vp, src), device_id_type=MESH).wait()


def sinkhorn_stats(z_s, z_t, protos, ema_protos, n_vp, n_dp):
    rows, width = z_s.shape
    rows_t = z_t.shape[0]
    n_col = protos.shape[1] // n_dp
    n_dev = n_vp * n_dp
    flops = 2 * rows * n_col * width * 2
    return pl.pallas_call(
        functools.partial(stats_kernel, n_vp, n_dp),
        out_shape=(jax.ShapeDtypeStruct((n_dp, 1, n_col), F32),
                   jax.ShapeDtypeStruct((1, rows), F32),
                   jax.ShapeDtypeStruct((1, rows_t), F32),
                   jax.ShapeDtypeStruct((rows, width), F32),
                   jax.ShapeDtypeStruct((1, LANES), F32)),
        in_specs=[VMEM, VMEM, HBM, HBM],
        out_specs=(VMEM,) * 5,
        scratch_shapes=[
            pltpu.VMEM((2, width, NB_A), BF16),
            pltpu.VMEM((2, width, NB_A), BF16),
            pltpu.SemaphoreType.DMA((2, 2)),
            pltpu.VMEM((width, n_col), BF16),
            pltpu.VMEM((rows_t, n_col), F32),
            pltpu.VMEM((rows, LANES), F32),
            pltpu.VMEM((rows_t, LANES), F32),
            pltpu.VMEM((rows_t, width), F32),
            pltpu.VMEM((4, 1, rows), F32),
            pltpu.VMEM((4, n_dev, 1, rows), F32),
            pltpu.SemaphoreType.DMA((4, n_dev)),
            pltpu.SemaphoreType.DMA((4, n_dev)),
            pltpu.SemaphoreType.DMA((n_dp,)),
            pltpu.SemaphoreType.DMA((n_dp,)),
        ],
        compiler_params=pltpu.CompilerParams(
            collective_id=1, has_side_effects=True, vmem_limit_bytes=60 << 20),
        cost_estimate=pl.CostEstimate(flops=flops, bytes_accessed=4 * width * n_col, transcendentals=rows * n_col),
        name="sinkhorn_stats",
    )(z_s, z_t, protos, ema_protos)


def grads_kernel(n_vp, n_dp, zs_ref, zst_ref, zt_ref, rs_ref, r_ref, c_ref, ge_ref, loss_ref, x_ref, v_hbm, vt_hbm,
                 g_hbm, ge_all, loss_all, x_all, vbuf, tbuf, obuf, part_ge, sum_ge, part_loss, in_sem, loc_sem, out_sem,
                 recv_sem, rs_out, rs_in, ag_out, ag_in, ls_out, ls_in, x_out, x_in, xf_out, xf_in, x_own):
    vp, dp = my_place()
    n_dev = n_vp * n_dp
    me = vp * n_dp + dp
    n_chip = n_dp // 2
    chip, core = dp // 2, dp % 2
    partner = chip * 2 + 1 - core
    rows, rows_t = zs_ref.shape[0], zt_ref.shape[0]
    n_img = rows // ALL_CROPS
    n_own = rows // n_dev
    n_loc = x_ref.shape[1]
    half = v_hbm.shape[1] // 2
    n_slice = c_ref.shape[2]
    n_blk = half // NB_B
    base = core * half
    barrier = pltpu.get_barrier_semaphore()
    for k in range(1, n_dev):
        peer = (me + k) % n_dev
        pl.semaphore_signal(barrier, inc=1, device_id=(peer // n_dp, peer % n_dp), device_id_type=MESH)

    def load(j, slot):
        cols = pl.ds(pl.multiple_of(base + j * NB_B, NB_B), NB_B)
        return (pltpu.make_async_copy(v_hbm.at[:, cols], vbuf.at[slot], in_sem.at[0, slot]),
                pltpu.make_async_copy(vt_hbm.at[:, cols], tbuf.at[slot], in_sem.at[1, slot]))

    def local_store(j):
        slot = j % OUT_SLOTS
        cols = pl.ds(pl.multiple_of(base + j * NB_B, NB_B), NB_B)
        return pltpu.make_async_copy(obuf.at[slot], g_hbm.at[:, cols], loc_sem.at[slot])

    def remote_store(j):
        slot = j % OUT_SLOTS
        cols = pl.ds(pl.multiple_of(base + j * NB_B, NB_B), NB_B)
        return pltpu.make_async_remote_copy(
            src_ref=obuf.at[slot], dst_ref=g_hbm.at[:, cols], send_sem=out_sem.at[slot],
            recv_sem=recv_sem.at[j], device_id=(vp, partner), device_id_type=MESH)

    def peer_of(k):
        peer = (me + k) % n_dev
        return peer, (peer // n_dp, peer % n_dp)

    def scatter(k, peer, dst, device):
        return pltpu.make_async_remote_copy(
            src_ref=ge_ref.at[pl.ds(pl.multiple_of(peer * n_own, n_own), n_own)], dst_ref=part_ge.at[dst],
            send_sem=rs_out.at[k], recv_sem=rs_in.at[dst], device_id=device, device_id_type=MESH)

    def spread(k, owner, device):
        return pltpu.make_async_remote_copy(
            src_ref=sum_ge, dst_ref=ge_all.at[pl.ds(pl.multiple_of(owner * n_own, n_own), n_own)],
            send_sem=ag_out.at[k], recv_sem=ag_in.at[owner], device_id=device, device_id_type=MESH)

    def loss_send(k, dst, device):
        return pltpu.make_async_remote_copy(
            src_ref=loss_ref, dst_ref=part_loss.at[dst], send_sem=ls_out.at[k], recv_sem=ls_in.at[dst],
            device_id=device, device_id_type=MESH)

    def x_part(slot):
        return x_all.at[:, pl.ds(pl.multiple_of(slot * n_loc, n_loc), n_loc)]

    def x_send(k, src_chip, slot, device):
        return pltpu.make_async_remote_copy(
            src_ref=x_ref, dst_ref=x_part(slot), send_sem=x_out.at[k], recv_sem=x_in.at[src_chip],
            device_id=device, device_id_type=MESH)

    def x_forward(src_chip, slot):
        return pltpu.make_async_remote_copy(
            src_ref=x_part(slot), dst_ref=x_part(slot), send_sem=xf_out.at[src_chip], recv_sem=xf_in.at[src_chip],
            device_id=(vp, partner), device_id_type=MESH)

    for copy in load(0, 0):
        copy.start()
    x_local = pltpu.make_async_copy(x_ref, x_part(dp), x_own.at[0])
    x_local.start()
    scale = 1.0 / (n_img * GLOBAL_CROPS * (ALL_CROPS - 1)) / TEMP_STUDENT
    lanes = lax.broadcasted_iota(jnp.int32, (1, rows), 1)
    weight = jnp.where(lanes < GLOBAL_CROPS * n_img, scale, GLOBAL_CROPS * scale)
    bias = to_column(jnp.log(weight / rs_ref[...]) * LOG2E)
    bias = jnp.concatenate([bias] * (NB_B // LANES), axis=1)
    r_col = to_column(r_ref[...] * scale)
    r_wide = jnp.concatenate([r_col] * (NB_B // LANES), axis=1)
    pl.semaphore_wait(barrier, n_dev - 1)
    for k in range(1, n_dev):
        peer, device = peer_of(k)
        loss_send(k, me, device).start()
        scatter(k, peer, me, device).start()
    for k in range(1, n_chip):
        x_send(k, chip, dp, (vp, ((chip + k) % n_chip) * 2 + core)).start()
    part_ge[me] = ge_ref[pl.ds(pl.multiple_of(me * n_own, n_own), n_own)]
    part_loss[me] = loss_ref[...]

    @pl.loop(0, n_blk)
    def _(j):
        slot = j % 2

        @pl.when(j + 1 < n_blk)
        def _():
            for copy in load(j + 1, 1 - slot):
                copy.start()

        @pl.when(j >= 1)
        def _():
            local_store(j - 1).start()
            remote_store(j - 1).start()

        @pl.when(j >= OUT_SLOTS)
        def _():
            local_store(j - OUT_SLOTS).wait()
            remote_store(j - OUT_SLOTS).wait_send()

        @pl.when(j == n_blk // 2)
        def _():
            for k in range(1, n_dev):
                src = (me + n_dev - k) % n_dev
                scatter(k, src, src, (vp, partner)).wait()
                loss_send(k, src, (vp, partner)).wait()
            total = part_ge[0]
            loss = part_loss[0]
            for k in range(1, n_dev):
                total = total + part_ge[k]
                loss = loss + part_loss[k]
            loss_all[...] = loss
            sum_ge[...] = total
            ge_all[pl.ds(pl.multiple_of(me * n_own, n_own), n_own)] = total

        @pl.when(j == n_blk // 2 + 1)
        def _():
            for k in range(1, n_dev):
                spread(k, me, peer_of(k)[1]).start()

        @pl.when(j == n_blk - 4)
        def _():
            x_local.wait()
            x_forward(chip, dp).start()
            for k in range(1, n_chip):
                src = (chip + n_chip - k) % n_chip
                x_send(k, src, src * 2 + core, (vp, partner)).wait()
                x_forward(src, src * 2 + core).start()

        for copy in load(j, slot):
            copy.wait()
        unit_t = unit_columns(tbuf[slot])[0].astype(BF16)
        col = base + j * NB_B
        c_row = c_ref[col // n_slice, :, pl.ds(pl.multiple_of(col % n_slice, NB_B), NB_B)]
        q_mat = jnp.exp2(dot(zt_ref[...], unit_t) * (LOG2E / TEMP_TEACHER)) * c_row * r_wide
        q_zero, q_one = q_mat[:n_img], q_mat[n_img:]
        q_both = q_zero + q_one
        unit, inv_col = unit_columns(vbuf[slot])
        logits = dot(zs_ref[...], unit.astype(BF16))
        soft = jnp.exp2(logits * (LOG2E / TEMP_STUDENT) + bias)
        target = jnp.concatenate([q_one, q_zero] + [q_both] * (ALL_CROPS - GLOBAL_CROPS), axis=0)
        g_unit = dot(zst_ref[...], (soft - target).astype(BF16))
        obuf[j % OUT_SLOTS] = (g_unit - unit * jnp.sum(unit * g_unit, axis=0, keepdims=True)) * inv_col

    local_store(n_blk - 1).start()
    remote_store(n_blk - 1).start()
    for j in range(n_blk - OUT_SLOTS, n_blk):
        local_store(j).wait()
        remote_store(j).wait_send()
    for k in range(1, n_dev):
        src = (me + n_dev - k) % n_dev
        spread(k, src, (vp, partner)).wait()
    for src in range(n_chip):
        pltpu.make_async_remote_copy(
            src_ref=x_part(src * 2 + core), dst_ref=x_part(src * 2 + 1 - core), send_sem=xf_out.at[src],
            recv_sem=xf_in.at[src], device_id=(vp, partner), device_id_type=MESH).wait()

    @pl.loop(0, n_blk)
    def _(j):
        remote_store(j).wait_recv()


def proto_grads(z_s, z_t, row_sum, r_row, c_all, g_emb, loss, x_loc, protos, ema_protos, n_vp, n_dp):
    rows, width = z_s.shape
    n_col = protos.shape[1]
    n_blk = n_col // 2 // NB_B
    n_dev = n_vp * n_dp
    dma = pltpu.SemaphoreType.DMA
    return pl.pallas_call(
        functools.partial(grads_kernel, n_vp, n_dp),
        out_shape=(jax.ShapeDtypeStruct((width, n_col), F32),
                   jax.ShapeDtypeStruct((rows, width), F32),
                   jax.ShapeDtypeStruct((1, LANES), F32),
                   jax.ShapeDtypeStruct((x_loc.shape[0], x_loc.shape[1] * n_dp, x_loc.shape[2]), F32)),
        in_specs=[VMEM] * 9 + [HBM] * 2,
        out_specs=(HBM, VMEM, VMEM, HBM),
        scratch_shapes=[
            pltpu.VMEM((2, width, NB_B), BF16),
            pltpu.VMEM((2, width, NB_B), BF16),
            pltpu.VMEM((OUT_SLOTS, width, NB_B), F32),
            pltpu.VMEM((n_dev, rows // n_dev, width), F32),
            pltpu.VMEM((rows // n_dev, width), F32),
            pltpu.VMEM((n_dev, 1, LANES), F32),
            dma((2, 2)),
            dma((OUT_SLOTS,)),
            dma((OUT_SLOTS,)),
            dma((n_blk,)),
        ] + [dma((n_dev,))] * 6 + [dma((n_dp // 2,))] * 4 + [dma((1,))],
        compiler_params=pltpu.CompilerParams(
            collective_id=2, has_side_effects=True, vmem_limit_bytes=60 << 20),
        cost_estimate=pl.CostEstimate(
            flops=2 * rows * n_col * width, bytes_accessed=4 * width * n_col, transcendentals=rows * n_col // 2),
        name="proto_grads",
    )(z_s, z_s.T, z_t, row_sum, r_row, c_all, g_emb, loss, x_loc, protos, ema_protos)


def head_kernel(x_hbm, wi_hbm, wm_hbm, wo_hbm, bi_ref, bm_ref, bo_ref, ge_ref,
                h1_hbm, h2_hbm, g2_hbm, g1_hbm, gp_ref, bias_ref,
                x_buf, wi, wm, wo, hid_one, hid_two, slope_one, slope_two, stage, grad_two, gp_stage, snd, rcv,
                ld_sem, loc_sem, out_sem, in_sem, gp_sem, bs_sem):
    vp, dp = my_place()
    chip, core = dp // 2, dp % 2
    partner = chip * 2 + 1 - core
    half, n_hid = hid_one.shape
    n_out = wo.shape[1]
    n_blk = n_hid // HB
    mine = pl.ds(pl.multiple_of(core * half, half), half)
    device = (vp, partner)
    barrier = pltpu.get_barrier_semaphore()
    pl.semaphore_signal(barrier, inc=1, device_id=device, device_id_type=MESH)
    loads = [pltpu.make_async_copy(x_hbm.at[mine], x_buf, ld_sem.at[0]),
             pltpu.make_async_copy(wi_hbm, wi, ld_sem.at[1]),
             pltpu.make_async_copy(wm_hbm, wm, ld_sem.at[2]),
             pltpu.make_async_copy(wo_hbm, wo, ld_sem.at[3])]
    for copy in loads:
        copy.start()
    pl.semaphore_wait(barrier, 1)

    def block(j):
        return pl.ds(pl.multiple_of(j * HB, HB), HB)

    def keep(array, dst, j):
        return pltpu.make_async_copy(
            stage.at[array % 2, :, block(j)], dst.at[mine, block(j)], loc_sem.at[array, j])

    def send(array, dst, j):
        return pltpu.make_async_remote_copy(
            src_ref=stage.at[array % 2, :, block(j)], dst_ref=dst.at[mine, block(j)], send_sem=out_sem.at[array, j],
            recv_sem=in_sem.at[array, j], device_id=device, device_id_type=MESH)

    def flush(array, dst, j):
        keep(array, dst, j).start()
        send(array, dst, j).start()

    def drain(array, dst):
        @pl.loop(0, n_blk)
        def _(j):
            keep(array, dst, j).wait()
            send(array, dst, j).wait_send()

    def layer(array, feats, weight, b_ref, hid, slope, dst):
        @pl.loop(0, n_blk)
        def _(j):
            @pl.when(j >= 1)
            def _():
                flush(array, dst, j - 1)

            pre = dot(feats, weight[:, block(j)]) + b_ref[:, block(j)].astype(F32)
            cdf = 0.5 * (1.0 + lax.erf(pre * 0.7071067811865476))
            low = (pre * cdf).astype(BF16)
            hid[:, block(j)] = low
            stage[array % 2, :, block(j)] = low.astype(F32)
            slope[:, block(j)] = cdf + pre * jnp.exp(-0.5 * pre * pre) * 0.3989422804014327
        flush(array, dst, n_blk - 1)

    loads[0].wait()
    loads[1].wait()
    layer(0, x_buf[...].astype(BF16), wi, bi_ref, hid_one, slope_one, h1_hbm)
    loads[2].wait()
    layer(1, hid_one[...], wm, bm_ref, hid_two, slope_two, h2_hbm)
    loads[3].wait()
    proj = dot(hid_two[...], wo[...]) + bo_ref[...].astype(F32)
    inv_norm = lax.rsqrt(jnp.sum(proj * proj, axis=-1, keepdims=True))
    unit = proj * inv_norm
    g_emb = ge_ref[mine]
    g_proj = (g_emb - unit * jnp.sum(unit * g_emb, axis=-1, keepdims=True)) * inv_norm
    gp_low = g_proj.astype(BF16)
    gp_stage[...] = gp_low.astype(F32)
    gp_ref[mine] = gp_low.astype(F32)
    snd[:, 2 * n_hid:] = jnp.sum(g_proj, axis=0, keepdims=True)
    drain(0, h1_hbm)

    @pl.loop(0, n_blk)
    def _(j):
        @pl.when(j >= 1)
        def _():
            flush(2, g2_hbm, j - 1)

        g_hid = dot_t(gp_low, wo[block(j), :])
        g_pre = g_hid.astype(BF16).astype(F32) * slope_two[:, block(j)]
        snd[:, block(j)] = jnp.sum(g_pre, axis=0, keepdims=True)
        low = g_pre.astype(BF16)
        grad_two[:, block(j)] = low
        stage[0, :, block(j)] = low.astype(F32)
    flush(2, g2_hbm, n_blk - 1)
    gp_send = pltpu.make_async_remote_copy(
        src_ref=gp_stage, dst_ref=gp_ref.at[mine], send_sem=gp_sem.at[0], recv_sem=gp_sem.at[1],
        device_id=device, device_id_type=MESH)
    gp_send.start()
    drain(1, h2_hbm)

    @pl.loop(0, n_blk)
    def _(j):
        @pl.when(j >= 1)
        def _():
            flush(3, g1_hbm, j - 1)

        g_hid = dot_t(grad_two[...], wm[block(j), :])
        g_pre = g_hid.astype(BF16).astype(F32) * slope_one[:, block(j)]
        snd[:, pl.ds(pl.multiple_of(n_hid + j * HB, HB), HB)] = jnp.sum(g_pre, axis=0, keepdims=True)
        stage[1, :, block(j)] = g_pre.astype(BF16).astype(F32)
    flush(3, g1_hbm, n_blk - 1)
    bias_send = pltpu.make_async_remote_copy(
        src_ref=snd, dst_ref=rcv, send_sem=bs_sem.at[0], recv_sem=bs_sem.at[1],
        device_id=device, device_id_type=MESH)
    bias_send.start()
    drain(2, g2_hbm)
    drain(3, g1_hbm)
    gp_send.wait()
    bias_send.wait()
    bias_ref[...] = snd[...] + rcv[...]
    for array, dst in enumerate((h1_hbm, h2_hbm, g2_hbm, g1_hbm)):
        @pl.loop(0, n_blk)
        def _(j):
            send(array, dst, j).wait_recv()


def head_pass(x_all, w_in, b_in, w_mid, b_mid, w_out, b_out, g_emb):
    rows, feat = x_all.shape
    n_hid, n_out = w_out.shape
    half = rows // 2
    n_blk = n_hid // HB
    n_bias = 2 * n_hid + n_out
    dma = pltpu.SemaphoreType.DMA
    wide = jax.ShapeDtypeStruct((rows, n_hid), F32)
    return pl.pallas_call(
        head_kernel,
        out_shape=(wide, wide, wide, wide, jax.ShapeDtypeStruct((rows, n_out), F32),
                   jax.ShapeDtypeStruct((1, n_bias), F32)),
        in_specs=[HBM] * 4 + [VMEM] * 4,
        out_specs=(HBM,) * 4 + (VMEM,) * 2,
        scratch_shapes=[
            pltpu.VMEM((half, feat), F32),
            pltpu.VMEM((feat, n_hid), BF16),
            pltpu.VMEM((n_hid, n_hid), BF16),
            pltpu.VMEM((n_hid, n_out), BF16),
            pltpu.VMEM((half, n_hid), BF16),
            pltpu.VMEM((half, n_hid), BF16),
            pltpu.VMEM((half, n_hid), F32),
            pltpu.VMEM((half, n_hid), F32),
            pltpu.VMEM((2, half, n_hid), F32),
            pltpu.VMEM((half, n_hid), BF16),
            pltpu.VMEM((half, n_out), F32),
            pltpu.VMEM((1, n_bias), F32),
            pltpu.VMEM((1, n_bias), F32),
            dma((4,)), dma((4, n_blk)), dma((4, n_blk)), dma((4, n_blk)), dma((2,)), dma((2,)),
        ],
        compiler_params=pltpu.CompilerParams(
            collective_id=3, has_side_effects=True, vmem_limit_bytes=63 << 20),
        cost_estimate=pl.CostEstimate(
            flops=2 * rows * (feat + 2 * n_hid) * n_hid, bytes_accessed=16 * rows * n_hid, transcendentals=2 * rows * n_hid),
        name="head_pass",
    )(x_all, w_in, w_mid, w_out, b_in.reshape(1, -1), b_mid.reshape(1, -1), b_out.reshape(1, -1), g_emb)


def wgrad_kernel(first, n_step, base, *refs):
    if first:
        a_ref, b_ref, src, out_ref, dst, low, cbuf, rd_sem, wr_sem = refs
    else:
        a_ref, b_ref, src, _, out_ref, dst, low, cbuf, rd_sem, wr_sem = refs
    i = pl.program_id(0)
    chunk = cbuf.shape[2]

    def cols(step):
        return pl.ds(pl.multiple_of(base + step * chunk, chunk), chunk)

    def read(step):
        return pltpu.make_async_copy(src.at[:, cols(step)], cbuf.at[step % 3], rd_sem.at[step % 3])

    def write(step):
        return pltpu.make_async_copy(cbuf.at[step % 3], dst.at[:, cols(step)], wr_sem.at[step % 3])

    @pl.when(i == 0)
    def _():
        read(0).start()
        low[...] = b_ref[...].astype(BF16)

    @pl.when(i >= 2)
    def _():
        write(i - 2).wait()

    @pl.when(i + 1 < n_step)
    def _():
        read(i + 1).start()

    read(i).wait()
    write(i).start()
    out_ref[...] = lax.dot_general(
        a_ref[...].astype(BF16), low[...], (((0,), (0,)), ((), ())), preferred_element_type=F32)

    @pl.when(i == n_step - 1)
    def _():
        write(i - 1).wait()
        write(i).wait()


def wgrad(left, right, src, dst, start, width, block=256):
    rows, n_left = left.shape
    n_right = right.shape[1]
    n_step = n_left // block
    first = dst is None
    chunk = width // n_step
    args = (left, right, src) + (() if first else (dst,))
    return pl.pallas_call(
        functools.partial(wgrad_kernel, first, n_step, start),
        grid=(n_step,),
        out_shape=(jax.ShapeDtypeStruct((n_left, n_right), F32), jax.ShapeDtypeStruct(src.shape, F32)),
        in_specs=[pl.BlockSpec((rows, block), lambda i: (0, i)),
                  pl.BlockSpec((rows, n_right), lambda i: (0, 0), pipeline_mode=pl.Buffered(1)),
                  HBM] + ([] if first else [HBM]),
        out_specs=(pl.BlockSpec((block, n_right), lambda i: (i, 0)), HBM),
        scratch_shapes=[pltpu.VMEM((rows, n_right), BF16),
                        pltpu.VMEM((3, src.shape[0], chunk), F32),
                        pltpu.SemaphoreType.DMA((3,)), pltpu.SemaphoreType.DMA((3,))],
        input_output_aliases={} if first else {3: 1},
        compiler_params=pltpu.CompilerParams(
            dimension_semantics=("arbitrary",), vmem_limit_bytes=60 << 20),
        cost_estimate=pl.CostEstimate(
            flops=2 * rows * n_left * n_right, bytes_accessed=8 * src.shape[0] * width, transcendentals=0),
        name="wgrad",
    )(*args)


def solution(mesh):
    n_vp = mesh.shape['vp']
    n_dp = mesh.shape['dp']

    def local_step(student_x, teacher_x, w_in, b_in, w_mid, b_mid, w_out, b_out, protos,
                   ema_w_in, ema_b_in, ema_w_mid, ema_b_mid, ema_w_out, ema_b_out, ema_protos):
        rows, feat = student_x.shape
        n_img = rows // ALL_CROPS
        width = protos.shape[0]
        x_loc = student_x.reshape(n_img, ALL_CROPS, feat).transpose(1, 0, 2)
        t_loc = teacher_x.reshape(n_img, GLOBAL_CROPS, feat).transpose(1, 0, 2).reshape(-1, feat)
        t_emb = mlp_forward(t_loc, ema_w_in, ema_b_in, ema_w_mid, ema_b_mid, ema_w_out, ema_b_out)
        s_emb = mlp_forward(x_loc.reshape(rows, feat), w_in, b_in, w_mid, b_mid, w_out, b_out)
        z_loc = jnp.concatenate([s_emb, t_emb], axis=0).reshape(ALL_CROPS + GLOBAL_CROPS, n_img, width)
        z_all = gather_dp(z_loc, n_dp, 0).reshape(-1, width).astype(BF16)
        z_s, z_t = z_all[:rows * n_dp], z_all[rows * n_dp:]
        c_all, row_sum, r_row, g_emb, loss = sinkhorn_stats(z_s, z_t, protos, ema_protos, n_vp, n_dp)
        g_temp, g_emb, loss, x_all = proto_grads(
            z_s, z_t, row_sum, r_row, c_all, g_emb, loss, x_loc.astype(F32), protos, ema_protos, n_vp, n_dp)
        x_all = x_all.reshape(rows * n_dp, feat)
        hid_one, hid_two, g_two, g_one, g_proj, biases = head_pass(
            x_all, w_in, b_in, w_mid, b_mid, w_out, b_out, g_emb)
        n_hid = w_mid.shape[0]
        part = protos.shape[1] // 8
        g_w_mid, g_protos = wgrad(hid_one, g_two, g_temp, None, 0, 4 * part)
        g_w_in, g_protos = wgrad(x_all, g_one, g_temp, g_protos, 4 * part, 3 * part)
        g_w_out, g_protos = wgrad(hid_two, g_proj, g_temp, g_protos, 7 * part, part)
        biases = biases.reshape(-1)
        g_b_mid, g_b_in, g_b_out = biases[:n_hid], biases[n_hid:2 * n_hid], biases[2 * n_hid:]
        return (jnp.sum(loss), g_w_in, g_b_in, g_w_mid, g_b_mid, g_w_out, g_b_out, g_protos)

    by_rows = P('dp', None)
    by_cols = P(None, 'vp')
    replicated = P()
    head_specs = (replicated,) * 6
    in_specs = (by_rows, by_rows) + head_specs + (by_cols,) + head_specs + (by_cols,)
    out_specs = (replicated,) * 7 + (by_cols,)
    return jax.shard_map(local_step, mesh=mesh, in_specs=in_specs, out_specs=out_specs, check_vma=False)
```

```python
import functools

import jax
import jax.numpy as jnp
from jax import lax
from jax.experimental import pallas as pl
from jax.experimental.pallas import tpu as pltpu
from jax.sharding import PartitionSpec as P

ALL_CROPS = 10
GLOBAL_CROPS = 2
TEMP_STUDENT = 0.1
TEMP_TEACHER = 0.04
LOG2E = 1.4426950408889634
LANES = 128
NB_A = 1024
NB_B = 1024
OUT_SLOTS = 3
HB = 512
RING = 4
F32 = jnp.float32
BF16 = jnp.bfloat16
MESH = pl.DeviceIdType.MESH
HBM = pl.BlockSpec(memory_space=pl.ANY)
VMEM = pl.BlockSpec(memory_space=pltpu.VMEM)


def mlp_forward(feats, w_in, b_in, w_mid, b_mid, w_out, b_out):
    pre_one = jnp.dot(feats, w_in, preferred_element_type=F32) + b_in.astype(F32)
    hid_one = jax.nn.gelu(pre_one, approximate=False).astype(BF16)
    pre_two = jnp.dot(hid_one, w_mid, preferred_element_type=F32) + b_mid.astype(F32)
    hid_two = jax.nn.gelu(pre_two, approximate=False).astype(BF16)
    proj = jnp.dot(hid_two, w_out, preferred_element_type=F32) + b_out.astype(F32)
    inv_norm = lax.rsqrt(jnp.sum(proj * proj, axis=-1, keepdims=True))
    return proj * inv_norm


def unit_columns(block):
    block_f = block.astype(F32)
    inv_col = lax.rsqrt(jnp.sum(block_f * block_f, axis=0, keepdims=True))
    return block_f * inv_col, inv_col


def dot(left, right):
    return jnp.dot(left, right, preferred_element_type=F32)


def dot_t(left, right):
    return lax.dot_general(left, right, (((1,), (1,)), ((), ())), preferred_element_type=F32)


def to_column(row):
    return jnp.transpose(jnp.broadcast_to(row, (LANES, row.shape[1])))


def to_row(acc):
    return jnp.sum(jnp.transpose(acc), axis=0, keepdims=True)


def fold_lanes(wide):
    total = wide[:, :LANES]
    for start in range(LANES, wide.shape[1], LANES):
        total = total + wide[:, start:start + LANES]
    return total


def my_place():
    return lax.axis_index('vp'), lax.axis_index('dp')


def gather_kernel(n_dp, block_ref, all_ref, out_sem, in_sem, fwd_out, fwd_in):
    vp, me = my_place()
    n_chip = n_dp // 2
    chip, core = me // 2, me % 2
    partner = chip * 2 + 1 - core
    n_row = block_ref.shape[1]

    def part(slot):
        return all_ref.at[:, pl.ds(pl.multiple_of(slot * n_row, n_row), n_row)]

    barrier = pltpu.get_barrier_semaphore()
    pl.semaphore_signal(barrier, inc=1, device_id=(vp, partner), device_id_type=MESH)
    for k in range(1, n_chip):
        peer = ((chip + k) % n_chip) * 2 + core
        pl.semaphore_signal(barrier, inc=1, device_id=(vp, peer), device_id_type=MESH)
    pl.semaphore_wait(barrier, n_chip)
    sends = []
    for k in range(1, n_chip):
        peer = ((chip + k) % n_chip) * 2 + core
        sends.append(pltpu.make_async_remote_copy(
            src_ref=block_ref, dst_ref=part(me), send_sem=out_sem.at[k], recv_sem=in_sem.at[chip],
            device_id=(vp, peer), device_id_type=MESH))
    own = pltpu.make_async_remote_copy(
        src_ref=block_ref, dst_ref=part(me), send_sem=fwd_out.at[chip], recv_sem=fwd_in.at[chip],
        device_id=(vp, partner), device_id_type=MESH)
    for copy in sends:
        copy.start()
    own.start()
    all_ref[:, pl.ds(pl.multiple_of(me * n_row, n_row), n_row)] = block_ref[...]
    for k in range(1, n_chip):
        src = (chip + n_chip - k) % n_chip
        slot = src * 2 + core
        peer_copy = pltpu.make_async_remote_copy(
            src_ref=block_ref, dst_ref=part(slot), send_sem=out_sem.at[k], recv_sem=in_sem.at[src],
            device_id=(vp, partner), device_id_type=MESH)
        peer_copy.wait_recv()
        forward = pltpu.make_async_remote_copy(
            src_ref=part(slot), dst_ref=part(slot), send_sem=fwd_out.at[src], recv_sem=fwd_in.at[src],
            device_id=(vp, partner), device_id_type=MESH)
        forward.start()
    for copy in sends:
        copy.wait_send()
    for src in range(n_chip):
        slot = src * 2 + core
        other = src * 2 + 1 - core
        pltpu.make_async_remote_copy(
            src_ref=part(slot), dst_ref=part(other), send_sem=fwd_out.at[src], recv_sem=fwd_in.at[src],
            device_id=(vp, partner), device_id_type=MESH).wait()


def gather_dp(block, n_dp, collective_id):
    groups, n_row, width = block.shape
    return pl.pallas_call(
        functools.partial(gather_kernel, n_dp),
        out_shape=jax.ShapeDtypeStruct((groups, n_row * n_dp, width), block.dtype),
        in_specs=[VMEM],
        out_specs=VMEM,
        scratch_shapes=[pltpu.SemaphoreType.DMA((n_dp // 2,))] * 4,
        compiler_params=pltpu.CompilerParams(
            collective_id=collective_id, has_side_effects=True, vmem_limit_bytes=48 << 20),
        name="gather_dp",
    )(block)


def stats_kernel(n_vp, n_dp, zs_ref, zt_ref, v_hbm, vt_hbm, c_ref, rs_ref, r_ref, ge_ref, loss_ref,
                 vbuf, tbuf, in_sem, ubuf, kbuf, acc_s, acc_r, wbuf, snd, rcv, send_sem, recv_sem, c_out, c_in):
    vp, dp = my_place()
    n_dev = n_vp * n_dp
    me = vp * n_dp + dp
    rows, rows_t = zs_ref.shape[0], zt_ref.shape[0]
    n_img = rows // ALL_CROPS
    n_col = kbuf.shape[1]
    n_blk = n_col // NB_A
    base = dp * n_col

    barrier = pltpu.get_barrier_semaphore()
    for k in range(1, n_dev):
        peer = (me + k) % n_dev
        pl.semaphore_signal(barrier, inc=1, device_id=(peer // n_dp, peer % n_dp), device_id_type=MESH)

    def load(which, j):
        src, buf = ((v_hbm, vbuf), (vt_hbm, tbuf))[which]
        cols = pl.ds(pl.multiple_of(base + j * NB_A, NB_A), NB_A)
        return pltpu.make_async_copy(src.at[:, cols], buf.at[j % 2], in_sem.at[which, j % 2])

    load(1, 0).start()
    load(0, 0).start()
    acc_s[...] = jnp.zeros_like(acc_s)
    acc_r[...] = jnp.zeros_like(acc_r)
    ge_ref[...] = jnp.zeros_like(ge_ref)

    @pl.loop(0, n_blk)
    def _(j):
        @pl.when(j + 1 < n_blk)
        def _():
            load(1, j + 1).start()

        load(1, j).wait()
        unit_t = unit_columns(tbuf[j % 2])[0].astype(BF16)
        kern = jnp.exp2(dot(zt_ref[...], unit_t) * (LOG2E / TEMP_TEACHER))
        kbuf[:, pl.ds(pl.multiple_of(j * NB_A, NB_A), NB_A)] = kern
        acc_r[...] += fold_lanes(kern * (1.0 / jnp.sum(kern, axis=0, keepdims=True)))

    pl.semaphore_wait(barrier, n_dev - 1)

    def message(step, k, dst, peer, width):
        return pltpu.make_async_remote_copy(
            src_ref=snd.at[step, :, :width], dst_ref=rcv.at[step, dst, :, :width],
            send_sem=send_sem.at[step, k], recv_sem=recv_sem.at[step, dst],
            device_id=(peer // n_dp, peer % n_dp), device_id_type=MESH)

    def publish(step, value):
        width = value.shape[1]
        snd[step, :, :width] = value
        for k in range(1, n_dev):
            message(step, k, me, (me + k) % n_dev, width).start()
        rcv[step, me, :, :width] = value

    def collect(step, width):
        for k in range(1, n_dev):
            src = (me + n_dev - k) % n_dev
            message(step, k, src, src, width).wait()
        total = rcv[step, 0, :, :width]
        for k in range(1, n_dev):
            total = total + rcv[step, k, :, :width]
        return total

    def rescale(r_row, keep):
        r_col = to_column(r_row)
        acc_r[...] = jnp.zeros_like(acc_r)
        span = 4 * LANES

        @pl.loop(0, n_col // span)
        def _(j):
            total = acc_r[...]
            for k in range(4):
                here = pl.ds(pl.multiple_of(j * span + k * LANES, LANES), LANES)
                kern = kbuf[:, here]
                c_row = 1.0 / jnp.sum(kern * r_col, axis=0, keepdims=True)
                total = total + kern * c_row
                if keep:
                    c_ref[dp, :, here] = c_row
            acc_r[...] = total

    third = (n_blk * 3) // 8
    publish(0, to_row(acc_r[...]))

    @pl.loop(0, n_blk)
    def _(j):
        @pl.when(j + 1 < n_blk)
        def _():
            load(0, j + 1).start()

        @pl.when(j == third)
        def _():
            rescale(1.0 / collect(0, rows_t), False)
            publish(1, to_row(acc_r[...]))

        @pl.when(j == 2 * third)
        def _():
            rescale(1.0 / collect(1, rows_t), True)
            publish(2, to_row(acc_r[...]))
            for k in range(1, n_dp):
                pltpu.make_async_remote_copy(
                    src_ref=c_ref.at[dp], dst_ref=c_ref.at[dp], send_sem=c_out.at[k], recv_sem=c_in.at[dp],
                    device_id=(vp, (dp + k) % n_dp), device_id_type=MESH).start()

        load(0, j).wait()
        unit = unit_columns(vbuf[j % 2])[0].astype(BF16)
        ubuf[:, pl.ds(pl.multiple_of(j * NB_A, NB_A), NB_A)] = unit
        exp_s = jnp.exp2(dot(zs_ref[...], unit) * (LOG2E / TEMP_STUDENT))
        acc_s[...] += fold_lanes(exp_s)
        ge_ref[...] += dot_t(exp_s.astype(BF16), unit)

    publish(3, to_row(acc_s[...]))
    r_row = 1.0 / collect(2, rows_t)
    r_ref[...] = r_row

    r_col = to_column(r_row)
    r_wide = jnp.concatenate([r_col] * (NB_A // LANES), axis=1)
    wbuf[...] = jnp.zeros_like(wbuf)

    @pl.loop(0, n_blk)
    def _(j):
        here = pl.ds(pl.multiple_of(j * NB_A, NB_A), NB_A)
        q_mat = kbuf[:, here] * c_ref[dp, :, here] * r_wide
        q_hi = q_mat.astype(BF16)
        q_lo = (q_mat - q_hi.astype(F32)).astype(BF16)
        both = dot_t(jnp.concatenate([q_hi, q_lo], axis=0), ubuf[:, here])
        wbuf[...] += both[:rows_t] + both[rows_t:]

    row_sum = collect(3, rows)
    rs_ref[...] = row_sum
    w_zero = wbuf[:n_img]
    w_one = wbuf[n_img:]
    w_both = w_zero + w_one
    scale = 1.0 / (n_img * GLOBAL_CROPS * (ALL_CROPS - 1))
    log_rs = jnp.log(row_sum)
    inv_rs = to_column(1.0 / row_sum)
    loss = jnp.zeros((1, LANES), F32)
    for v in range(ALL_CROPS):
        block = pl.ds(v * n_img, n_img)
        count = float(GLOBAL_CROPS - (v < GLOBAL_CROPS))
        w_v = (w_one, w_zero)[v] if v < GLOBAL_CROPS else w_both
        inv = inv_rs[v * n_img:(v + 1) * n_img]
        inv = jnp.concatenate([inv] * (ge_ref.shape[1] // LANES), axis=1)
        dots = fold_lanes(jnp.sum(zs_ref[block].astype(F32) * w_v, axis=0, keepdims=True))
        logs = log_rs[:, v * n_img:(v + 1) * n_img]
        loss += (count / n_dev) * logs - (1.0 / TEMP_STUDENT) * dots
        ge_ref[block] = (count * (ge_ref[block] * inv) - w_v) * (scale / TEMP_STUDENT)
    loss_ref[...] = loss * scale

    for k in range(1, n_dp):
        src = (dp + n_dp - k) % n_dp
        pltpu.make_async_remote_copy(
            src_ref=c_ref.at[dp], dst_ref=c_ref.at[src], send_sem=c_out.at[k], recv_sem=c_in.at[src],
            device_id=(vp, src), device_id_type=MESH).wait()


def sinkhorn_stats(z_s, z_t, protos, ema_protos, n_vp, n_dp):
    rows, width = z_s.shape
    rows_t = z_t.shape[0]
    n_col = protos.shape[1] // n_dp
    n_dev = n_vp * n_dp
    flops = 2 * rows * n_col * width * 2
    return pl.pallas_call(
        functools.partial(stats_kernel, n_vp, n_dp),
        out_shape=(jax.ShapeDtypeStruct((n_dp, 1, n_col), F32),
                   jax.ShapeDtypeStruct((1, rows), F32),
                   jax.ShapeDtypeStruct((1, rows_t), F32),
                   jax.ShapeDtypeStruct((rows, width), F32),
                   jax.ShapeDtypeStruct((1, LANES), F32)),
        in_specs=[VMEM, VMEM, HBM, HBM],
        out_specs=(VMEM,) * 5,
        scratch_shapes=[
            pltpu.VMEM((2, width, NB_A), BF16),
            pltpu.VMEM((2, width, NB_A), BF16),
            pltpu.SemaphoreType.DMA((2, 2)),
            pltpu.VMEM((width, n_col), BF16),
            pltpu.VMEM((rows_t, n_col), F32),
            pltpu.VMEM((rows, LANES), F32),
            pltpu.VMEM((rows_t, LANES), F32),
            pltpu.VMEM((rows_t, width), F32),
            pltpu.VMEM((4, 1, rows), F32),
            pltpu.VMEM((4, n_dev, 1, rows), F32),
            pltpu.SemaphoreType.DMA((4, n_dev)),
            pltpu.SemaphoreType.DMA((4, n_dev)),
            pltpu.SemaphoreType.DMA((n_dp,)),
            pltpu.SemaphoreType.DMA((n_dp,)),
        ],
        compiler_params=pltpu.CompilerParams(
            collective_id=1, has_side_effects=True, vmem_limit_bytes=63 << 20),
        cost_estimate=pl.CostEstimate(flops=flops, bytes_accessed=4 * width * n_col, transcendentals=rows * n_col),
        name="sinkhorn_stats",
    )(z_s, z_t, protos, ema_protos)


def grads_kernel(n_vp, n_dp, zs_ref, zst_ref, zt_ref, rs_ref, r_ref, c_ref, ge_ref, loss_ref, x_ref, v_hbm, vt_hbm,
                 g_hbm, ge_all, loss_all, x_all, vbuf, tbuf, obuf, part_ge, sum_ge, part_loss, in_sem, loc_sem, out_sem,
                 recv_sem, rs_out, rs_in, ag_out, ag_in, ls_out, ls_in, x_out, x_in, xf_out, xf_in, x_own):
    vp, dp = my_place()
    n_dev = n_vp * n_dp
    me = vp * n_dp + dp
    n_chip = n_dp // 2
    chip, core = dp // 2, dp % 2
    partner = chip * 2 + 1 - core
    rows, rows_t = zs_ref.shape[0], zt_ref.shape[0]
    n_img = rows // ALL_CROPS
    n_own = rows // n_dev
    n_loc = x_ref.shape[1]
    half = v_hbm.shape[1] // 2
    n_slice = c_ref.shape[2]
    n_blk = half // NB_B
    base = core * half
    barrier = pltpu.get_barrier_semaphore()
    for k in range(1, n_dev):
        peer = (me + k) % n_dev
        pl.semaphore_signal(barrier, inc=1, device_id=(peer // n_dp, peer % n_dp), device_id_type=MESH)

    def load(j, slot):
        cols = pl.ds(pl.multiple_of(base + j * NB_B, NB_B), NB_B)
        return (pltpu.make_async_copy(v_hbm.at[:, cols], vbuf.at[slot], in_sem.at[0, slot]),
                pltpu.make_async_copy(vt_hbm.at[:, cols], tbuf.at[slot], in_sem.at[1, slot]))

    def local_store(j):
        slot = j % OUT_SLOTS
        cols = pl.ds(pl.multiple_of(base + j * NB_B, NB_B), NB_B)
        return pltpu.make_async_copy(obuf.at[slot], g_hbm.at[:, cols], loc_sem.at[slot])

    def remote_store(j):
        slot = j % OUT_SLOTS
        cols = pl.ds(pl.multiple_of(base + j * NB_B, NB_B), NB_B)
        return pltpu.make_async_remote_copy(
            src_ref=obuf.at[slot], dst_ref=g_hbm.at[:, cols], send_sem=out_sem.at[slot],
            recv_sem=recv_sem.at[j], device_id=(vp, partner), device_id_type=MESH)

    def peer_of(k):
        peer = (me + k) % n_dev
        return peer, (peer // n_dp, peer % n_dp)

    def scatter(k, peer, dst, device):
        return pltpu.make_async_remote_copy(
            src_ref=ge_ref.at[pl.ds(pl.multiple_of(peer * n_own, n_own), n_own)], dst_ref=part_ge.at[dst],
            send_sem=rs_out.at[k], recv_sem=rs_in.at[dst], device_id=device, device_id_type=MESH)

    def spread(k, owner, device):
        return pltpu.make_async_remote_copy(
            src_ref=sum_ge, dst_ref=ge_all.at[pl.ds(pl.multiple_of(owner * n_own, n_own), n_own)],
            send_sem=ag_out.at[k], recv_sem=ag_in.at[owner], device_id=device, device_id_type=MESH)

    def loss_send(k, dst, device):
        return pltpu.make_async_remote_copy(
            src_ref=loss_ref, dst_ref=part_loss.at[dst], send_sem=ls_out.at[k], recv_sem=ls_in.at[dst],
            device_id=device, device_id_type=MESH)

    def x_part(slot):
        return x_all.at[:, pl.ds(pl.multiple_of(slot * n_loc, n_loc), n_loc)]

    def x_send(k, src_chip, slot, device):
        return pltpu.make_async_remote_copy(
            src_ref=x_ref, dst_ref=x_part(slot), send_sem=x_out.at[k], recv_sem=x_in.at[src_chip],
            device_id=device, device_id_type=MESH)

    def x_forward(src_chip, slot):
        return pltpu.make_async_remote_copy(
            src_ref=x_part(slot), dst_ref=x_part(slot), send_sem=xf_out.at[src_chip], recv_sem=xf_in.at[src_chip],
            device_id=(vp, partner), device_id_type=MESH)

    for copy in load(0, 0):
        copy.start()
    x_local = pltpu.make_async_copy(x_ref, x_part(dp), x_own.at[0])
    x_local.start()
    scale = 1.0 / (n_img * GLOBAL_CROPS * (ALL_CROPS - 1)) / TEMP_STUDENT
    lanes = lax.broadcasted_iota(jnp.int32, (1, rows), 1)
    weight = jnp.where(lanes < GLOBAL_CROPS * n_img, scale, GLOBAL_CROPS * scale)
    bias = to_column(jnp.log(weight / rs_ref[...]) * LOG2E)
    bias = jnp.concatenate([bias] * (NB_B // LANES), axis=1)
    r_col = to_column(r_ref[...] * scale)
    r_wide = jnp.concatenate([r_col] * (NB_B // LANES), axis=1)
    pl.semaphore_wait(barrier, n_dev - 1)
    for k in range(1, n_dev):
        peer, device = peer_of(k)
        loss_send(k, me, device).start()
        scatter(k, peer, me, device).start()
    for k in range(1, n_chip):
        x_send(k, chip, dp, (vp, ((chip + k) % n_chip) * 2 + core)).start()
    part_ge[me] = ge_ref[pl.ds(pl.multiple_of(me * n_own, n_own), n_own)]
    part_loss[me] = loss_ref[...]

    @pl.loop(0, n_blk)
    def _(j):
        slot = j % 2

        @pl.when(j + 1 < n_blk)
        def _():
            for copy in load(j + 1, 1 - slot):
                copy.start()

        @pl.when(j >= 1)
        def _():
            local_store(j - 1).start()
            remote_store(j - 1).start()

        @pl.when(j >= OUT_SLOTS)
        def _():
            local_store(j - OUT_SLOTS).wait()
            remote_store(j - OUT_SLOTS).wait_send()

        @pl.when(j == n_blk // 2)
        def _():
            for k in range(1, n_dev):
                src = (me + n_dev - k) % n_dev
                scatter(k, src, src, (vp, partner)).wait()
                loss_send(k, src, (vp, partner)).wait()
            total = part_ge[0]
            loss = part_loss[0]
            for k in range(1, n_dev):
                total = total + part_ge[k]
                loss = loss + part_loss[k]
            loss_all[...] = jnp.sum(loss, axis=1, keepdims=True)
            sum_ge[...] = total
            ge_all[pl.ds(pl.multiple_of(me * n_own, n_own), n_own)] = total

        @pl.when(j == n_blk // 2 + 1)
        def _():
            for k in range(1, n_dev):
                spread(k, me, peer_of(k)[1]).start()

        @pl.when(j == n_blk - 4)
        def _():
            x_local.wait()
            x_forward(chip, dp).start()
            for k in range(1, n_chip):
                src = (chip + n_chip - k) % n_chip
                x_send(k, src, src * 2 + core, (vp, partner)).wait()
                x_forward(src, src * 2 + core).start()

        for copy in load(j, slot):
            copy.wait()
        unit_t = unit_columns(tbuf[slot])[0].astype(BF16)
        col = base + j * NB_B
        c_row = c_ref[col // n_slice, :, pl.ds(pl.multiple_of(col % n_slice, NB_B), NB_B)]
        q_mat = jnp.exp2(dot(zt_ref[...], unit_t) * (LOG2E / TEMP_TEACHER)) * c_row * r_wide
        q_zero, q_one = q_mat[:n_img], q_mat[n_img:]
        q_both = q_zero + q_one
        unit, inv_col = unit_columns(vbuf[slot])
        logits = dot(zs_ref[...], unit.astype(BF16))
        soft = jnp.exp2(logits * (LOG2E / TEMP_STUDENT) + bias)
        target = jnp.concatenate([q_one, q_zero] + [q_both] * (ALL_CROPS - GLOBAL_CROPS), axis=0)
        g_unit = dot(zst_ref[...], (soft - target).astype(BF16))
        obuf[j % OUT_SLOTS] = (g_unit - unit * jnp.sum(unit * g_unit, axis=0, keepdims=True)) * inv_col

    local_store(n_blk - 1).start()
    remote_store(n_blk - 1).start()
    for j in range(n_blk - OUT_SLOTS, n_blk):
        local_store(j).wait()
        remote_store(j).wait_send()
    for k in range(1, n_dev):
        src = (me + n_dev - k) % n_dev
        spread(k, src, (vp, partner)).wait()
    for src in range(n_chip):
        pltpu.make_async_remote_copy(
            src_ref=x_part(src * 2 + core), dst_ref=x_part(src * 2 + 1 - core), send_sem=xf_out.at[src],
            recv_sem=xf_in.at[src], device_id=(vp, partner), device_id_type=MESH).wait()

    @pl.loop(0, n_blk)
    def _(j):
        remote_store(j).wait_recv()


def proto_grads(z_s, z_t, row_sum, r_row, c_all, g_emb, loss, x_loc, protos, ema_protos, n_vp, n_dp):
    rows, width = z_s.shape
    n_col = protos.shape[1]
    n_blk = n_col // 2 // NB_B
    n_dev = n_vp * n_dp
    dma = pltpu.SemaphoreType.DMA
    return pl.pallas_call(
        functools.partial(grads_kernel, n_vp, n_dp),
        out_shape=(jax.ShapeDtypeStruct((width, n_col), F32),
                   jax.ShapeDtypeStruct((rows, width), F32),
                   jax.ShapeDtypeStruct((1, 1), F32),
                   jax.ShapeDtypeStruct((x_loc.shape[0], x_loc.shape[1] * n_dp, x_loc.shape[2]), F32)),
        in_specs=[VMEM] * 9 + [HBM] * 2,
        out_specs=(HBM, VMEM, VMEM, HBM),
        scratch_shapes=[
            pltpu.VMEM((2, width, NB_B), BF16),
            pltpu.VMEM((2, width, NB_B), BF16),
            pltpu.VMEM((OUT_SLOTS, width, NB_B), F32),
            pltpu.VMEM((n_dev, rows // n_dev, width), F32),
            pltpu.VMEM((rows // n_dev, width), F32),
            pltpu.VMEM((n_dev, 1, LANES), F32),
            dma((2, 2)),
            dma((OUT_SLOTS,)),
            dma((OUT_SLOTS,)),
            dma((n_blk,)),
        ] + [dma((n_dev,))] * 6 + [dma((n_dp // 2,))] * 4 + [dma((1,))],
        compiler_params=pltpu.CompilerParams(
            collective_id=2, has_side_effects=True, vmem_limit_bytes=63 << 20),
        cost_estimate=pl.CostEstimate(
            flops=2 * rows * n_col * width, bytes_accessed=4 * width * n_col, transcendentals=rows * n_col // 2),
        name="proto_grads",
    )(z_s, z_s.T, z_t, row_sum, r_row, c_all, g_emb, loss, x_loc, protos, ema_protos)


def head_kernel(x_hbm, wi_hbm, wm_hbm, wo_hbm, bi_ref, bm_ref, bo_ref, ge_ref,
                h1_hbm, h2_hbm, g2_hbm, g1_hbm, gp_ref, bias_ref,
                x_buf, wi, wm, wo, hid_one, hid_two, slope_one, slope_two, stage, grad_two, gp_stage, snd, rcv,
                ld_sem, loc_sem, out_sem, in_sem, gp_sem, bs_sem):
    vp, dp = my_place()
    chip, core = dp // 2, dp % 2
    partner = chip * 2 + 1 - core
    half, n_hid = hid_one.shape
    n_out = wo.shape[1]
    n_blk = n_hid // HB
    mine = pl.ds(pl.multiple_of(core * half, half), half)
    device = (vp, partner)
    barrier = pltpu.get_barrier_semaphore()
    pl.semaphore_signal(barrier, inc=1, device_id=device, device_id_type=MESH)
    loads = [pltpu.make_async_copy(x_hbm.at[mine], x_buf, ld_sem.at[0]),
             pltpu.make_async_copy(wi_hbm, wi, ld_sem.at[1]),
             pltpu.make_async_copy(wm_hbm, wm, ld_sem.at[2]),
             pltpu.make_async_copy(wo_hbm, wo, ld_sem.at[3])]
    for copy in loads:
        copy.start()
    pl.semaphore_wait(barrier, 1)

    def block(j):
        return pl.ds(pl.multiple_of(j * HB, HB), HB)

    def keep(array, dst, j):
        return pltpu.make_async_copy(
            stage.at[array % 2, :, block(j)], dst.at[mine, block(j)], loc_sem.at[array, j])

    def send(array, dst, j):
        return pltpu.make_async_remote_copy(
            src_ref=stage.at[array % 2, :, block(j)], dst_ref=dst.at[mine, block(j)], send_sem=out_sem.at[array, j],
            recv_sem=in_sem.at[array, j], device_id=device, device_id_type=MESH)

    def flush(array, dst, j):
        keep(array, dst, j).start()
        send(array, dst, j).start()

    def drain(array, dst):
        @pl.loop(0, n_blk)
        def _(j):
            keep(array, dst, j).wait()
            send(array, dst, j).wait_send()

    def layer(array, feats, weight, b_ref, hid, slope, dst):
        @pl.loop(0, n_blk)
        def _(j):
            @pl.when(j >= 1)
            def _():
                flush(array, dst, j - 1)

            pre = dot(feats, weight[:, block(j)]) + b_ref[:, block(j)].astype(F32)
            cdf = 0.5 * (1.0 + lax.erf(pre * 0.7071067811865476))
            low = (pre * cdf).astype(BF16)
            hid[:, block(j)] = low
            stage[array % 2, :, block(j)] = low.astype(F32)
            slope[:, block(j)] = cdf + pre * jnp.exp(-0.5 * pre * pre) * 0.3989422804014327
        flush(array, dst, n_blk - 1)

    loads[0].wait()
    loads[1].wait()
    layer(0, x_buf[...].astype(BF16), wi, bi_ref, hid_one, slope_one, h1_hbm)
    loads[2].wait()
    layer(1, hid_one[...], wm, bm_ref, hid_two, slope_two, h2_hbm)
    loads[3].wait()
    proj = dot(hid_two[...], wo[...]) + bo_ref[...].astype(F32)
    inv_norm = lax.rsqrt(jnp.sum(proj * proj, axis=-1, keepdims=True))
    unit = proj * inv_norm
    g_emb = ge_ref[mine]
    g_proj = (g_emb - unit * jnp.sum(unit * g_emb, axis=-1, keepdims=True)) * inv_norm
    gp_low = g_proj.astype(BF16)
    gp_stage[...] = gp_low.astype(F32)
    gp_ref[mine] = gp_low.astype(F32)
    snd[:, 2 * n_hid:] = jnp.sum(g_proj, axis=0, keepdims=True)
    drain(0, h1_hbm)

    @pl.loop(0, n_blk)
    def _(j):
        @pl.when(j >= 1)
        def _():
            flush(2, g2_hbm, j - 1)

        g_hid = dot_t(gp_low, wo[block(j), :])
        g_pre = g_hid.astype(BF16).astype(F32) * slope_two[:, block(j)]
        snd[:, block(j)] = jnp.sum(g_pre, axis=0, keepdims=True)
        low = g_pre.astype(BF16)
        grad_two[:, block(j)] = low
        stage[0, :, block(j)] = low.astype(F32)
    flush(2, g2_hbm, n_blk - 1)
    gp_send = pltpu.make_async_remote_copy(
        src_ref=gp_stage, dst_ref=gp_ref.at[mine], send_sem=gp_sem.at[0], recv_sem=gp_sem.at[1],
        device_id=device, device_id_type=MESH)
    gp_send.start()
    drain(1, h2_hbm)

    @pl.loop(0, n_blk)
    def _(j):
        @pl.when(j >= 1)
        def _():
            flush(3, g1_hbm, j - 1)

        g_hid = dot_t(grad_two[...], wm[block(j), :])
        g_pre = g_hid.astype(BF16).astype(F32) * slope_one[:, block(j)]
        snd[:, pl.ds(pl.multiple_of(n_hid + j * HB, HB), HB)] = jnp.sum(g_pre, axis=0, keepdims=True)
        stage[1, :, block(j)] = g_pre.astype(BF16).astype(F32)
    flush(3, g1_hbm, n_blk - 1)
    bias_send = pltpu.make_async_remote_copy(
        src_ref=snd, dst_ref=rcv, send_sem=bs_sem.at[0], recv_sem=bs_sem.at[1],
        device_id=device, device_id_type=MESH)
    bias_send.start()
    drain(2, g2_hbm)
    drain(3, g1_hbm)
    gp_send.wait()
    bias_send.wait()
    bias_ref[...] = snd[...] + rcv[...]
    for array, dst in enumerate((h1_hbm, h2_hbm, g2_hbm, g1_hbm)):
        @pl.loop(0, n_blk)
        def _(j):
            send(array, dst, j).wait_recv()


def head_pass(x_all, w_in, b_in, w_mid, b_mid, w_out, b_out, g_emb):
    rows, feat = x_all.shape
    n_hid, n_out = w_out.shape
    half = rows // 2
    n_blk = n_hid // HB
    n_bias = 2 * n_hid + n_out
    dma = pltpu.SemaphoreType.DMA
    wide = jax.ShapeDtypeStruct((rows, n_hid), F32)
    return pl.pallas_call(
        head_kernel,
        out_shape=(wide, wide, wide, wide, jax.ShapeDtypeStruct((rows, n_out), F32),
                   jax.ShapeDtypeStruct((1, n_bias), F32)),
        in_specs=[HBM] * 4 + [VMEM] * 4,
        out_specs=(HBM,) * 4 + (VMEM,) * 2,
        scratch_shapes=[
            pltpu.VMEM((half, feat), F32),
            pltpu.VMEM((feat, n_hid), BF16),
            pltpu.VMEM((n_hid, n_hid), BF16),
            pltpu.VMEM((n_hid, n_out), BF16),
            pltpu.VMEM((half, n_hid), BF16),
            pltpu.VMEM((half, n_hid), BF16),
            pltpu.VMEM((half, n_hid), F32),
            pltpu.VMEM((half, n_hid), F32),
            pltpu.VMEM((2, half, n_hid), F32),
            pltpu.VMEM((half, n_hid), BF16),
            pltpu.VMEM((half, n_out), F32),
            pltpu.VMEM((1, n_bias), F32),
            pltpu.VMEM((1, n_bias), F32),
            dma((4,)), dma((4, n_blk)), dma((4, n_blk)), dma((4, n_blk)), dma((2,)), dma((2,)),
        ],
        compiler_params=pltpu.CompilerParams(
            collective_id=3, has_side_effects=True, vmem_limit_bytes=63 << 20),
        cost_estimate=pl.CostEstimate(
            flops=2 * rows * (feat + 2 * n_hid) * n_hid, bytes_accessed=16 * rows * n_hid, transcendentals=2 * rows * n_hid),
        name="head_pass",
    )(x_all, w_in, w_mid, w_out, b_in.reshape(1, -1), b_mid.reshape(1, -1), b_out.reshape(1, -1), g_emb)


def wgrad_kernel(first, n_step, base, *refs):
    if first:
        a_ref, b_ref, src, out_ref, dst, low, cbuf, rd_sem, wr_sem = refs
    else:
        a_ref, b_ref, src, _, out_ref, dst, low, cbuf, rd_sem, wr_sem = refs
    i = pl.program_id(0)
    chunk = cbuf.shape[2]

    def cols(step):
        return pl.ds(pl.multiple_of(base + step * chunk, chunk), chunk)

    def read(step):
        return pltpu.make_async_copy(src.at[:, cols(step)], cbuf.at[step % RING], rd_sem.at[step % RING])

    def write(step):
        return pltpu.make_async_copy(cbuf.at[step % RING], dst.at[:, cols(step)], wr_sem.at[step % RING])

    @pl.when(i == 0)
    def _():
        read(0).start()
        read(1).start()
        low[...] = b_ref[...].astype(BF16)

    @pl.when(i >= 2)
    def _():
        write(i - 2).wait()

    @pl.when(i + 2 < n_step)
    def _():
        read(i + 2).start()

    read(i).wait()
    write(i).start()
    out_ref[...] = lax.dot_general(
        a_ref[...].astype(BF16), low[...], (((0,), (0,)), ((), ())), preferred_element_type=F32)

    @pl.when(i == n_step - 1)
    def _():
        write(i - 1).wait()
        write(i).wait()


def wgrad(left, right, src, dst, start, width, block=256):
    rows, n_left = left.shape
    n_right = right.shape[1]
    n_step = n_left // block
    first = dst is None
    chunk = width // n_step
    args = (left, right, src) + (() if first else (dst,))
    return pl.pallas_call(
        functools.partial(wgrad_kernel, first, n_step, start),
        grid=(n_step,),
        out_shape=(jax.ShapeDtypeStruct((n_left, n_right), F32), jax.ShapeDtypeStruct(src.shape, F32)),
        in_specs=[pl.BlockSpec((rows, block), lambda i: (0, i)),
                  pl.BlockSpec((rows, n_right), lambda i: (0, 0), pipeline_mode=pl.Buffered(1)),
                  HBM] + ([] if first else [HBM]),
        out_specs=(pl.BlockSpec((block, n_right), lambda i: (i, 0)), HBM),
        scratch_shapes=[pltpu.VMEM((rows, n_right), BF16),
                        pltpu.VMEM((RING, src.shape[0], chunk), F32),
                        pltpu.SemaphoreType.DMA((RING,)), pltpu.SemaphoreType.DMA((RING,))],
        input_output_aliases={} if first else {3: 1},
        compiler_params=pltpu.CompilerParams(
            dimension_semantics=("arbitrary",), vmem_limit_bytes=63 << 20),
        cost_estimate=pl.CostEstimate(
            flops=2 * rows * n_left * n_right, bytes_accessed=8 * src.shape[0] * width, transcendentals=0),
        name="wgrad",
    )(*args)


def solution(mesh):
    n_vp = mesh.shape['vp']
    n_dp = mesh.shape['dp']

    def local_step(student_x, teacher_x, w_in, b_in, w_mid, b_mid, w_out, b_out, protos,
                   ema_w_in, ema_b_in, ema_w_mid, ema_b_mid, ema_w_out, ema_b_out, ema_protos):
        rows, feat = student_x.shape
        n_img = rows // ALL_CROPS
        width = protos.shape[0]
        x_loc = student_x.reshape(n_img, ALL_CROPS, feat).transpose(1, 0, 2)
        t_loc = teacher_x.reshape(n_img, GLOBAL_CROPS, feat).transpose(1, 0, 2).reshape(-1, feat)
        t_emb = mlp_forward(t_loc, ema_w_in, ema_b_in, ema_w_mid, ema_b_mid, ema_w_out, ema_b_out)
        s_emb = mlp_forward(x_loc.reshape(rows, feat), w_in, b_in, w_mid, b_mid, w_out, b_out)
        z_loc = jnp.concatenate([s_emb, t_emb], axis=0).reshape(ALL_CROPS + GLOBAL_CROPS, n_img, width)
        z_all = gather_dp(z_loc, n_dp, 0).reshape(-1, width).astype(BF16)
        z_s, z_t = z_all[:rows * n_dp], z_all[rows * n_dp:]
        c_all, row_sum, r_row, g_emb, loss = sinkhorn_stats(z_s, z_t, protos, ema_protos, n_vp, n_dp)
        g_temp, g_emb, loss, x_all = proto_grads(
            z_s, z_t, row_sum, r_row, c_all, g_emb, loss, x_loc.astype(F32), protos, ema_protos, n_vp, n_dp)
        x_all = x_all.reshape(rows * n_dp, feat)
        hid_one, hid_two, g_two, g_one, g_proj, biases = head_pass(
            x_all, w_in, b_in, w_mid, b_mid, w_out, b_out, g_emb)
        n_hid = w_mid.shape[0]
        part = protos.shape[1] // 8
        g_w_mid, g_protos = wgrad(hid_one, g_two, g_temp, None, 0, 4 * part)
        g_w_in, g_protos = wgrad(x_all, g_one, g_temp, g_protos, 4 * part, 3 * part)
        g_w_out, g_protos = wgrad(hid_two, g_proj, g_temp, g_protos, 7 * part, part)
        biases = biases.reshape(-1)
        g_b_mid, g_b_in, g_b_out = biases[:n_hid], biases[n_hid:2 * n_hid], biases[2 * n_hid:]
        return (loss.reshape(()), g_w_in, g_b_in, g_w_mid, g_b_mid, g_w_out, g_b_out, g_protos)

    by_rows = P('dp', None)
    by_cols = P(None, 'vp')
    replicated = P()
    head_specs = (replicated,) * 6
    in_specs = (by_rows, by_rows) + head_specs + (by_cols,) + head_specs + (by_cols,)
    out_specs = (replicated,) * 7 + (by_cols,)
    return jax.shard_map(local_step, mesh=mesh, in_specs=in_specs, out_specs=out_specs, check_vma=False)
```

```python
import functools

import jax
import jax.numpy as jnp
from jax import lax
from jax.experimental import pallas as pl
from jax.experimental.pallas import tpu as pltpu
from jax.sharding import PartitionSpec as P

ALL_CROPS = 10
GLOBAL_CROPS = 2
TEMP_STUDENT = 0.1
TEMP_TEACHER = 0.04
LOG2E = 1.4426950408889634
LANES = 128
NB_A = 1024
NB_B = 1024
OUT_SLOTS = 5
HB = 512
RING = 4
F32 = jnp.float32
BF16 = jnp.bfloat16
MESH = pl.DeviceIdType.MESH
HBM = pl.BlockSpec(memory_space=pl.ANY)
VMEM = pl.BlockSpec(memory_space=pltpu.VMEM)


def mlp_forward(feats, w_in, b_in, w_mid, b_mid, w_out, b_out):
    pre_one = jnp.dot(feats, w_in, preferred_element_type=F32) + b_in.astype(F32)
    hid_one = jax.nn.gelu(pre_one, approximate=False).astype(BF16)
    pre_two = jnp.dot(hid_one, w_mid, preferred_element_type=F32) + b_mid.astype(F32)
    hid_two = jax.nn.gelu(pre_two, approximate=False).astype(BF16)
    proj = jnp.dot(hid_two, w_out, preferred_element_type=F32) + b_out.astype(F32)
    inv_norm = lax.rsqrt(jnp.sum(proj * proj, axis=-1, keepdims=True))
    return proj * inv_norm


def unit_columns(block):
    block_f = block.astype(F32)
    inv_col = lax.rsqrt(jnp.sum(block_f * block_f, axis=0, keepdims=True))
    return block_f * inv_col, inv_col


def dot(left, right):
    return jnp.dot(left, right, preferred_element_type=F32)


def dot_t(left, right):
    return lax.dot_general(left, right, (((1,), (1,)), ((), ())), preferred_element_type=F32)


def to_column(row):
    return jnp.transpose(jnp.broadcast_to(row, (LANES, row.shape[1])))


def to_row(acc):
    return jnp.sum(jnp.transpose(acc), axis=0, keepdims=True)


def fold_lanes(wide):
    total = wide[:, :LANES]
    for start in range(LANES, wide.shape[1], LANES):
        total = total + wide[:, start:start + LANES]
    return total


def my_place():
    return lax.axis_index('vp'), lax.axis_index('dp')


def gather_kernel(n_dp, block_ref, all_ref, out_sem, in_sem, fwd_out, fwd_in):
    vp, me = my_place()
    n_chip = n_dp // 2
    chip, core = me // 2, me % 2
    partner = chip * 2 + 1 - core
    n_row = block_ref.shape[1]

    def part(slot):
        return all_ref.at[:, pl.ds(pl.multiple_of(slot * n_row, n_row), n_row)]

    barrier = pltpu.get_barrier_semaphore()
    pl.semaphore_signal(barrier, inc=1, device_id=(vp, partner), device_id_type=MESH)
    for k in range(1, n_chip):
        peer = ((chip + k) % n_chip) * 2 + core
        pl.semaphore_signal(barrier, inc=1, device_id=(vp, peer), device_id_type=MESH)
    pl.semaphore_wait(barrier, n_chip)
    sends = []
    for k in range(1, n_chip):
        peer = ((chip + k) % n_chip) * 2 + core
        sends.append(pltpu.make_async_remote_copy(
            src_ref=block_ref, dst_ref=part(me), send_sem=out_sem.at[k], recv_sem=in_sem.at[chip],
            device_id=(vp, peer), device_id_type=MESH))
    own = pltpu.make_async_remote_copy(
        src_ref=block_ref, dst_ref=part(me), send_sem=fwd_out.at[chip], recv_sem=fwd_in.at[chip],
        device_id=(vp, partner), device_id_type=MESH)
    for copy in sends:
        copy.start()
    own.start()
    all_ref[:, pl.ds(pl.multiple_of(me * n_row, n_row), n_row)] = block_ref[...]
    for k in range(1, n_chip):
        src = (chip + n_chip - k) % n_chip
        slot = src * 2 + core
        peer_copy = pltpu.make_async_remote_copy(
            src_ref=block_ref, dst_ref=part(slot), send_sem=out_sem.at[k], recv_sem=in_sem.at[src],
            device_id=(vp, partner), device_id_type=MESH)
        peer_copy.wait_recv()
        forward = pltpu.make_async_remote_copy(
            src_ref=part(slot), dst_ref=part(slot), send_sem=fwd_out.at[src], recv_sem=fwd_in.at[src],
            device_id=(vp, partner), device_id_type=MESH)
        forward.start()
    for copy in sends:
        copy.wait_send()
    for src in range(n_chip):
        slot = src * 2 + core
        other = src * 2 + 1 - core
        pltpu.make_async_remote_copy(
            src_ref=part(slot), dst_ref=part(other), send_sem=fwd_out.at[src], recv_sem=fwd_in.at[src],
            device_id=(vp, partner), device_id_type=MESH).wait()


def gather_dp(block, n_dp, collective_id):
    groups, n_row, width = block.shape
    return pl.pallas_call(
        functools.partial(gather_kernel, n_dp),
        out_shape=jax.ShapeDtypeStruct((groups, n_row * n_dp, width), block.dtype),
        in_specs=[VMEM],
        out_specs=VMEM,
        scratch_shapes=[pltpu.SemaphoreType.DMA((n_dp // 2,))] * 4,
        compiler_params=pltpu.CompilerParams(
            collective_id=collective_id, has_side_effects=True, vmem_limit_bytes=48 << 20),
        name="gather_dp",
    )(block)


def stats_kernel(n_vp, n_dp, zs_ref, zt_ref, v_hbm, vt_hbm, c_ref, rs_ref, r_ref, ge_ref, loss_ref,
                 vbuf, tbuf, in_sem, ubuf, kbuf, acc_s, acc_r, wbuf, snd, rcv, send_sem, recv_sem, c_out, c_in):
    vp, dp = my_place()
    n_dev = n_vp * n_dp
    me = vp * n_dp + dp
    rows, rows_t = zs_ref.shape[0], zt_ref.shape[0]
    n_img = rows // ALL_CROPS
    n_col = kbuf.shape[1]
    n_blk = n_col // NB_A
    base = dp * n_col

    barrier = pltpu.get_barrier_semaphore()
    for k in range(1, n_dev):
        peer = (me + k) % n_dev
        pl.semaphore_signal(barrier, inc=1, device_id=(peer // n_dp, peer % n_dp), device_id_type=MESH)

    def load(which, j):
        src, buf = ((v_hbm, vbuf), (vt_hbm, tbuf))[which]
        cols = pl.ds(pl.multiple_of(base + j * NB_A, NB_A), NB_A)
        return pltpu.make_async_copy(src.at[:, cols], buf.at[j % 2], in_sem.at[which, j % 2])

    load(1, 0).start()
    load(0, 0).start()
    acc_s[...] = jnp.zeros_like(acc_s)
    acc_r[...] = jnp.zeros_like(acc_r)
    ge_ref[...] = jnp.zeros_like(ge_ref)

    @pl.loop(0, n_blk)
    def _(j):
        @pl.when(j + 1 < n_blk)
        def _():
            load(1, j + 1).start()

        load(1, j).wait()
        unit_t = unit_columns(tbuf[j % 2])[0].astype(BF16)
        kern = jnp.exp2(dot(zt_ref[...], unit_t) * (LOG2E / TEMP_TEACHER))
        kbuf[:, pl.ds(pl.multiple_of(j * NB_A, NB_A), NB_A)] = kern
        acc_r[...] += fold_lanes(kern * (1.0 / jnp.sum(kern, axis=0, keepdims=True)))

    pl.semaphore_wait(barrier, n_dev - 1)

    def message(step, k, dst, peer, width):
        return pltpu.make_async_remote_copy(
            src_ref=snd.at[step, :, :width], dst_ref=rcv.at[step, dst, :, :width],
            send_sem=send_sem.at[step, k], recv_sem=recv_sem.at[step, dst],
            device_id=(peer // n_dp, peer % n_dp), device_id_type=MESH)

    def publish(step, value):
        width = value.shape[1]
        snd[step, :, :width] = value
        for k in range(1, n_dev):
            message(step, k, me, (me + k) % n_dev, width).start()
        rcv[step, me, :, :width] = value

    def collect(step, width):
        for k in range(1, n_dev):
            src = (me + n_dev - k) % n_dev
            message(step, k, src, src, width).wait()
        total = rcv[step, 0, :, :width]
        for k in range(1, n_dev):
            total = total + rcv[step, k, :, :width]
        return total

    def rescale(r_row, keep):
        r_col = to_column(r_row)
        acc_r[...] = jnp.zeros_like(acc_r)
        span = 4 * LANES

        @pl.loop(0, n_col // span)
        def _(j):
            total = acc_r[...]
            for k in range(4):
                here = pl.ds(pl.multiple_of(j * span + k * LANES, LANES), LANES)
                kern = kbuf[:, here]
                c_row = 1.0 / jnp.sum(kern * r_col, axis=0, keepdims=True)
                total = total + kern * c_row
                if keep:
                    c_ref[dp, :, here] = c_row
            acc_r[...] = total

    third = (n_blk * 3) // 8
    publish(0, to_row(acc_r[...]))

    @pl.loop(0, n_blk)
    def _(j):
        @pl.when(j + 1 < n_blk)
        def _():
            load(0, j + 1).start()

        @pl.when(j == third)
        def _():
            rescale(1.0 / collect(0, rows_t), False)
            publish(1, to_row(acc_r[...]))

        @pl.when(j == 2 * third)
        def _():
            rescale(1.0 / collect(1, rows_t), True)
            publish(2, to_row(acc_r[...]))
            for k in range(1, n_dp):
                pltpu.make_async_remote_copy(
                    src_ref=c_ref.at[dp], dst_ref=c_ref.at[dp], send_sem=c_out.at[k], recv_sem=c_in.at[dp],
                    device_id=(vp, (dp + k) % n_dp), device_id_type=MESH).start()

        load(0, j).wait()
        unit = unit_columns(vbuf[j % 2])[0].astype(BF16)
        ubuf[:, pl.ds(pl.multiple_of(j * NB_A, NB_A), NB_A)] = unit
        exp_s = jnp.exp2(dot(zs_ref[...], unit) * (LOG2E / TEMP_STUDENT))
        acc_s[...] += fold_lanes(exp_s)
        ge_ref[...] += dot_t(exp_s.astype(BF16), unit)

    publish(3, to_row(acc_s[...]))
    r_row = 1.0 / collect(2, rows_t)
    r_ref[...] = r_row

    r_col = to_column(r_row)
    r_wide = jnp.concatenate([r_col] * (NB_A // LANES), axis=1)
    wbuf[...] = jnp.zeros_like(wbuf)

    @pl.loop(0, n_blk)
    def _(j):
        here = pl.ds(pl.multiple_of(j * NB_A, NB_A), NB_A)
        q_mat = kbuf[:, here] * c_ref[dp, :, here] * r_wide
        q_hi = q_mat.astype(BF16)
        q_lo = (q_mat - q_hi.astype(F32)).astype(BF16)
        both = dot_t(jnp.concatenate([q_hi, q_lo], axis=0), ubuf[:, here])
        wbuf[...] += both[:rows_t] + both[rows_t:]

    row_sum = collect(3, rows)
    rs_ref[...] = row_sum
    w_zero = wbuf[:n_img]
    w_one = wbuf[n_img:]
    w_both = w_zero + w_one
    scale = 1.0 / (n_img * GLOBAL_CROPS * (ALL_CROPS - 1))
    log_rs = jnp.log(row_sum)
    inv_rs = to_column(1.0 / row_sum)
    loss = jnp.zeros((1, LANES), F32)
    for v in range(ALL_CROPS):
        block = pl.ds(v * n_img, n_img)
        count = float(GLOBAL_CROPS - (v < GLOBAL_CROPS))
        w_v = (w_one, w_zero)[v] if v < GLOBAL_CROPS else w_both
        inv = inv_rs[v * n_img:(v + 1) * n_img]
        inv = jnp.concatenate([inv] * (ge_ref.shape[1] // LANES), axis=1)
        dots = fold_lanes(jnp.sum(zs_ref[block].astype(F32) * w_v, axis=0, keepdims=True))
        logs = log_rs[:, v * n_img:(v + 1) * n_img]
        loss += (count / n_dev) * logs - (1.0 / TEMP_STUDENT) * dots
        ge_ref[block] = (count * (ge_ref[block] * inv) - w_v) * (scale / TEMP_STUDENT)
    loss_ref[...] = loss * scale

    for k in range(1, n_dp):
        src = (dp + n_dp - k) % n_dp
        pltpu.make_async_remote_copy(
            src_ref=c_ref.at[dp], dst_ref=c_ref.at[src], send_sem=c_out.at[k], recv_sem=c_in.at[src],
            device_id=(vp, src), device_id_type=MESH).wait()


def sinkhorn_stats(z_s, z_t, protos, ema_protos, n_vp, n_dp):
    rows, width = z_s.shape
    rows_t = z_t.shape[0]
    n_col = protos.shape[1] // n_dp
    n_dev = n_vp * n_dp
    flops = 2 * rows * n_col * width * 2
    return pl.pallas_call(
        functools.partial(stats_kernel, n_vp, n_dp),
        out_shape=(jax.ShapeDtypeStruct((n_dp, 1, n_col), F32),
                   jax.ShapeDtypeStruct((1, rows), F32),
                   jax.ShapeDtypeStruct((1, rows_t), F32),
                   jax.ShapeDtypeStruct((rows, width), F32),
                   jax.ShapeDtypeStruct((1, LANES), F32)),
        in_specs=[VMEM, VMEM, HBM, HBM],
        out_specs=(VMEM,) * 5,
        scratch_shapes=[
            pltpu.VMEM((2, width, NB_A), BF16),
            pltpu.VMEM((2, width, NB_A), BF16),
            pltpu.SemaphoreType.DMA((2, 2)),
            pltpu.VMEM((width, n_col), BF16),
            pltpu.VMEM((rows_t, n_col), F32),
            pltpu.VMEM((rows, LANES), F32),
            pltpu.VMEM((rows_t, LANES), F32),
            pltpu.VMEM((rows_t, width), F32),
            pltpu.VMEM((4, 1, rows), F32),
            pltpu.VMEM((4, n_dev, 1, rows), F32),
            pltpu.SemaphoreType.DMA((4, n_dev)),
            pltpu.SemaphoreType.DMA((4, n_dev)),
            pltpu.SemaphoreType.DMA((n_dp,)),
            pltpu.SemaphoreType.DMA((n_dp,)),
        ],
        compiler_params=pltpu.CompilerParams(
            collective_id=1, has_side_effects=True, vmem_limit_bytes=63 << 20),
        cost_estimate=pl.CostEstimate(flops=flops, bytes_accessed=4 * width * n_col, transcendentals=rows * n_col),
        name="sinkhorn_stats",
    )(z_s, z_t, protos, ema_protos)


def grads_kernel(n_vp, n_dp, zs_ref, zst_ref, zt_ref, rs_ref, r_ref, c_ref, ge_ref, loss_ref, x_ref, v_hbm, vt_hbm,
                 g_hbm, ge_all, loss_all, x_all, vbuf, tbuf, obuf, part_ge, sum_ge, part_loss, in_sem, loc_sem, out_sem,
                 recv_sem, rs_out, rs_in, ag_out, ag_in, ls_out, ls_in, x_out, x_in, xf_out, xf_in, x_own):
    vp, dp = my_place()
    n_dev = n_vp * n_dp
    me = vp * n_dp + dp
    n_chip = n_dp // 2
    chip, core = dp // 2, dp % 2
    partner = chip * 2 + 1 - core
    rows, rows_t = zs_ref.shape[0], zt_ref.shape[0]
    n_img = rows // ALL_CROPS
    n_own = rows // n_dev
    n_loc = x_ref.shape[1]
    half = v_hbm.shape[1] // 2
    n_slice = c_ref.shape[2]
    n_blk = half // NB_B
    base = core * half
    barrier = pltpu.get_barrier_semaphore()
    for k in range(1, n_dev):
        peer = (me + k) % n_dev
        pl.semaphore_signal(barrier, inc=1, device_id=(peer // n_dp, peer % n_dp), device_id_type=MESH)

    def load(j, slot):
        cols = pl.ds(pl.multiple_of(base + j * NB_B, NB_B), NB_B)
        return (pltpu.make_async_copy(v_hbm.at[:, cols], vbuf.at[slot], in_sem.at[0, slot]),
                pltpu.make_async_copy(vt_hbm.at[:, cols], tbuf.at[slot], in_sem.at[1, slot]))

    def local_store(j):
        slot = j % OUT_SLOTS
        cols = pl.ds(pl.multiple_of(base + j * NB_B, NB_B), NB_B)
        return pltpu.make_async_copy(obuf.at[slot], g_hbm.at[:, cols], loc_sem.at[slot])

    def remote_store(j):
        slot = j % OUT_SLOTS
        cols = pl.ds(pl.multiple_of(base + j * NB_B, NB_B), NB_B)
        return pltpu.make_async_remote_copy(
            src_ref=obuf.at[slot], dst_ref=g_hbm.at[:, cols], send_sem=out_sem.at[slot],
            recv_sem=recv_sem.at[j], device_id=(vp, partner), device_id_type=MESH)

    def peer_of(k):
        peer = (me + k) % n_dev
        return peer, (peer // n_dp, peer % n_dp)

    def scatter(k, peer, dst, device):
        return pltpu.make_async_remote_copy(
            src_ref=ge_ref.at[pl.ds(pl.multiple_of(peer * n_own, n_own), n_own)], dst_ref=part_ge.at[dst],
            send_sem=rs_out.at[k], recv_sem=rs_in.at[dst], device_id=device, device_id_type=MESH)

    def spread(k, owner, device):
        return pltpu.make_async_remote_copy(
            src_ref=sum_ge, dst_ref=ge_all.at[pl.ds(pl.multiple_of(owner * n_own, n_own), n_own)],
            send_sem=ag_out.at[k], recv_sem=ag_in.at[owner], device_id=device, device_id_type=MESH)

    def loss_send(k, dst, device):
        return pltpu.make_async_remote_copy(
            src_ref=loss_ref, dst_ref=part_loss.at[dst], send_sem=ls_out.at[k], recv_sem=ls_in.at[dst],
            device_id=device, device_id_type=MESH)

    def x_part(slot):
        return x_all.at[:, pl.ds(pl.multiple_of(slot * n_loc, n_loc), n_loc)]

    def x_send(k, src_chip, slot, device):
        return pltpu.make_async_remote_copy(
            src_ref=x_ref, dst_ref=x_part(slot), send_sem=x_out.at[k], recv_sem=x_in.at[src_chip],
            device_id=device, device_id_type=MESH)

    def x_forward(src_chip, slot):
        return pltpu.make_async_remote_copy(
            src_ref=x_part(slot), dst_ref=x_part(slot), send_sem=xf_out.at[src_chip], recv_sem=xf_in.at[src_chip],
            device_id=(vp, partner), device_id_type=MESH)

    for copy in load(0, 0):
        copy.start()
    x_local = pltpu.make_async_copy(x_ref, x_part(dp), x_own.at[0])
    x_local.start()
    scale = 1.0 / (n_img * GLOBAL_CROPS * (ALL_CROPS - 1)) / TEMP_STUDENT
    lanes = lax.broadcasted_iota(jnp.int32, (1, rows), 1)
    weight = jnp.where(lanes < GLOBAL_CROPS * n_img, scale, GLOBAL_CROPS * scale)
    bias = to_column(jnp.log(weight / rs_ref[...]) * LOG2E)
    bias = jnp.concatenate([bias] * (NB_B // LANES), axis=1)
    r_col = to_column(r_ref[...] * scale)
    r_wide = jnp.concatenate([r_col] * (NB_B // LANES), axis=1)
    pl.semaphore_wait(barrier, n_dev - 1)
    for k in range(1, n_dev):
        peer, device = peer_of(k)
        loss_send(k, me, device).start()
        scatter(k, peer, me, device).start()
    for k in range(1, n_chip):
        x_send(k, chip, dp, (vp, ((chip + k) % n_chip) * 2 + core)).start()
    part_ge[me] = ge_ref[pl.ds(pl.multiple_of(me * n_own, n_own), n_own)]
    part_loss[me] = loss_ref[...]

    @pl.loop(0, n_blk)
    def _(j):
        slot = j % 2

        @pl.when(j + 1 < n_blk)
        def _():
            for copy in load(j + 1, 1 - slot):
                copy.start()

        @pl.when(j >= 1)
        def _():
            local_store(j - 1).start()
            remote_store(j - 1).start()

        @pl.when(j >= OUT_SLOTS)
        def _():
            local_store(j - OUT_SLOTS).wait()
            remote_store(j - OUT_SLOTS).wait_send()

        @pl.when(j == n_blk // 2)
        def _():
            for k in range(1, n_dev):
                src = (me + n_dev - k) % n_dev
                scatter(k, src, src, (vp, partner)).wait()
                loss_send(k, src, (vp, partner)).wait()
            total = part_ge[0]
            loss = part_loss[0]
            for k in range(1, n_dev):
                total = total + part_ge[k]
                loss = loss + part_loss[k]
            loss_all[...] = jnp.sum(loss, axis=1, keepdims=True)
            sum_ge[...] = total
            ge_all[pl.ds(pl.multiple_of(me * n_own, n_own), n_own)] = total

        @pl.when(j == n_blk // 2 + 1)
        def _():
            for k in range(1, n_dev):
                spread(k, me, peer_of(k)[1]).start()

        @pl.when(j == n_blk - 4)
        def _():
            x_local.wait()
            x_forward(chip, dp).start()
            for k in range(1, n_chip):
                src = (chip + n_chip - k) % n_chip
                x_send(k, src, src * 2 + core, (vp, partner)).wait()
                x_forward(src, src * 2 + core).start()

        for copy in load(j, slot):
            copy.wait()
        unit_t = unit_columns(tbuf[slot])[0].astype(BF16)
        col = base + j * NB_B
        c_row = c_ref[col // n_slice, :, pl.ds(pl.multiple_of(col % n_slice, NB_B), NB_B)]
        q_mat = jnp.exp2(dot(zt_ref[...], unit_t) * (LOG2E / TEMP_TEACHER)) * c_row * r_wide
        q_zero, q_one = q_mat[:n_img], q_mat[n_img:]
        q_both = q_zero + q_one
        unit, inv_col = unit_columns(vbuf[slot])
        logits = dot(zs_ref[...], unit.astype(BF16))
        soft = jnp.exp2(logits * (LOG2E / TEMP_STUDENT) + bias)
        target = jnp.concatenate([q_one, q_zero] + [q_both] * (ALL_CROPS - GLOBAL_CROPS), axis=0)
        g_unit = dot(zst_ref[...], (soft - target).astype(BF16))
        obuf[j % OUT_SLOTS] = (g_unit - unit * jnp.sum(unit * g_unit, axis=0, keepdims=True)) * inv_col

    local_store(n_blk - 1).start()
    remote_store(n_blk - 1).start()
    for j in range(n_blk - OUT_SLOTS, n_blk):
        local_store(j).wait()
        remote_store(j).wait_send()
    for k in range(1, n_dev):
        src = (me + n_dev - k) % n_dev
        spread(k, src, (vp, partner)).wait()
    for src in range(n_chip):
        pltpu.make_async_remote_copy(
            src_ref=x_part(src * 2 + core), dst_ref=x_part(src * 2 + 1 - core), send_sem=xf_out.at[src],
            recv_sem=xf_in.at[src], device_id=(vp, partner), device_id_type=MESH).wait()

    @pl.loop(0, n_blk)
    def _(j):
        remote_store(j).wait_recv()


def proto_grads(z_s, z_t, row_sum, r_row, c_all, g_emb, loss, x_loc, protos, ema_protos, n_vp, n_dp):
    rows, width = z_s.shape
    n_col = protos.shape[1]
    n_blk = n_col // 2 // NB_B
    n_dev = n_vp * n_dp
    dma = pltpu.SemaphoreType.DMA
    return pl.pallas_call(
        functools.partial(grads_kernel, n_vp, n_dp),
        out_shape=(jax.ShapeDtypeStruct((width, n_col), F32),
                   jax.ShapeDtypeStruct((rows, width), F32),
                   jax.ShapeDtypeStruct((1, 1), F32),
                   jax.ShapeDtypeStruct((x_loc.shape[0], x_loc.shape[1] * n_dp, x_loc.shape[2]), F32)),
        in_specs=[VMEM] * 9 + [HBM] * 2,
        out_specs=(HBM, VMEM, VMEM, HBM),
        scratch_shapes=[
            pltpu.VMEM((2, width, NB_B), BF16),
            pltpu.VMEM((2, width, NB_B), BF16),
            pltpu.VMEM((OUT_SLOTS, width, NB_B), F32),
            pltpu.VMEM((n_dev, rows // n_dev, width), F32),
            pltpu.VMEM((rows // n_dev, width), F32),
            pltpu.VMEM((n_dev, 1, LANES), F32),
            dma((2, 2)),
            dma((OUT_SLOTS,)),
            dma((OUT_SLOTS,)),
            dma((n_blk,)),
        ] + [dma((n_dev,))] * 6 + [dma((n_dp // 2,))] * 4 + [dma((1,))],
        compiler_params=pltpu.CompilerParams(
            collective_id=2, has_side_effects=True, vmem_limit_bytes=63 << 20),
        cost_estimate=pl.CostEstimate(
            flops=2 * rows * n_col * width, bytes_accessed=4 * width * n_col, transcendentals=rows * n_col // 2),
        name="proto_grads",
    )(z_s, z_s.T, z_t, row_sum, r_row, c_all, g_emb, loss, x_loc, protos, ema_protos)


def head_kernel(x_hbm, wi_hbm, wm_hbm, wo_hbm, bi_ref, bm_ref, bo_ref, ge_ref,
                h1_hbm, h2_hbm, g2_hbm, g1_hbm, gp_ref, bias_ref,
                x_buf, wi, wm, wo, hid_one, hid_two, slope_one, slope_two, stage, grad_two, gp_stage, snd, rcv,
                ld_sem, loc_sem, out_sem, in_sem, gp_sem, bs_sem):
    vp, dp = my_place()
    chip, core = dp // 2, dp % 2
    partner = chip * 2 + 1 - core
    half, n_hid = hid_one.shape
    n_out = wo.shape[1]
    n_blk = n_hid // HB
    mine = pl.ds(pl.multiple_of(core * half, half), half)
    device = (vp, partner)
    barrier = pltpu.get_barrier_semaphore()
    pl.semaphore_signal(barrier, inc=1, device_id=device, device_id_type=MESH)
    loads = [pltpu.make_async_copy(x_hbm.at[mine], x_buf, ld_sem.at[0]),
             pltpu.make_async_copy(wi_hbm, wi, ld_sem.at[1]),
             pltpu.make_async_copy(wm_hbm, wm, ld_sem.at[2]),
             pltpu.make_async_copy(wo_hbm, wo, ld_sem.at[3])]
    for copy in loads:
        copy.start()
    pl.semaphore_wait(barrier, 1)

    def block(j):
        return pl.ds(pl.multiple_of(j * HB, HB), HB)

    def keep(array, dst, j):
        return pltpu.make_async_copy(
            stage.at[array % 2, :, block(j)], dst.at[mine, block(j)], loc_sem.at[array, j])

    def send(array, dst, j):
        return pltpu.make_async_remote_copy(
            src_ref=stage.at[array % 2, :, block(j)], dst_ref=dst.at[mine, block(j)], send_sem=out_sem.at[array, j],
            recv_sem=in_sem.at[array, j], device_id=device, device_id_type=MESH)

    def flush(array, dst, j):
        keep(array, dst, j).start()
        send(array, dst, j).start()

    def drain(array, dst):
        @pl.loop(0, n_blk)
        def _(j):
            keep(array, dst, j).wait()
            send(array, dst, j).wait_send()

    def layer(array, feats, weight, b_ref, hid, slope, dst):
        @pl.loop(0, n_blk)
        def _(j):
            @pl.when(j >= 1)
            def _():
                flush(array, dst, j - 1)

            pre = dot(feats, weight[:, block(j)]) + b_ref[:, block(j)].astype(F32)
            cdf = 0.5 * (1.0 + lax.erf(pre * 0.7071067811865476))
            low = (pre * cdf).astype(BF16)
            hid[:, block(j)] = low
            stage[array % 2, :, block(j)] = low.astype(F32)
            slope[:, block(j)] = cdf + pre * jnp.exp(-0.5 * pre * pre) * 0.3989422804014327
        flush(array, dst, n_blk - 1)

    loads[0].wait()
    loads[1].wait()
    layer(0, x_buf[...].astype(BF16), wi, bi_ref, hid_one, slope_one, h1_hbm)
    loads[2].wait()
    layer(1, hid_one[...], wm, bm_ref, hid_two, slope_two, h2_hbm)
    loads[3].wait()
    proj = dot(hid_two[...], wo[...]) + bo_ref[...].astype(F32)
    inv_norm = lax.rsqrt(jnp.sum(proj * proj, axis=-1, keepdims=True))
    unit = proj * inv_norm
    g_emb = ge_ref[mine]
    g_proj = (g_emb - unit * jnp.sum(unit * g_emb, axis=-1, keepdims=True)) * inv_norm
    gp_low = g_proj.astype(BF16)
    gp_stage[...] = gp_low.astype(F32)
    gp_ref[mine] = gp_low.astype(F32)
    snd[:, 2 * n_hid:] = jnp.sum(g_proj, axis=0, keepdims=True)
    drain(0, h1_hbm)

    @pl.loop(0, n_blk)
    def _(j):
        @pl.when(j >= 1)
        def _():
            flush(2, g2_hbm, j - 1)

        g_hid = dot_t(gp_low, wo[block(j), :])
        g_pre = g_hid.astype(BF16).astype(F32) * slope_two[:, block(j)]
        snd[:, block(j)] = jnp.sum(g_pre, axis=0, keepdims=True)
        low = g_pre.astype(BF16)
        grad_two[:, block(j)] = low
        stage[0, :, block(j)] = low.astype(F32)
    flush(2, g2_hbm, n_blk - 1)
    gp_send = pltpu.make_async_remote_copy(
        src_ref=gp_stage, dst_ref=gp_ref.at[mine], send_sem=gp_sem.at[0], recv_sem=gp_sem.at[1],
        device_id=device, device_id_type=MESH)
    gp_send.start()
    drain(1, h2_hbm)

    @pl.loop(0, n_blk)
    def _(j):
        @pl.when(j >= 1)
        def _():
            flush(3, g1_hbm, j - 1)

        g_hid = dot_t(grad_two[...], wm[block(j), :])
        g_pre = g_hid.astype(BF16).astype(F32) * slope_one[:, block(j)]
        snd[:, pl.ds(pl.multiple_of(n_hid + j * HB, HB), HB)] = jnp.sum(g_pre, axis=0, keepdims=True)
        stage[1, :, block(j)] = g_pre.astype(BF16).astype(F32)
    flush(3, g1_hbm, n_blk - 1)
    bias_send = pltpu.make_async_remote_copy(
        src_ref=snd, dst_ref=rcv, send_sem=bs_sem.at[0], recv_sem=bs_sem.at[1],
        device_id=device, device_id_type=MESH)
    bias_send.start()
    drain(2, g2_hbm)
    drain(3, g1_hbm)
    gp_send.wait()
    bias_send.wait()
    bias_ref[...] = snd[...] + rcv[...]
    for array, dst in enumerate((h1_hbm, h2_hbm, g2_hbm, g1_hbm)):
        @pl.loop(0, n_blk)
        def _(j):
            send(array, dst, j).wait_recv()


def head_pass(x_all, w_in, b_in, w_mid, b_mid, w_out, b_out, g_emb):
    rows, feat = x_all.shape
    n_hid, n_out = w_out.shape
    half = rows // 2
    n_blk = n_hid // HB
    n_bias = 2 * n_hid + n_out
    dma = pltpu.SemaphoreType.DMA
    wide = jax.ShapeDtypeStruct((rows, n_hid), F32)
    return pl.pallas_call(
        head_kernel,
        out_shape=(wide, wide, wide, wide, jax.ShapeDtypeStruct((rows, n_out), F32),
                   jax.ShapeDtypeStruct((1, n_bias), F32)),
        in_specs=[HBM] * 4 + [VMEM] * 4,
        out_specs=(HBM,) * 4 + (VMEM,) * 2,
        scratch_shapes=[
            pltpu.VMEM((half, feat), F32),
            pltpu.VMEM((feat, n_hid), BF16),
            pltpu.VMEM((n_hid, n_hid), BF16),
            pltpu.VMEM((n_hid, n_out), BF16),
            pltpu.VMEM((half, n_hid), BF16),
            pltpu.VMEM((half, n_hid), BF16),
            pltpu.VMEM((half, n_hid), F32),
            pltpu.VMEM((half, n_hid), F32),
            pltpu.VMEM((2, half, n_hid), F32),
            pltpu.VMEM((half, n_hid), BF16),
            pltpu.VMEM((half, n_out), F32),
            pltpu.VMEM((1, n_bias), F32),
            pltpu.VMEM((1, n_bias), F32),
            dma((4,)), dma((4, n_blk)), dma((4, n_blk)), dma((4, n_blk)), dma((2,)), dma((2,)),
        ],
        compiler_params=pltpu.CompilerParams(
            collective_id=3, has_side_effects=True, vmem_limit_bytes=63 << 20),
        cost_estimate=pl.CostEstimate(
            flops=2 * rows * (feat + 2 * n_hid) * n_hid, bytes_accessed=16 * rows * n_hid, transcendentals=2 * rows * n_hid),
        name="head_pass",
    )(x_all, w_in, w_mid, w_out, b_in.reshape(1, -1), b_mid.reshape(1, -1), b_out.reshape(1, -1), g_emb)


def wgrad_kernel(first, n_step, base, *refs):
    if first:
        a_ref, b_ref, src, out_ref, dst, low, cbuf, rd_sem, wr_sem = refs
    else:
        a_ref, b_ref, src, _, out_ref, dst, low, cbuf, rd_sem, wr_sem = refs
    i = pl.program_id(0)
    chunk = cbuf.shape[2]

    def cols(step):
        return pl.ds(pl.multiple_of(base + step * chunk, chunk), chunk)

    def read(step):
        return pltpu.make_async_copy(src.at[:, cols(step)], cbuf.at[step % RING], rd_sem.at[step % RING])

    def write(step):
        return pltpu.make_async_copy(cbuf.at[step % RING], dst.at[:, cols(step)], wr_sem.at[step % RING])

    @pl.when(i == 0)
    def _():
        read(0).start()
        read(1).start()
        low[...] = b_ref[...].astype(BF16)

    @pl.when(i >= 2)
    def _():
        write(i - 2).wait()

    @pl.when(i + 2 < n_step)
    def _():
        read(i + 2).start()

    read(i).wait()
    write(i).start()
    out_ref[...] = lax.dot_general(
        a_ref[...].astype(BF16), low[...], (((0,), (0,)), ((), ())), preferred_element_type=F32)

    @pl.when(i == n_step - 1)
    def _():
        write(i - 1).wait()
        write(i).wait()


def wgrad(left, right, src, dst, start, width, block=256):
    rows, n_left = left.shape
    n_right = right.shape[1]
    n_step = n_left // block
    first = dst is None
    chunk = width // n_step
    args = (left, right, src) + (() if first else (dst,))
    return pl.pallas_call(
        functools.partial(wgrad_kernel, first, n_step, start),
        grid=(n_step,),
        out_shape=(jax.ShapeDtypeStruct((n_left, n_right), F32), jax.ShapeDtypeStruct(src.shape, F32)),
        in_specs=[pl.BlockSpec((rows, block), lambda i: (0, i)),
                  pl.BlockSpec((rows, n_right), lambda i: (0, 0), pipeline_mode=pl.Buffered(1)),
                  HBM] + ([] if first else [HBM]),
        out_specs=(pl.BlockSpec((block, n_right), lambda i: (i, 0)), HBM),
        scratch_shapes=[pltpu.VMEM((rows, n_right), BF16),
                        pltpu.VMEM((RING, src.shape[0], chunk), F32),
                        pltpu.SemaphoreType.DMA((RING,)), pltpu.SemaphoreType.DMA((RING,))],
        input_output_aliases={} if first else {3: 1},
        compiler_params=pltpu.CompilerParams(
            dimension_semantics=("arbitrary",), vmem_limit_bytes=63 << 20),
        cost_estimate=pl.CostEstimate(
            flops=2 * rows * n_left * n_right, bytes_accessed=8 * src.shape[0] * width, transcendentals=0),
        name="wgrad",
    )(*args)


def solution(mesh):
    n_vp = mesh.shape['vp']
    n_dp = mesh.shape['dp']

    def local_step(student_x, teacher_x, w_in, b_in, w_mid, b_mid, w_out, b_out, protos,
                   ema_w_in, ema_b_in, ema_w_mid, ema_b_mid, ema_w_out, ema_b_out, ema_protos):
        rows, feat = student_x.shape
        n_img = rows // ALL_CROPS
        width = protos.shape[0]
        x_loc = student_x.reshape(n_img, ALL_CROPS, feat).transpose(1, 0, 2)
        t_loc = teacher_x.reshape(n_img, GLOBAL_CROPS, feat).transpose(1, 0, 2).reshape(-1, feat)
        t_emb = mlp_forward(t_loc, ema_w_in, ema_b_in, ema_w_mid, ema_b_mid, ema_w_out, ema_b_out)
        s_emb = mlp_forward(x_loc.reshape(rows, feat), w_in, b_in, w_mid, b_mid, w_out, b_out)
        z_loc = jnp.concatenate([s_emb, t_emb], axis=0).reshape(ALL_CROPS + GLOBAL_CROPS, n_img, width)
        z_all = gather_dp(z_loc, n_dp, 0).reshape(-1, width).astype(BF16)
        z_s, z_t = z_all[:rows * n_dp], z_all[rows * n_dp:]
        c_all, row_sum, r_row, g_emb, loss = sinkhorn_stats(z_s, z_t, protos, ema_protos, n_vp, n_dp)
        g_temp, g_emb, loss, x_all = proto_grads(
            z_s, z_t, row_sum, r_row, c_all, g_emb, loss, x_loc.astype(F32), protos, ema_protos, n_vp, n_dp)
        x_all = x_all.reshape(rows * n_dp, feat)
        hid_one, hid_two, g_two, g_one, g_proj, biases = head_pass(
            x_all, w_in, b_in, w_mid, b_mid, w_out, b_out, g_emb)
        n_hid = w_mid.shape[0]
        part = protos.shape[1] // 8
        g_w_mid, g_protos = wgrad(hid_one, g_two, g_temp, None, 0, 4 * part)
        g_w_in, g_protos = wgrad(x_all, g_one, g_temp, g_protos, 4 * part, 3 * part)
        g_w_out, g_protos = wgrad(hid_two, g_proj, g_temp, g_protos, 7 * part, part)
        biases = biases.reshape(-1)
        g_b_mid, g_b_in, g_b_out = biases[:n_hid], biases[n_hid:2 * n_hid], biases[2 * n_hid:]
        return (loss.reshape(()), g_w_in, g_b_in, g_w_mid, g_b_mid, g_w_out, g_b_out, g_protos)

    by_rows = P('dp', None)
    by_cols = P(None, 'vp')
    replicated = P()
    head_specs = (replicated,) * 6
    in_specs = (by_rows, by_rows) + head_specs + (by_cols,) + head_specs + (by_cols,)
    out_specs = (replicated,) * 7 + (by_cols,)
    return jax.shard_map(local_step, mesh=mesh, in_specs=in_specs, out_specs=out_specs, check_vma=False)
```
